32 devices in a mesh: section: 2 (over x), ctx: 2 (over y), dp: 8 (over z, core).
Axes of the slice: x: 2, y: 2, z: 4, core: 2. Of those that a mesh axis runs over, the one named last changes fastest.
Arguments:
- tokens: bfloat16 [2, 8, 256, 2048], P(None, 'dp', 'ctx'), may hold values from -6 to 6
- cotangent: bfloat16 [2, 8, 256, 2048], P(None, 'dp', 'ctx'), may hold values from -6 to 6
- segment_ids: int32 [2, 8, 256], P(None, 'dp'), may hold values from 0 to 7, never falling along the last dimension, each value on 1 to 192 neighbouring positions
- w_query: bfloat16 [2, 2048, 2048], P('section', 'dp'), may hold values from -0.125 to 0.125
- w_keyvalue: bfloat16 [2, 2048, 256], P('section', 'dp'), may hold values from -0.125 to 0.125
- w_out: bfloat16 [2, 2048, 2048], P('section', 'dp'), may hold values from -0.75 to 0.75
- w_up: bfloat16 [2, 2048, 8192], P('section', 'dp'), may hold values from -0.125 to 0.125
- w_down: bfloat16 [2, 8192, 2048], P('section', 'dp'), may hold values from -0.0625 to 0.0625
- ln_gains: bfloat16 [2, 2, 2048], P('section', None, 'dp'), may hold values from 0.25 to 1.75
- ln_biases: bfloat16 [2, 2, 2048], P('section', None, 'dp'), may hold values from -1.5 to 1.5
Outputs:
- section_outputs: bfloat16 [2, 2, 8, 256, 2048], P('section', None, 'dp', 'ctx')
- input_grads: bfloat16 [2, 2, 8, 256, 2048], P('section', None, 'dp', 'ctx')
- grad_query: float32 [2, 2048, 2048], P('section', 'dp')
- grad_keyvalue: float32 [2, 2048, 256], P('section', 'dp')
- grad_out: float32 [2, 2048, 2048], P('section', 'dp')
- grad_up: float32 [2, 2048, 8192], P('section', 'dp')
- grad_down: float32 [2, 8192, 2048], P('section', 'dp')
- grad_gains: float32 [2, 2, 2048], P('section', None, 'dp')
- grad_biases: float32 [2, 2, 2048], P('section', None, 'dp')
The draws below stay inside these ranges and needn't reach their ends.
Inputs may be any that keep to these rules, and one draw needn't show every extreme that they name: `segment_ids`: in each sequence the ids start at 0 and never fall; 8 documents of 1 to 192 tokens, the longest exactly 192.
All inputs are finite; a program needn't handle non-finite values.
Results may differ from the reference program's by a relative error of at most 0.024.
Values may be sent and summed in bfloat16 or wider, within the bound.
A program may use at most 384 MiB of HBM per device.

```python
import math
import jax
import jax.numpy as jnp
import numpy as np
from jax import lax

D = 2048
HEADS = 16
HEAD = 128
FF = 8192
MICRO = 2
LEN = 256
SEQS = 8
DOCS = 8
MOST = 192


def levels(rng, shape, cuts, least, high):
    loudness = 1.0
    for axis_at, parts in cuts:
        heights = jax.random.uniform(jax.random.fold_in(jax.random.fold_in(rng, 6), axis_at), (parts,), jnp.float32, least / len(cuts), high / len(cuts))
        loudness = loudness * jnp.repeat(jnp.exp(heights), shape[axis_at] // parts).reshape((-1,) + (1,) * (len(shape) - 1 - axis_at))
    return loudness


def length_profile(number_of, total, most, lean):
    portions = [(1 << 20) // math.isqrt(rank ** lean) + 1 for rank in range(2, number_of + 1)]
    rest, given = total - most - (number_of - 1), [1] * (number_of - 1)
    while rest > 0:
        candidates = [i for i in range(number_of - 1) if given[i] < most]
        mass, left = sum([portions[i] for i in candidates]), rest
        for i in candidates:
            extra = min(most - given[i], max(1, left * portions[i] // mass), rest)
            given[i] = given[i] + extra
            rest = rest - extra
    return np.array([most] + given)


def ragged_sizes(key, count, total, bound, skew):
    if count == 2:
        one = jax.random.randint(key, (), max(1, total - bound), min(bound, total - 1) + 1)
        return jnp.stack([one, total - one])
    lengths = jnp.asarray(length_profile(count, total, bound, skew), jnp.int32)
    pairs = (count - 1) // 2
    source_of, taker = lengths[1:1 + 2 * pairs:2], lengths[2:2 + 2 * pairs:2]
    margin = jnp.minimum(source_of - 1, bound - taker)
    shifted = jax.random.randint(jax.random.fold_in(key, 1), (pairs,), 0, 1 << 20) % (margin + 1)
    lengths = lengths.at[1:1 + 2 * pairs:2].set(source_of - shifted).at[2:2 + 2 * pairs:2].set(taker + shifted)
    return lengths[jax.random.permutation(jax.random.fold_in(key, 2), count)]


def scatter_about(key, extent, width, limit, pieces=(), held_as=jnp.bfloat16):
    values = width * jax.random.normal(key, extent, jnp.float32)
    if pieces:
        values = values * levels(key, extent, pieces, -0.22, 0.18)
    return jnp.clip(values, -limit, limit).astype(held_as)


def setup_inputs(seed: int = 0) -> dict:
    seeds = jax.random.split(jax.random.key(seed), 11)
    return {
        "tokens": scatter_about(seeds[0], (MICRO, SEQS, LEN, D), 1.0, 6.0, ((1, 8), (2, 2))),
        "cotangent": scatter_about(seeds[1], (MICRO, SEQS, LEN, D), 1.0, 6.0, ((1, 8), (2, 2))),
        "segment_ids": jax.vmap(lambda own: jnp.searchsorted(jnp.cumsum(ragged_sizes(own, DOCS, LEN, MOST, 2)), jnp.arange(LEN), side="right"))(jax.random.split(seeds[2], MICRO * SEQS)).reshape((MICRO, SEQS, LEN)).astype(jnp.int32),
        "w_query": scatter_about(seeds[3], (2, D, D), D ** -0.5, 0.125, ((0, 2), (1, 8))),
        "w_keyvalue": scatter_about(seeds[4], (2, D, 2 * HEAD), D ** -0.5, 0.125, ((0, 2), (1, 8))),
        "w_out": scatter_about(seeds[5], (2, D, D), (D // 32) ** -0.5, 0.75, ((0, 2), (1, 8))),
        "w_up": scatter_about(seeds[6], (2, D, FF), D ** -0.5, 0.125, ((0, 2), (1, 8))),
        "w_down": scatter_about(seeds[7], (2, FF, D), FF ** -0.5, 0.0625, ((0, 2), (1, 8))),
        "ln_gains": jnp.clip(1.0 + 0.15 * jax.random.normal(seeds[8], (2, 2, D), jnp.float32), 0.25, 1.75).astype(jnp.bfloat16),
        "ln_biases": scatter_about(seeds[9], (2, 2, D), 0.3, 1.5, ((0, 2), (2, 8))),
    }


epsilon = 1e-05
masked_score = -1000000000.0

@jax.custom_vjp
def low(v):
    return lax.optimization_barrier(v.astype(jnp.bfloat16)).astype(jnp.float32)

@jax.custom_vjp
def low_back(v):
    return v

def low_keep(v):
    return (low(v), None)

def low_pass(kept, grad):
    return (grad,)

def back_keep(v):
    return (v, None)

def back_low(kept, grad):
    return (low(grad),)
low.defvjp(low_keep, low_pass)
low_back.defvjp(back_keep, back_low)

def product(left, right):
    return jnp.dot(left, right, precision=lax.Precision.HIGHEST, preferred_element_type=jnp.float32)

def layer_norm(values_in, gain_row, bias_row):
    mean_row = lax.optimization_barrier(jnp.mean(values_in, axis=-1, keepdims=True))
    centered = values_in - mean_row
    variance = lax.optimization_barrier(jnp.mean(centered * centered, axis=-1, keepdims=True))
    return centered * lax.rsqrt(variance + epsilon) * gain_row + bias_row

def attend(inputs):
    query_rows, keyvalue, segments = inputs
    length = query_rows.shape[0]
    heads_view = query_rows.reshape(length, HEADS, HEAD)
    key_rows = keyvalue[:, :HEAD]
    values = keyvalue[:, HEAD:]
    scores = jnp.einsum('qhd,kd->hqk', heads_view, key_rows, precision=lax.Precision.HIGHEST) * HEAD ** (-0.5)
    scores = low_back(scores)
    position = jnp.arange(length, dtype=jnp.int32)
    allowed = (position[:, None] >= position[None, :]) & (segments[:, None] == segments[None, :])
    scores = jnp.where(allowed[None], scores, masked_score)
    attn_probs = low(jax.nn.softmax(scores, axis=-1))
    mixed_rows = jnp.einsum('hqk,kd->qhd', attn_probs, values, precision=lax.Precision.HIGHEST)
    return mixed_rows.reshape(length, HEADS * HEAD)

def layer(hidden, segments, w_query, w_keyvalue, w_out, w_up, w_down, gains, biases):
    shape_in = hidden.shape
    number = segments.shape[0]
    flat_rows = hidden.reshape(-1, D)
    normed = low(layer_norm(flat_rows, gains[0], biases[0]))
    query_rows = low(low_back(product(normed, w_query)))
    keyvalue = low(low_back(product(normed, w_keyvalue)))
    mixed_rows = lax.map(jax.checkpoint(attend), (query_rows.reshape(number, -1, D), keyvalue.reshape(number, -1, 2 * HEAD), segments))
    mixed_rows = low(low_back(mixed_rows.reshape(-1, D)))
    after = flat_rows + low_back(product(mixed_rows, w_out))
    normed_two = low(layer_norm(after, gains[1], biases[1]))
    up_rows = low_back(product(normed_two, w_up))
    activated = low(jax.nn.gelu(up_rows, approximate=True))
    result = after + low_back(product(activated, w_down))
    return result.reshape(shape_in)

def reference(tokens, cotangent, segment_ids, w_query, w_keyvalue, w_out, w_up, w_down, ln_gains, ln_biases):
    segments = segment_ids.reshape(-1, LEN).astype(jnp.int32)
    start = tokens.astype(jnp.float32).reshape(-1, LEN, D)
    probe = jnp.zeros_like(start)
    query_all = w_query.astype(jnp.float32)
    keyvalue_all = w_keyvalue.astype(jnp.float32)
    out_all = w_out.astype(jnp.float32)
    up_all = w_up.astype(jnp.float32)
    down_all = w_down.astype(jnp.float32)
    gains_all = ln_gains.astype(jnp.float32)
    biases_all = ln_biases.astype(jnp.float32)

    def forward(first_in, probe_in, query_w, keyvalue_w, out_w, up_w, down_w, gains_w, biases_w):
        first = layer(first_in, segments, query_w[0], keyvalue_w[0], out_w[0], up_w[0], down_w[0], gains_w[0], biases_w[0])
        passed = low(low_back(first)) + probe_in
        second = layer(passed, segments, query_w[1], keyvalue_w[1], out_w[1], up_w[1], down_w[1], gains_w[1], biases_w[1])
        return (first, second)
    outputs, pullback = jax.vjp(forward, start, probe, query_all, keyvalue_all, out_all, up_all, down_all, gains_all, biases_all)
    first, second = outputs
    grads = pullback((jnp.zeros_like(first), cotangent.astype(jnp.float32).reshape(-1, LEN, D)))
    shape_out = (2,) + tokens.shape
    section_outputs = jnp.stack([first, second]).reshape(shape_out).astype(jnp.bfloat16)
    input_grads = jnp.stack([grads[0], grads[1]]).reshape(shape_out).astype(jnp.bfloat16)
    return (section_outputs, input_grads, grads[2], grads[3], grads[4], grads[5], grads[6], grads[7], grads[8])
```

```python
import jax
import jax.numpy as jnp
from jax import lax
from jax.sharding import PartitionSpec as P

HEADS = 16
HEAD = 128


epsilon = 1e-05
masked_score = -1000000000.0


def from_behind(x, axis, by):
    devices = lax.axis_size(axis)
    pairs = [(i, i + by) for i in range(devices) if 0 <= i + by < devices]
    return lax.ppermute(x, axis, pairs)


def layer_norm(values_in, gain_row, bias_row):
    mean_row = jnp.mean(values_in, axis=-1, keepdims=True)
    centered = values_in - mean_row
    variance = jnp.mean(centered * centered, axis=-1, keepdims=True)
    return centered * lax.rsqrt(variance + epsilon) * gain_row + bias_row


def dense(left, right):
    return jnp.dot(left, right, preferred_element_type=jnp.float32)


def dense_left(left, right):
    return lax.dot_general(
        left, right, (((0,), (0,)), ((), ())), preferred_element_type=jnp.float32
    )


def dense_right(left, right):
    return lax.dot_general(
        left, right, (((1,), (1,)), ((), ())), preferred_element_type=jnp.float32
    )


def allowed_keys(segments, cycle_place, cycle_size, tok_rows):
    offsets = jnp.arange(tok_rows, dtype=jnp.int32)
    query_pos = cycle_place * tok_rows + offsets
    query_seg = lax.dynamic_slice_in_dim(segments, cycle_place * tok_rows, tok_rows, axis=1)
    blocks = []
    for cycle_step in range(cycle_size):
        source = cycle_place - cycle_step
        key_pos = source * tok_rows + offsets
        key_seg = lax.dynamic_slice_in_dim(
            segments, jnp.maximum(source, 0) * tok_rows, tok_rows, axis=1
        )
        blocks.append(
            (source >= 0)
            & (key_pos[None, None, :] <= query_pos[None, :, None])
            & (key_seg[:, None, :] == query_seg[:, :, None])
        )
    return jnp.concatenate(blocks, axis=2)


def batched(left, right, left_dim, right_dim):
    return lax.dot_general(
        left, right, (((left_dim,), (right_dim,)), ((0,), (0,))), preferred_element_type=jnp.float32
    )


def head_scores(query, keyvalue_all, allowed):
    micro, rows, _ = allowed.shape
    head_rows = query.reshape(micro, rows * HEADS, HEAD)
    scores = batched(head_rows, keyvalue_all[:, :, :HEAD], 2, 2) * HEAD ** (-0.5)
    scores = scores.reshape(micro, rows, HEADS, -1)
    scores = jnp.where(allowed[:, :, None, :], scores, masked_score)
    return (scores.reshape(micro, rows * HEADS, -1), head_rows)


def layer_forward(hidden, segments, weights, micro, cycle_place, cycle_size):
    w_query, w_keyvalue, w_out, w_up, w_down, gains, biases = weights
    rows = hidden.shape[0] // micro
    normed = layer_norm(hidden, gains[0], biases[0]).astype(jnp.bfloat16)
    query = dense(normed, w_query).astype(jnp.bfloat16)
    keyvalue = dense(normed, w_keyvalue).astype(jnp.bfloat16)
    moving = from_behind(keyvalue, "ctx", 1)
    keyvalue_all = jnp.concatenate(
        [keyvalue.reshape(micro, rows, -1), moving.reshape(micro, rows, -1)], axis=1
    )
    allowed = allowed_keys(segments, cycle_place, cycle_size, rows)
    scores, _ = head_scores(query, keyvalue_all, allowed)
    top_score = jnp.max(scores, axis=2, keepdims=True)
    log_total = top_score + jnp.log(jnp.sum(jnp.exp(scores - top_score), axis=2, keepdims=True))
    attn_probs = jnp.exp(scores - log_total).astype(jnp.bfloat16)
    mixed = (
        batched(attn_probs, keyvalue_all[:, :, HEAD:], 2, 1)
        .reshape(micro * rows, HEADS * HEAD)
        .astype(jnp.bfloat16)
    )
    after = hidden + dense(mixed, w_out)
    normed_two = layer_norm(after, gains[1], biases[1]).astype(jnp.bfloat16)
    up_rows = dense(normed_two, w_up)
    activated = jax.nn.gelu(up_rows, approximate=True).astype(jnp.bfloat16)
    result = after + dense(activated, w_down)
    kept = (
        hidden,
        normed,
        query,
        keyvalue_all,
        log_total,
        mixed,
        after,
        normed_two,
        up_rows,
        activated,
    )
    return (result, kept)


def layer_backward(grad_result, kept, segments, weights, micro, cycle_place, cycle_size):
    w_query, w_keyvalue, w_out, w_up, w_down, gains, biases = weights
    hidden, normed, query, keyvalue_all, log_total, mixed, after, normed_two, up_rows, activated = (
        kept
    )
    rows = hidden.shape[0] // micro
    grad_low = grad_result.astype(jnp.bfloat16)
    grad_act = dense_right(grad_low, w_down)
    _, gelu_back = jax.vjp(lambda entries: jax.nn.gelu(entries, approximate=True), up_rows)
    grad_upper = gelu_back(grad_act)[0].astype(jnp.bfloat16)
    _, norm_back_two = jax.vjp(layer_norm, after, gains[1], biases[1])
    grad_after_norm, grad_gain_two, grad_bias_two = norm_back_two(dense_right(grad_upper, w_up))
    grad_after = grad_result + grad_after_norm
    grad_branch = grad_after.astype(jnp.bfloat16)
    grad_mixed = (
        dense_right(grad_branch, w_out).astype(jnp.bfloat16).reshape(micro, rows * HEADS, HEAD)
    )
    allowed = allowed_keys(segments, cycle_place, cycle_size, rows)
    scores, head_rows = head_scores(query, keyvalue_all, allowed)
    attn_probs = jnp.exp(scores - log_total)
    grad_probs = batched(grad_mixed, keyvalue_all[:, :, HEAD:], 2, 2)
    grad_values = batched(attn_probs.astype(jnp.bfloat16), grad_mixed, 1, 1)
    inner = jnp.sum(attn_probs * grad_probs, axis=2, keepdims=True)
    grad_scores = (attn_probs * (grad_probs - inner)).astype(jnp.bfloat16)
    scale_factor = HEAD ** (-0.5)
    grad_queries = (
        (batched(grad_scores, keyvalue_all[:, :, :HEAD], 2, 1) * scale_factor)
        .astype(jnp.bfloat16)
        .reshape(micro * rows, HEADS * HEAD)
    )
    grad_keys = batched(grad_scores, head_rows, 1, 1) * scale_factor
    grad_pieces = jnp.concatenate([grad_keys, grad_values], axis=2)
    carried = grad_pieces[:, (cycle_size - 1) * rows :]
    carried = (
        from_behind(carried.astype(jnp.bfloat16), "ctx", -1).astype(carried.dtype)
        + grad_pieces[:, 0:rows]
    )
    grad_kv = carried.astype(jnp.bfloat16).reshape(micro * rows, -1)
    grad_normed = dense_right(grad_queries, w_query) + dense_right(grad_kv, w_keyvalue)
    _, norm_back_one = jax.vjp(layer_norm, hidden, gains[0], biases[0])
    grad_hidden, grad_gain_one, grad_bias_one = norm_back_one(grad_normed)
    grad_input = grad_after + grad_hidden
    terms = (
        normed,
        grad_queries,
        grad_kv,
        mixed,
        grad_branch,
        normed_two,
        grad_upper,
        activated,
        grad_low,
        jnp.stack([grad_gain_one, grad_gain_two, grad_bias_one, grad_bias_two]),
    )
    return (grad_input, terms)


def body(
    tokens, cotangent, segment_ids, w_query, w_keyvalue, w_out, w_up, w_down, ln_gains, ln_biases
):
    section_index = lax.axis_index("section")
    cycle_place = lax.axis_index("ctx")
    cycle_size = lax.axis_size("ctx")
    micro = tokens.shape[0]
    width = tokens.shape[3]
    early = section_index == 0
    late = section_index == 1
    segments = segment_ids[:, 0]
    own_tokens = tokens[:, 0].reshape(-1, width)
    own_cotangent = cotangent[:, 0].reshape(-1, width)

    def spread(weight):
        half = weight.shape[1] // cycle_size
        part = lax.dynamic_slice_in_dim(weight, cycle_place * half, half, axis=1)
        return lax.all_gather(part, ("dp", "ctx"), axis=1, tiled=True)[0]

    scales = lax.all_gather(
        jnp.concatenate([ln_gains, ln_biases], axis=1), "dp", axis=2, tiled=True
    )[0].astype(jnp.float32)
    weights = (
        spread(w_query),
        lax.all_gather(w_keyvalue, "dp", axis=1, tiled=True)[0],
        spread(w_out),
        spread(w_up),
        spread(w_down),
        scales[0:2],
        scales[2:4],
    )
    result, kept_first = layer_forward(
        own_tokens.astype(jnp.float32), segments, weights, micro, cycle_place, cycle_size
    )
    first_low = result.astype(jnp.bfloat16)
    incoming = from_behind(first_low, "section", 1)
    result, kept_second = layer_forward(
        incoming.astype(jnp.float32), segments, weights, micro, cycle_place, cycle_size
    )
    second_low = result.astype(jnp.bfloat16)
    grad, terms_second = layer_backward(
        own_cotangent.astype(jnp.float32), kept_second, segments, weights, micro, cycle_place,
        cycle_size,
    )
    grad_second = grad.astype(jnp.bfloat16)
    arriving = from_behind(grad_second, "section", -1)
    grad, terms_first = layer_backward(
        arriving.astype(jnp.float32), kept_first, segments, weights, micro, cycle_place, cycle_size
    )
    grad_first = grad.astype(jnp.bfloat16)
    section_rows = jnp.where(early, first_low, second_low)
    grad_rows = jnp.where(early, grad_first, grad_second)
    (
        normed_all,
        grad_queries_all,
        grad_kv_all,
        mixed_all,
        grad_branch_all,
        normed_two_all,
        grad_upper_all,
        activated_all,
        grad_low_all,
        scale_terms,
    ) = [jnp.where(early, one, two) for one, two in zip(terms_first, terms_second)]

    def reduced(left, right):
        part = dense_left(left, right).astype(jnp.bfloat16)
        piece = lax.psum_scatter(part, ("dp", "ctx"), scatter_dimension=0, tiled=True)
        return lax.all_gather(piece, "ctx", axis=0, tiled=True).astype(jnp.float32)[None]

    grad_down = reduced(activated_all, grad_low_all)
    grad_up = reduced(normed_two_all, grad_upper_all)
    grad_out = reduced(mixed_all, grad_branch_all)
    grad_query = reduced(normed_all, grad_queries_all)
    grad_keyvalue = reduced(normed_all, grad_kv_all)
    scale_grads = lax.psum(
        lax.psum_scatter(
            scale_terms.astype(jnp.bfloat16), "dp", scatter_dimension=1, tiled=True
        ),
        "ctx",
    ).astype(jnp.float32)[None]
    local = (1, micro, 1, own_tokens.shape[0] // micro, width)
    return (
        section_rows.reshape(local),
        grad_rows.reshape(local),
        grad_query,
        grad_keyvalue,
        grad_out,
        grad_up,
        grad_down,
        scale_grads[:, 0:2],
        scale_grads[:, 2:4],
    )


def solution(mesh):
    in_specs = (
        P(None, "dp", "ctx", None),
        P(None, "dp", "ctx", None),
        P(None, "dp", None),
        P("section", "dp", None),
        P("section", "dp", None),
        P("section", "dp", None),
        P("section", "dp", None),
        P("section", "dp", None),
        P("section", None, "dp"),
        P("section", None, "dp"),
    )
    out_specs = (
        P("section", None, "dp", "ctx", None),
        P("section", None, "dp", "ctx", None),
        P("section", "dp", None),
        P("section", "dp", None),
        P("section", "dp", None),
        P("section", "dp", None),
        P("section", "dp", None),
        P("section", None, "dp"),
        P("section", None, "dp"),
    )
    return jax.shard_map(body, mesh=mesh, in_specs=in_specs, out_specs=out_specs, check_vma=False)
```

```python
import functools
import math

import jax
import jax.numpy as jnp
from jax import lax
from jax.experimental import pallas as pl
from jax.experimental.pallas import tpu as pltpu
from jax.sharding import PartitionSpec as P

HEADS = 16
HEAD = 128


epsilon = 1e-05
masked_score = -1000000000.0


def layer_norm(values_in, gain_row, bias_row):
    mean_row = jnp.mean(values_in, axis=-1, keepdims=True)
    centered = values_in - mean_row
    variance = jnp.mean(centered * centered, axis=-1, keepdims=True)
    return centered * lax.rsqrt(variance + epsilon) * gain_row + bias_row


def dense(left, right):
    return jnp.dot(left, right, preferred_element_type=jnp.float32)


def dense_left(left, right):
    return lax.dot_general(
        left, right, (((0,), (0,)), ((), ())), preferred_element_type=jnp.float32
    )


def dense_right(left, right):
    return lax.dot_general(
        left, right, (((1,), (1,)), ((), ())), preferred_element_type=jnp.float32
    )


MESH = pl.DeviceIdType.MESH
PARTS = 2


def gelu(v):
    inner = math.sqrt(2.0 / math.pi) * (v + 0.044715 * v * v * v)
    return 0.5 * v * (1.0 + jnp.tanh(inner))


def gelu_slope(v):
    scale = math.sqrt(2.0 / math.pi)
    tanh = jnp.tanh(scale * (v + 0.044715 * v * v * v))
    return 0.5 * (1.0 + tanh) + 0.5 * v * (1.0 - tanh * tanh) * scale * (1.0 + 0.134145 * v * v)


def tile_at(step, size):
    return pl.ds(pl.multiple_of(step * size, size), size)


def flat(block):
    return block.reshape(block.shape[0] * block.shape[1], block.shape[2])


def store_part(part, columns, values):
    rows = part.shape[1]
    part[0, :, columns] = values[:rows]
    part[1, :, columns] = values[rows:]


def masked_probs(query, key, mask):
    scores = dense_right(query, key) * HEAD ** (-0.5)
    scores = jnp.where(mask, scores, masked_score)
    scores = jnp.exp(scores - jnp.max(scores, axis=1, keepdims=True))
    return scores / jnp.sum(scores, axis=1, keepdims=True)


def mask_of(seg_col, seg_row, at):
    length = seg_row.shape[2]
    place = lax.broadcasted_iota(jnp.int32, (length, length), 0)
    source = lax.broadcasted_iota(jnp.int32, (length, length), 1)
    return (source <= place) & (seg_col[at] == seg_row[at])


def ffn_forward_at(at, gath, part, weights, ins, outs):
    w_up, w_down = weights
    up_out, act_out = outs
    size = 256

    def up_tile(step, carry):
        columns = tile_at(step, size)
        up_rows = dense(flat(gath[at]), w_up[:, columns])
        up_out[at, :, columns] = up_rows.astype(jnp.bfloat16)
        act_out[at, :, columns] = gelu(up_rows).astype(jnp.bfloat16)
        return carry

    lax.fori_loop(0, w_up.shape[1] // size, up_tile, 0)

    def down_tile(step, carry):
        columns = tile_at(step, size)
        store_part(part, columns, dense(act_out[at], w_down[:, columns]))
        return carry

    lax.fori_loop(0, w_down.shape[1] // size, down_tile, 0)


def ffn_backward_at(at, gath, part, weights, ins, outs):
    w_up, w_down = weights
    (up_in,) = ins
    (upper_out,) = outs
    size = 256

    def act_tile(step, carry):
        columns = tile_at(step, size)
        grad_act = dense_right(flat(gath[at]), w_down[columns, :])
        slope = gelu_slope(up_in[at, :, columns].astype(jnp.float32))
        upper_out[at, :, columns] = (grad_act * slope).astype(jnp.bfloat16)
        return carry

    lax.fori_loop(0, w_down.shape[0] // size, act_tile, 0)

    def back_tile(step, carry):
        columns = tile_at(step, size)
        store_part(part, columns, dense_right(upper_out[at], w_up[columns, :]))
        return carry

    lax.fori_loop(0, w_up.shape[0] // size, back_tile, 0)


def attention_forward_at(at, gath, part, weights, ins, outs):
    w_query, w_keyvalue, w_out = weights
    seg_col, seg_row = ins
    query_out, keyvalue_out, mixed_out = outs
    size = 256
    rows = flat(gath[at])
    query_out[at] = dense(rows, w_query[...]).astype(jnp.bfloat16)
    keyvalue_out[at] = dense(rows, w_keyvalue[...]).astype(jnp.bfloat16)
    mask = mask_of(seg_col, seg_row, at)
    for head in range(w_query.shape[1] // HEAD):
        own = slice(head * HEAD, (head + 1) * HEAD)
        probs = masked_probs(query_out[at, :, own], keyvalue_out[at, :, :HEAD], mask)
        mixed = dense(probs.astype(jnp.bfloat16), keyvalue_out[at, :, HEAD:])
        mixed_out[at, :, own] = mixed.astype(jnp.bfloat16)

    def out_tile(step, carry):
        columns = tile_at(step, size)
        store_part(part, columns, dense(mixed_out[at], w_out[:, columns]))
        return carry

    lax.fori_loop(0, w_out.shape[1] // size, out_tile, 0)


def attention_backward_at(at, gath, part, weights, ins, outs):
    w_query, w_keyvalue, w_out = weights
    seg_col, seg_row, query_in, keyvalue_in = ins
    query_out, keyvalue_out = outs
    size = 256
    scale = HEAD ** (-0.5)
    grad_mixed = dense_right(flat(gath[at]), w_out[...]).astype(jnp.bfloat16)
    key = keyvalue_in[at, :, :HEAD]
    value = keyvalue_in[at, :, HEAD:]
    mask = mask_of(seg_col, seg_row, at)
    grad_key = jnp.zeros(key.shape, jnp.float32)
    grad_value = jnp.zeros(value.shape, jnp.float32)
    for head in range(w_query.shape[1] // HEAD):
        own = slice(head * HEAD, (head + 1) * HEAD)
        query = query_in[at, :, own]
        branch = grad_mixed[:, own]
        probs = masked_probs(query, key, mask)
        grad_probs = dense_right(branch, value)
        inner = jnp.sum(probs * grad_probs, axis=1, keepdims=True)
        grad_scores = (probs * (grad_probs - inner)).astype(jnp.bfloat16)
        query_out[at, :, own] = (dense(grad_scores, key) * scale).astype(jnp.bfloat16)
        grad_key = grad_key + dense_left(grad_scores, query)
        grad_value = grad_value + dense_left(probs.astype(jnp.bfloat16), branch)
    keyvalue_out[at, :, :HEAD] = (grad_key * scale).astype(jnp.bfloat16)
    keyvalue_out[at, :, HEAD:] = grad_value.astype(jnp.bfloat16)

    def back_tile(step, carry):
        columns = tile_at(step, size)
        store_part(
            part,
            columns,
            dense_right(query_out[at], w_query[columns, :])
            + dense_right(keyvalue_out[at], w_keyvalue[columns, :]),
        )
        return carry

    lax.fori_loop(0, w_query.shape[0] // size, back_tile, 0)


def pass_kernel(compute, n_weights, n_ins, n_outs, places, *refs):
    refs = list(refs)
    take = lambda count: [refs.pop(0) for _ in range(count)]
    (x_ref,) = take(1)
    early_weights = take(n_weights)
    late_weights = take(n_weights)
    ins = take(n_ins)
    y_ref, gath = take(2)
    outs = take(n_outs)
    weights = take(n_weights)
    part, partner_out, partner_in, total, line_out, from_left, from_right = take(7)
    (
        weight_sem, gather_right, gather_left, gather_partner, gather_line_in, gather_partner_in,
        partner_send, partner_recv, right_send, right_recv, left_send, left_recv,
    ) = take(12)

    section = lax.axis_index("section")
    me = lax.axis_index("dp")
    z = me // 2
    k = me % 2
    last = places - 1
    rows = x_ref.shape[0]
    size = rows // PARTS
    right = {"dp": me + 2}
    left = {"dp": me - 2}
    partner = {"dp": 2 * z + 1 - k}
    has_left = z > 0
    has_right = z < last

    barrier = pltpu.get_barrier_semaphore()
    pl.semaphore_signal(barrier, inc=1, device_id=partner, device_id_type=MESH)

    @pl.when(has_left)
    def _():
        pl.semaphore_signal(barrier, inc=1, device_id=left, device_id_type=MESH)

    @pl.when(has_right)
    def _():
        pl.semaphore_signal(barrier, inc=1, device_id=right, device_id_type=MESH)

    for index in range(n_weights):

        @pl.when(section == 0)
        def _():
            pltpu.make_async_copy(early_weights[index], weights[index], weight_sem.at[index]).start()

        @pl.when(section != 0)
        def _():
            pltpu.make_async_copy(late_weights[index], weights[index], weight_sem.at[index]).start()

    peers = 1 + jnp.where(has_left, 1, 0) + jnp.where(has_right, 1, 0)
    pl.semaphore_wait(barrier, peers)

    def cut(index):
        return pl.ds(index * size, size)

    def to_right(block, index, source):
        return pltpu.make_async_remote_copy(
            source, gath.at[block, k, cut(index)], gather_right.at[block, index],
            gather_line_in.at[block, index], device_id=right, device_id_type=MESH,
        )

    def to_left(block, index, source):
        return pltpu.make_async_remote_copy(
            source, gath.at[block, k, cut(index)], gather_left.at[block, index],
            gather_line_in.at[block, index], device_id=left, device_id_type=MESH,
        )

    def to_partner(block, source):
        return pltpu.make_async_remote_copy(
            source, gath.at[block, k], gather_partner.at[block],
            gather_partner_in.at[block], device_id=partner, device_id_type=MESH,
        )

    def sum_to_partner(block):
        return pltpu.make_async_remote_copy(
            partner_out.at[block], partner_in.at[block], partner_send.at[block],
            partner_recv.at[block], device_id=partner, device_id_type=MESH,
        )

    def sum_to_right(block, index):
        return pltpu.make_async_remote_copy(
            line_out.at[block, cut(index)], from_left.at[block, cut(index)],
            right_send.at[block, index], right_recv.at[block, index],
            device_id=right, device_id_type=MESH,
        )

    def sum_to_left(block, index):
        return pltpu.make_async_remote_copy(
            line_out.at[block, cut(index)], from_right.at[block, cut(index)],
            left_send.at[block, index], left_recv.at[block, index],
            device_id=left, device_id_type=MESH,
        )

    for index in range(PARTS):

        @pl.when(has_right)
        def _():
            to_right(z, index, x_ref.at[cut(index)]).start()

        @pl.when(has_left)
        def _():
            to_left(z, index, x_ref.at[cut(index)]).start()

    to_partner(z, x_ref).start()
    gath[z, k] = x_ref[...]

    at_end = (z == 0) | (z == last)
    low_half = z < places // 2

    def step(i, carry):
        inner_block = jnp.where(i == 0, 1, jnp.where(i == 1, 0, i))
        low_block = jnp.where(z == 0, i, inner_block)
        high_block = last - jnp.where(z == last, i, inner_block)
        block = jnp.where(low_half, low_block, high_block)
        wave = jnp.where(at_end, i, jnp.where(i == 1, 1, jnp.where(i == 3, 2, 0)))
        from_low = z - wave
        from_high = z + wave

        @pl.when((wave > 0) & (from_low >= 0))
        def _():
            for index in range(PARTS):
                to_right(from_low, index, gath.at[from_low, k, cut(index)]).wait_recv()

                @pl.when(has_right)
                def _():
                    to_right(from_low, index, gath.at[from_low, k, cut(index)]).start()

            to_partner(from_low, gath.at[from_low, k]).start()

        @pl.when((wave > 0) & (from_high <= last))
        def _():
            for index in range(PARTS):
                to_left(from_high, index, gath.at[from_high, k, cut(index)]).wait_recv()

                @pl.when(has_left)
                def _():
                    to_left(from_high, index, gath.at[from_high, k, cut(index)]).start()

            to_partner(from_high, gath.at[from_high, k]).start()

        pltpu.make_async_remote_copy(
            gath.at[block, 1 - k], gath.at[block, 1 - k], gather_partner.at[block],
            gather_partner_in.at[block], device_id=partner, device_id_type=MESH,
        ).wait_recv()

        @pl.when(i == 0)
        def _():
            for index in range(n_weights):
                pltpu.make_async_copy(
                    early_weights[index], weights[index], weight_sem.at[index]
                ).wait()

        compute(block, gath, part, weights, ins, outs)
        partner_out[block] = part[1 - k].astype(jnp.bfloat16)
        sum_to_partner(block).start()
        sum_to_partner(block).wait_recv()
        total[block] = part[k] + partner_in[block].astype(jnp.float32)

        @pl.when((z == 0) & (block > 0))
        def _():
            line_out[block] = total[block].astype(jnp.bfloat16)
            for index in range(PARTS):
                sum_to_right(block, index).start()

        @pl.when((z == last) & (block < last))
        def _():
            line_out[block] = total[block].astype(jnp.bfloat16)
            for index in range(PARTS):
                sum_to_left(block, index).start()

        return carry

    lax.fori_loop(0, places, step, 0)

    n_left = jnp.where(has_left, places - z, 0)
    n_right = jnp.where(has_right, z + 1, 0)
    n_first = jnp.where(low_half, n_left, n_right)

    def finish(i, carry):
        in_first = i < n_first
        turn = jnp.where(in_first, i, i - n_first)
        is_left = in_first == low_half
        block = jnp.where(is_left, z + turn, z - turn)

        @pl.when(is_left)
        def _():
            for index in range(PARTS):
                sum_to_right(block, index).wait_recv()
                total[block, cut(index)] += from_left[block, cut(index)].astype(jnp.float32)

                @pl.when(block > z)
                def _():
                    line_out[block, cut(index)] = total[block, cut(index)].astype(jnp.bfloat16)
                    sum_to_right(block, index).start()

        @pl.when(jnp.logical_not(is_left))
        def _():
            for index in range(PARTS):
                sum_to_left(block, index).wait_recv()
                total[block, cut(index)] += from_right[block, cut(index)].astype(jnp.float32)

                @pl.when(block < z)
                def _():
                    line_out[block, cut(index)] = total[block, cut(index)].astype(jnp.bfloat16)
                    sum_to_left(block, index).start()

        return carry

    lax.fori_loop(0, n_left + n_right, finish, 0)
    y_ref[...] = total[z]

    def drain(block, carry):
        to_partner(block, gath.at[block, k]).wait_send()
        sum_to_partner(block).wait_send()
        for index in range(PARTS):

            @pl.when((block <= z) & has_right)
            def _():
                to_right(block, index, gath.at[block, k, cut(index)]).wait_send()

            @pl.when((block >= z) & has_left)
            def _():
                to_left(block, index, gath.at[block, k, cut(index)]).wait_send()

            @pl.when(block > z)
            def _():
                sum_to_right(block, index).wait_send()

            @pl.when(block < z)
            def _():
                sum_to_left(block, index).wait_send()

        return carry

    lax.fori_loop(0, places, drain, 0)


def tensor_pass(compute, name, ident, x, early_weights, late_weights, ins, out_widths):
    rows, width = x.shape
    places = lax.axis_size("dp") // 2
    vmem = pl.BlockSpec(memory_space=pltpu.VMEM)
    hbm = pl.BlockSpec(memory_space=pl.ANY)
    count = len(early_weights)
    dma = pltpu.SemaphoreType.DMA
    kernel = functools.partial(pass_kernel, compute, count, len(ins), len(out_widths), places)
    return pl.pallas_call(
        kernel,
        name=name,
        out_shape=[
            jax.ShapeDtypeStruct((rows, width), jnp.float32),
            jax.ShapeDtypeStruct((places, 2, rows, width), jnp.bfloat16),
        ]
        + [jax.ShapeDtypeStruct((places, 2 * rows, out), jnp.bfloat16) for out in out_widths],
        in_specs=[vmem] + [hbm] * (2 * count) + [vmem] * len(ins),
        out_specs=[vmem] * (2 + len(out_widths)),
        scratch_shapes=[pltpu.VMEM(weight.shape, weight.dtype) for weight in early_weights]
        + [
            pltpu.VMEM((2, rows, width), jnp.float32),
            pltpu.VMEM((places, rows, width), jnp.bfloat16),
            pltpu.VMEM((places, rows, width), jnp.bfloat16),
            pltpu.VMEM((places, rows, width), jnp.float32),
            pltpu.VMEM((places, rows, width), jnp.bfloat16),
            pltpu.VMEM((places, rows, width), jnp.bfloat16),
            pltpu.VMEM((places, rows, width), jnp.bfloat16),
            dma((count,)),
            dma((places, PARTS)),
            dma((places, PARTS)),
            dma((places,)),
            dma((places, PARTS)),
            dma((places,)),
            dma((places,)),
            dma((places,)),
            dma((places, PARTS)),
            dma((places, PARTS)),
            dma((places, PARTS)),
            dma((places, PARTS)),
        ],
        compiler_params=pltpu.CompilerParams(
            collective_id=ident, has_side_effects=True, vmem_limit_bytes=60 * 1024 * 1024
        ),
    )(x, *early_weights, *late_weights, *ins)


def swapped(size, places):
    pairs = []
    for ctx in range(2):
        for at in range(size):
            z, k = at // 2, at % 2
            pairs.append((ctx * size + at, k * size + 2 * z + ctx))
    return pairs


def regroup(x):
    size = lax.axis_size("dp")
    return lax.ppermute(x, ("ctx", "dp"), swapped(size, size // 2))


def regroup_across(x):
    size = lax.axis_size("dp")
    half = 2 * size
    pairs = swapped(size, size // 2)
    across = [(a, b + half) for a, b in pairs] + [(a + half, b) for a, b in pairs]
    return lax.ppermute(x, ("section", "ctx", "dp"), across)


def exchange(x):
    return lax.ppermute(x, "section", [(0, 1), (1, 0)])


def spread_body(
    tokens, cotangent, segment_ids, w_query, w_keyvalue, w_out, w_up, w_down, ln_gains, ln_biases
):
    section = lax.axis_index("section")
    ctx = lax.axis_index("ctx")
    size = lax.axis_size("dp")
    places = size // 2
    early = section == 0
    width = tokens.shape[3]
    length = segment_ids.shape[2]
    tall = (places * tokens.shape[2] * 2, -1)

    def own_micro(x):
        return lax.dynamic_index_in_dim(x, section, 0, keepdims=False)[0]

    hidden = regroup(own_micro(tokens)).astype(jnp.float32)
    segments = lax.all_gather(own_micro(segment_ids), "dp").reshape(places, 2, length)
    segments = lax.dynamic_index_in_dim(segments, ctx, 1, keepdims=False)
    segs = [segments[:, :, None], segments[:, None, :]]
    scales = lax.all_gather(
        jnp.concatenate([ln_gains[0], ln_biases[0]], axis=0), ("section", "dp")
    ).reshape(2, size, 4, -1)
    scales = scales.transpose(0, 2, 1, 3).reshape(2, 4, width).astype(jnp.float32)
    keyvalue = lax.all_gather(w_keyvalue[0], ("section", "dp"), axis=0, tiled=True)
    keyvalue = keyvalue.reshape(2, width, -1)
    query = lax.all_to_all(w_query[0], "dp", 1, 0, tiled=True)
    out = w_out[0]
    up = lax.all_to_all(w_up[0], "dp", 1, 0, tiled=True)
    down = w_down[0]
    query_far, out_far = exchange(query), exchange(out)
    up_far, down_far = exchange(up), exchange(down)
    attention_weights = [
        ([query, keyvalue[0], out], [query_far, keyvalue[0], out_far]),
        ([query_far, keyvalue[1], out_far], [query, keyvalue[1], out]),
    ]
    ffn_weights = [([up, down], [up_far, down_far]), ([up_far, down_far], [up, down])]
    head_width = query.shape[1]
    unit_width = up.shape[1]

    def forward(layer, hidden):
        normed = layer_norm(hidden, scales[layer, 0], scales[layer, 2]).astype(jnp.bfloat16)
        y, normed_all, q, kv, mixed = tensor_pass(
            attention_forward_at, "attention_forward", 0, normed, *attention_weights[layer], segs,
            [head_width, keyvalue.shape[2], head_width],
        )
        after = hidden + y
        normed_two = layer_norm(after, scales[layer, 1], scales[layer, 3]).astype(jnp.bfloat16)
        y, normed_two_all, up_rows, activated = tensor_pass(
            ffn_forward_at, "ffn_forward", 1, normed_two, *ffn_weights[layer], [],
            [unit_width, unit_width],
        )
        result = (after + y).astype(jnp.bfloat16)
        return result, (hidden, normed_all, q, kv, mixed, after, normed_two_all, up_rows, activated)

    def backward(layer, grad_low, kept):
        hidden, normed_all, q, kv, mixed, after, normed_two_all, up_rows, activated = kept
        y, grad_low_all, grad_upper = tensor_pass(
            ffn_backward_at, "ffn_backward", 2, grad_low, *ffn_weights[layer], [up_rows],
            [unit_width],
        )
        _, norm_back = jax.vjp(layer_norm, after, scales[layer, 1], scales[layer, 3])
        grad_norm, gain_two, bias_two = norm_back(y)
        grad_after = grad_low.astype(jnp.float32) + grad_norm
        y, grad_branch_all, grad_query, grad_kv = tensor_pass(
            attention_backward_at, "attention_backward", 3, grad_after.astype(jnp.bfloat16),
            *attention_weights[layer], segs + [q, kv], [head_width, keyvalue.shape[2]],
        )
        _, norm_back = jax.vjp(layer_norm, hidden, scales[layer, 0], scales[layer, 2])
        grad_norm, gain_one, bias_one = norm_back(y)
        grad_input = (grad_after + grad_norm).astype(jnp.bfloat16)

        def product(left, right):
            return dense_left(left.reshape(tall), right.reshape(tall)).astype(jnp.bfloat16)

        weight_grads = (
            product(activated, grad_low_all),
            product(normed_two_all, grad_upper),
            product(mixed, grad_branch_all),
            product(normed_all, grad_query),
            product(normed_all, grad_kv),
        )
        return grad_input, weight_grads, jnp.stack([gain_one, gain_two, bias_one, bias_two])

    first, kept_first = forward(0, hidden)
    second, kept_second = forward(1, first.astype(jnp.float32))
    grad_low = regroup(own_micro(cotangent))
    grad_second, weights_second, scales_second = backward(1, grad_low, kept_second)
    grad_first, weights_first, scales_first = backward(0, grad_second, kept_first)

    def both_rows(one, two):
        near = regroup(jnp.where(early, one, two))
        far = regroup_across(jnp.where(early, two, one))
        return jnp.stack([jnp.where(early, near, far), jnp.where(early, far, near)])[None, :, None]

    def total(grad):
        return lax.psum(grad, ("section", "ctx"))

    def own(one, two):
        return jnp.where(early, one, two)

    def summed(index):
        return own(total(weights_first[index]), total(weights_second[index]))

    down_grad, up_grad, out_grad, query_grad = [summed(index) for index in range(4)]
    up_grad = lax.all_to_all(up_grad, "dp", 0, 1, tiled=True)
    query_grad = lax.all_to_all(query_grad, "dp", 0, 1, tiled=True)
    keyvalue_grad = own(
        *[
            total(lax.psum_scatter(pair[4], "dp", scatter_dimension=0, tiled=True))
            for pair in (weights_first, weights_second)
        ]
    )
    scale_grads = lax.psum(jnp.stack([scales_first, scales_second]), ("section", "ctx", "dp"))
    scale_grads = lax.dynamic_index_in_dim(scale_grads, section, 0, keepdims=True)
    scale_grads = lax.dynamic_slice_in_dim(
        scale_grads, lax.axis_index("dp") * ln_gains.shape[2], ln_gains.shape[2], axis=2
    )

    def given(grad):
        return grad.astype(jnp.float32)[None]

    return (
        both_rows(first, second),
        both_rows(grad_first, grad_second),
        given(query_grad),
        given(keyvalue_grad),
        given(out_grad),
        given(up_grad),
        given(down_grad),
        scale_grads[:, 0:2],
        scale_grads[:, 2:4],
    )


def from_behind(x, axis, by):
    devices = lax.axis_size(axis)
    pairs = [(i, i + by) for i in range(devices) if 0 <= i + by < devices]
    return lax.ppermute(x, axis, pairs)


def allowed_keys(segments, cycle_place, cycle_size, tok_rows):
    offsets = jnp.arange(tok_rows, dtype=jnp.int32)
    query_pos = cycle_place * tok_rows + offsets
    query_seg = lax.dynamic_slice_in_dim(segments, cycle_place * tok_rows, tok_rows, axis=1)
    blocks = []
    for cycle_step in range(cycle_size):
        source = cycle_place - cycle_step
        key_pos = source * tok_rows + offsets
        key_seg = lax.dynamic_slice_in_dim(
            segments, jnp.maximum(source, 0) * tok_rows, tok_rows, axis=1
        )
        blocks.append(
            (source >= 0)
            & (key_pos[None, None, :] <= query_pos[None, :, None])
            & (key_seg[:, None, :] == query_seg[:, :, None])
        )
    return jnp.concatenate(blocks, axis=2)


def batched(left, right, left_dim, right_dim):
    return lax.dot_general(
        left, right, (((left_dim,), (right_dim,)), ((0,), (0,))), preferred_element_type=jnp.float32
    )


def head_scores(query, keyvalue_all, allowed):
    micro, rows, _ = allowed.shape
    head_rows = query.reshape(micro, rows * HEADS, HEAD)
    scores = batched(head_rows, keyvalue_all[:, :, :HEAD], 2, 2) * HEAD ** (-0.5)
    scores = scores.reshape(micro, rows, HEADS, -1)
    scores = jnp.where(allowed[:, :, None, :], scores, masked_score)
    return (scores.reshape(micro, rows * HEADS, -1), head_rows)


def layer_forward(hidden, segments, weights, micro, cycle_place, cycle_size):
    w_query, w_keyvalue, w_out, w_up, w_down, gains, biases = weights
    rows = hidden.shape[0] // micro
    normed = layer_norm(hidden, gains[0], biases[0]).astype(jnp.bfloat16)
    query = dense(normed, w_query).astype(jnp.bfloat16)
    keyvalue = dense(normed, w_keyvalue).astype(jnp.bfloat16)
    moving = from_behind(keyvalue, "ctx", 1)
    keyvalue_all = jnp.concatenate(
        [keyvalue.reshape(micro, rows, -1), moving.reshape(micro, rows, -1)], axis=1
    )
    allowed = allowed_keys(segments, cycle_place, cycle_size, rows)
    scores, _ = head_scores(query, keyvalue_all, allowed)
    top_score = jnp.max(scores, axis=2, keepdims=True)
    log_total = top_score + jnp.log(jnp.sum(jnp.exp(scores - top_score), axis=2, keepdims=True))
    attn_probs = jnp.exp(scores - log_total).astype(jnp.bfloat16)
    mixed = (
        batched(attn_probs, keyvalue_all[:, :, HEAD:], 2, 1)
        .reshape(micro * rows, HEADS * HEAD)
        .astype(jnp.bfloat16)
    )
    after = hidden + dense(mixed, w_out)
    normed_two = layer_norm(after, gains[1], biases[1]).astype(jnp.bfloat16)
    up_rows = dense(normed_two, w_up)
    activated = jax.nn.gelu(up_rows, approximate=True).astype(jnp.bfloat16)
    result = after + dense(activated, w_down)
    kept = (
        hidden,
        normed,
        query,
        keyvalue_all,
        log_total,
        mixed,
        after,
        normed_two,
        up_rows,
        activated,
    )
    return (result, kept)


def layer_backward(grad_result, kept, segments, weights, micro, cycle_place, cycle_size):
    w_query, w_keyvalue, w_out, w_up, w_down, gains, biases = weights
    hidden, normed, query, keyvalue_all, log_total, mixed, after, normed_two, up_rows, activated = (
        kept
    )
    rows = hidden.shape[0] // micro
    grad_low = grad_result.astype(jnp.bfloat16)
    grad_act = dense_right(grad_low, w_down)
    _, gelu_back = jax.vjp(lambda entries: jax.nn.gelu(entries, approximate=True), up_rows)
    grad_upper = gelu_back(grad_act)[0].astype(jnp.bfloat16)
    _, norm_back_two = jax.vjp(layer_norm, after, gains[1], biases[1])
    grad_after_norm, grad_gain_two, grad_bias_two = norm_back_two(dense_right(grad_upper, w_up))
    grad_after = grad_result + grad_after_norm
    grad_branch = grad_after.astype(jnp.bfloat16)
    grad_mixed = (
        dense_right(grad_branch, w_out).astype(jnp.bfloat16).reshape(micro, rows * HEADS, HEAD)
    )
    allowed = allowed_keys(segments, cycle_place, cycle_size, rows)
    scores, head_rows = head_scores(query, keyvalue_all, allowed)
    attn_probs = jnp.exp(scores - log_total)
    grad_probs = batched(grad_mixed, keyvalue_all[:, :, HEAD:], 2, 2)
    grad_values = batched(attn_probs.astype(jnp.bfloat16), grad_mixed, 1, 1)
    inner = jnp.sum(attn_probs * grad_probs, axis=2, keepdims=True)
    grad_scores = (attn_probs * (grad_probs - inner)).astype(jnp.bfloat16)
    scale_factor = HEAD ** (-0.5)
    grad_queries = (
        (batched(grad_scores, keyvalue_all[:, :, :HEAD], 2, 1) * scale_factor)
        .astype(jnp.bfloat16)
        .reshape(micro * rows, HEADS * HEAD)
    )
    grad_keys = batched(grad_scores, head_rows, 1, 1) * scale_factor
    grad_pieces = jnp.concatenate([grad_keys, grad_values], axis=2)
    carried = grad_pieces[:, (cycle_size - 1) * rows :]
    carried = (
        from_behind(carried.astype(jnp.bfloat16), "ctx", -1).astype(carried.dtype)
        + grad_pieces[:, 0:rows]
    )
    grad_kv = carried.astype(jnp.bfloat16).reshape(micro * rows, -1)
    grad_normed = dense_right(grad_queries, w_query) + dense_right(grad_kv, w_keyvalue)
    _, norm_back_one = jax.vjp(layer_norm, hidden, gains[0], biases[0])
    grad_hidden, grad_gain_one, grad_bias_one = norm_back_one(grad_normed)
    grad_input = grad_after + grad_hidden
    terms = (
        normed,
        grad_queries,
        grad_kv,
        mixed,
        grad_branch,
        normed_two,
        grad_upper,
        activated,
        grad_low,
        jnp.stack([grad_gain_one, grad_gain_two, grad_bias_one, grad_bias_two]),
    )
    return (grad_input, terms)


def body(
    tokens, cotangent, segment_ids, w_query, w_keyvalue, w_out, w_up, w_down, ln_gains, ln_biases
):
    section_index = lax.axis_index("section")
    cycle_place = lax.axis_index("ctx")
    cycle_size = lax.axis_size("ctx")
    micro = tokens.shape[0]
    width = tokens.shape[3]
    early = section_index == 0
    late = section_index == 1
    segments = segment_ids[:, 0]
    own_tokens = tokens[:, 0].reshape(-1, width)
    own_cotangent = cotangent[:, 0].reshape(-1, width)

    def spread(weight):
        half = weight.shape[1] // cycle_size
        part = lax.dynamic_slice_in_dim(weight, cycle_place * half, half, axis=1)
        return lax.all_gather(part, ("dp", "ctx"), axis=1, tiled=True)[0]

    scales = lax.all_gather(
        jnp.concatenate([ln_gains, ln_biases], axis=1), "dp", axis=2, tiled=True
    )[0].astype(jnp.float32)
    weights = (
        spread(w_query),
        lax.all_gather(w_keyvalue, "dp", axis=1, tiled=True)[0],
        spread(w_out),
        spread(w_up),
        spread(w_down),
        scales[0:2],
        scales[2:4],
    )
    result, kept_first = layer_forward(
        own_tokens.astype(jnp.float32), segments, weights, micro, cycle_place, cycle_size
    )
    first_low = result.astype(jnp.bfloat16)
    incoming = from_behind(first_low, "section", 1)
    result, kept_second = layer_forward(
        incoming.astype(jnp.float32), segments, weights, micro, cycle_place, cycle_size
    )
    second_low = result.astype(jnp.bfloat16)
    grad, terms_second = layer_backward(
        own_cotangent.astype(jnp.float32), kept_second, segments, weights, micro, cycle_place,
        cycle_size,
    )
    grad_second = grad.astype(jnp.bfloat16)
    arriving = from_behind(grad_second, "section", -1)
    grad, terms_first = layer_backward(
        arriving.astype(jnp.float32), kept_first, segments, weights, micro, cycle_place, cycle_size
    )
    grad_first = grad.astype(jnp.bfloat16)
    section_rows = jnp.where(early, first_low, second_low)
    grad_rows = jnp.where(early, grad_first, grad_second)
    (
        normed_all,
        grad_queries_all,
        grad_kv_all,
        mixed_all,
        grad_branch_all,
        normed_two_all,
        grad_upper_all,
        activated_all,
        grad_low_all,
        scale_terms,
    ) = [jnp.where(early, one, two) for one, two in zip(terms_first, terms_second)]

    def reduced(left, right):
        part = dense_left(left, right).astype(jnp.bfloat16)
        piece = lax.psum_scatter(part, ("dp", "ctx"), scatter_dimension=0, tiled=True)
        return lax.all_gather(piece, "ctx", axis=0, tiled=True).astype(jnp.float32)[None]

    grad_down = reduced(activated_all, grad_low_all)
    grad_up = reduced(normed_two_all, grad_upper_all)
    grad_out = reduced(mixed_all, grad_branch_all)
    grad_query = reduced(normed_all, grad_queries_all)
    grad_keyvalue = reduced(normed_all, grad_kv_all)
    scale_grads = lax.psum(
        lax.psum_scatter(
            scale_terms.astype(jnp.bfloat16), "dp", scatter_dimension=1, tiled=True
        ),
        "ctx",
    ).astype(jnp.float32)[None]
    local = (1, micro, 1, own_tokens.shape[0] // micro, width)
    return (
        section_rows.reshape(local),
        grad_rows.reshape(local),
        grad_query,
        grad_keyvalue,
        grad_out,
        grad_up,
        grad_down,
        scale_grads[:, 0:2],
        scale_grads[:, 2:4],
    )


def solution(mesh):
    in_specs = (
        P(None, "dp", "ctx", None),
        P(None, "dp", "ctx", None),
        P(None, "dp", None),
        P("section", "dp", None),
        P("section", "dp", None),
        P("section", "dp", None),
        P("section", "dp", None),
        P("section", "dp", None),
        P("section", None, "dp"),
        P("section", None, "dp"),
    )
    out_specs = (
        P("section", None, "dp", "ctx", None),
        P("section", None, "dp", "ctx", None),
        P("section", "dp", None),
        P("section", "dp", None),
        P("section", "dp", None),
        P("section", "dp", None),
        P("section", "dp", None),
        P("section", None, "dp"),
        P("section", None, "dp"),
    )
    step = spread_body if mesh.shape["dp"] == 8 else body
    return jax.shard_map(step, mesh=mesh, in_specs=in_specs, out_specs=out_specs, check_vma=False)
```

```python
import functools
import math

import jax
import jax.numpy as jnp
from jax import lax
from jax.experimental import pallas as pl
from jax.experimental.pallas import tpu as pltpu
from jax.sharding import PartitionSpec as P

HEADS = 16
HEAD = 128


epsilon = 1e-05
masked_score = -1000000000.0


def layer_norm(values_in, gain_row, bias_row):
    mean_row = jnp.mean(values_in, axis=-1, keepdims=True)
    centered = values_in - mean_row
    variance = jnp.mean(centered * centered, axis=-1, keepdims=True)
    return centered * lax.rsqrt(variance + epsilon) * gain_row + bias_row


def dense(left, right):
    return jnp.dot(left, right, preferred_element_type=jnp.float32)


def dense_left(left, right):
    return lax.dot_general(
        left, right, (((0,), (0,)), ((), ())), preferred_element_type=jnp.float32
    )


def dense_right(left, right):
    return lax.dot_general(
        left, right, (((1,), (1,)), ((), ())), preferred_element_type=jnp.float32
    )


MESH = pl.DeviceIdType.MESH
PARTS = 2


def gelu(v):
    inner = math.sqrt(2.0 / math.pi) * (v + 0.044715 * v * v * v)
    return 0.5 * v * (1.0 + jnp.tanh(inner))


def gelu_slope(v):
    scale = math.sqrt(2.0 / math.pi)
    tanh = jnp.tanh(scale * (v + 0.044715 * v * v * v))
    return 0.5 * (1.0 + tanh) + 0.5 * v * (1.0 - tanh * tanh) * scale * (1.0 + 0.134145 * v * v)


def tile_at(step, size):
    return pl.ds(pl.multiple_of(step * size, size), size)


def flat(block):
    return block.reshape(block.shape[0] * block.shape[1], block.shape[2])


def store_part(part, columns, values):
    rows = part.shape[1]
    part[0, :, columns] = values[:rows]
    part[1, :, columns] = values[rows:]


def masked_probs(query, key, mask):
    scores = dense_right(query, key) * HEAD ** (-0.5)
    scores = jnp.where(mask, scores, masked_score)
    scores = jnp.exp(scores - jnp.max(scores, axis=1, keepdims=True))
    return scores / jnp.sum(scores, axis=1, keepdims=True)


def mask_of(seg_col, seg_row, at):
    length = seg_row.shape[2]
    place = lax.broadcasted_iota(jnp.int32, (length, length), 0)
    source = lax.broadcasted_iota(jnp.int32, (length, length), 1)
    return (source <= place) & (seg_col[at] == seg_row[at])


def ffn_forward_at(at, gath, part, weights, ins, outs):
    w_up, w_down = weights
    up_out, act_out = outs
    size = 256

    def up_tile(step, carry):
        columns = tile_at(step, size)
        up_rows = dense(flat(gath[at]), w_up[:, columns])
        up_out[at, :, columns] = up_rows.astype(jnp.bfloat16)
        act_out[at, :, columns] = gelu(up_rows).astype(jnp.bfloat16)
        return carry

    lax.fori_loop(0, w_up.shape[1] // size, up_tile, 0)

    def down_tile(step, carry):
        columns = tile_at(step, size)
        store_part(part, columns, dense(act_out[at], w_down[:, columns]))
        return carry

    lax.fori_loop(0, w_down.shape[1] // size, down_tile, 0)


def ffn_backward_at(at, gath, part, weights, ins, outs):
    w_up, w_down = weights
    (up_in,) = ins
    (upper_out,) = outs
    size = 256

    def act_tile(step, carry):
        columns = tile_at(step, size)
        grad_act = dense_right(flat(gath[at]), w_down[columns, :])
        slope = gelu_slope(up_in[at, :, columns].astype(jnp.float32))
        upper_out[at, :, columns] = (grad_act * slope).astype(jnp.bfloat16)
        return carry

    lax.fori_loop(0, w_down.shape[0] // size, act_tile, 0)

    def back_tile(step, carry):
        columns = tile_at(step, size)
        store_part(part, columns, dense_right(upper_out[at], w_up[columns, :]))
        return carry

    lax.fori_loop(0, w_up.shape[0] // size, back_tile, 0)


def attention_forward_at(at, gath, part, weights, ins, outs):
    w_query, w_keyvalue, w_out = weights
    seg_col, seg_row = ins
    query_out, keyvalue_out, mixed_out = outs
    size = 256
    rows = flat(gath[at])
    query_out[at] = dense(rows, w_query[...]).astype(jnp.bfloat16)
    keyvalue_out[at] = dense(rows, w_keyvalue[...]).astype(jnp.bfloat16)
    mask = mask_of(seg_col, seg_row, at)
    for head in range(w_query.shape[1] // HEAD):
        own = slice(head * HEAD, (head + 1) * HEAD)
        probs = masked_probs(query_out[at, :, own], keyvalue_out[at, :, :HEAD], mask)
        mixed = dense(probs.astype(jnp.bfloat16), keyvalue_out[at, :, HEAD:])
        mixed_out[at, :, own] = mixed.astype(jnp.bfloat16)

    def out_tile(step, carry):
        columns = tile_at(step, size)
        store_part(part, columns, dense(mixed_out[at], w_out[:, columns]))
        return carry

    lax.fori_loop(0, w_out.shape[1] // size, out_tile, 0)


def attention_backward_at(at, gath, part, weights, ins, outs):
    w_query, w_keyvalue, w_out = weights
    seg_col, seg_row, query_in, keyvalue_in = ins
    query_out, keyvalue_out = outs
    size = 256
    scale = HEAD ** (-0.5)
    grad_mixed = dense_right(flat(gath[at]), w_out[...]).astype(jnp.bfloat16)
    key = keyvalue_in[at, :, :HEAD]
    value = keyvalue_in[at, :, HEAD:]
    mask = mask_of(seg_col, seg_row, at)
    grad_key = jnp.zeros(key.shape, jnp.float32)
    grad_value = jnp.zeros(value.shape, jnp.float32)
    for head in range(w_query.shape[1] // HEAD):
        own = slice(head * HEAD, (head + 1) * HEAD)
        query = query_in[at, :, own]
        branch = grad_mixed[:, own]
        probs = masked_probs(query, key, mask)
        grad_probs = dense_right(branch, value)
        inner = jnp.sum(probs * grad_probs, axis=1, keepdims=True)
        grad_scores = (probs * (grad_probs - inner)).astype(jnp.bfloat16)
        query_out[at, :, own] = (dense(grad_scores, key) * scale).astype(jnp.bfloat16)
        grad_key = grad_key + dense_left(grad_scores, query)
        grad_value = grad_value + dense_left(probs.astype(jnp.bfloat16), branch)
    keyvalue_out[at, :, :HEAD] = (grad_key * scale).astype(jnp.bfloat16)
    keyvalue_out[at, :, HEAD:] = grad_value.astype(jnp.bfloat16)

    def back_tile(step, carry):
        columns = tile_at(step, size)
        store_part(
            part,
            columns,
            dense_right(query_out[at], w_query[columns, :])
            + dense_right(keyvalue_out[at], w_keyvalue[columns, :]),
        )
        return carry

    lax.fori_loop(0, w_query.shape[0] // size, back_tile, 0)


def pass_kernel(compute, n_weights, n_ins, n_outs, places, *refs):
    refs = list(refs)
    take = lambda count: [refs.pop(0) for _ in range(count)]
    (x_ref,) = take(1)
    early_weights = take(n_weights)
    late_weights = take(n_weights)
    ins = take(n_ins)
    y_ref, gath = take(2)
    outs = take(n_outs)
    weights = take(n_weights)
    part, partner_out, partner_in, total, line_out, from_left, from_right = take(7)
    (
        weight_sem, gather_right, gather_left, gather_partner, gather_line_in, gather_partner_in,
        partner_send, partner_recv, right_send, right_recv, left_send, left_recv,
    ) = take(12)

    section = lax.axis_index("section")
    me = lax.axis_index("dp")
    z = me // 2
    k = me % 2
    last = places - 1
    rows = x_ref.shape[0]
    size = rows // PARTS
    right = {"dp": me + 2}
    left = {"dp": me - 2}
    partner = {"dp": 2 * z + 1 - k}
    has_left = z > 0
    has_right = z < last

    barrier = pltpu.get_barrier_semaphore()
    pl.semaphore_signal(barrier, inc=1, device_id=partner, device_id_type=MESH)

    @pl.when(has_left)
    def _():
        pl.semaphore_signal(barrier, inc=1, device_id=left, device_id_type=MESH)

    @pl.when(has_right)
    def _():
        pl.semaphore_signal(barrier, inc=1, device_id=right, device_id_type=MESH)

    for index in range(n_weights):

        @pl.when(section == 0)
        def _():
            pltpu.make_async_copy(early_weights[index], weights[index], weight_sem.at[index]).start()

        @pl.when(section != 0)
        def _():
            pltpu.make_async_copy(late_weights[index], weights[index], weight_sem.at[index]).start()

    peers = 1 + jnp.where(has_left, 1, 0) + jnp.where(has_right, 1, 0)
    pl.semaphore_wait(barrier, peers)

    def cut(index):
        return pl.ds(index * size, size)

    def to_right(block, index, source):
        return pltpu.make_async_remote_copy(
            source, gath.at[block, k, cut(index)], gather_right.at[block, index],
            gather_line_in.at[block, index], device_id=right, device_id_type=MESH,
        )

    def to_left(block, index, source):
        return pltpu.make_async_remote_copy(
            source, gath.at[block, k, cut(index)], gather_left.at[block, index],
            gather_line_in.at[block, index], device_id=left, device_id_type=MESH,
        )

    def to_partner(block, source):
        return pltpu.make_async_remote_copy(
            source, gath.at[block, k], gather_partner.at[block],
            gather_partner_in.at[block], device_id=partner, device_id_type=MESH,
        )

    def sum_to_partner(block):
        return pltpu.make_async_remote_copy(
            partner_out.at[block], partner_in.at[block], partner_send.at[block],
            partner_recv.at[block], device_id=partner, device_id_type=MESH,
        )

    def sum_to_right(block, index):
        return pltpu.make_async_remote_copy(
            line_out.at[block, cut(index)], from_left.at[block, cut(index)],
            right_send.at[block, index], right_recv.at[block, index],
            device_id=right, device_id_type=MESH,
        )

    def sum_to_left(block, index):
        return pltpu.make_async_remote_copy(
            line_out.at[block, cut(index)], from_right.at[block, cut(index)],
            left_send.at[block, index], left_recv.at[block, index],
            device_id=left, device_id_type=MESH,
        )

    for index in range(PARTS):

        @pl.when(has_right)
        def _():
            to_right(z, index, x_ref.at[cut(index)]).start()

        @pl.when(has_left)
        def _():
            to_left(z, index, x_ref.at[cut(index)]).start()

    to_partner(z, x_ref).start()
    gath[z, k] = x_ref[...]

    at_end = (z == 0) | (z == last)
    low_half = z < places // 2

    def step(i, carry):
        inner_block = jnp.where(i == 0, 1, jnp.where(i == 1, 0, i))
        low_block = jnp.where(z == 0, i, inner_block)
        high_block = last - jnp.where(z == last, i, inner_block)
        block = jnp.where(low_half, low_block, high_block)
        wave = jnp.where(at_end, i, jnp.where(i == 1, 1, jnp.where(i == 3, 2, 0)))
        from_low = z - wave
        from_high = z + wave

        @pl.when((wave > 0) & (from_low >= 0))
        def _():
            for index in range(PARTS):
                to_right(from_low, index, gath.at[from_low, k, cut(index)]).wait_recv()

                @pl.when(has_right)
                def _():
                    to_right(from_low, index, gath.at[from_low, k, cut(index)]).start()

            to_partner(from_low, gath.at[from_low, k]).start()

        @pl.when((wave > 0) & (from_high <= last))
        def _():
            for index in range(PARTS):
                to_left(from_high, index, gath.at[from_high, k, cut(index)]).wait_recv()

                @pl.when(has_left)
                def _():
                    to_left(from_high, index, gath.at[from_high, k, cut(index)]).start()

            to_partner(from_high, gath.at[from_high, k]).start()

        pltpu.make_async_remote_copy(
            gath.at[block, 1 - k], gath.at[block, 1 - k], gather_partner.at[block],
            gather_partner_in.at[block], device_id=partner, device_id_type=MESH,
        ).wait_recv()

        @pl.when(i == 0)
        def _():
            for index in range(n_weights):
                pltpu.make_async_copy(
                    early_weights[index], weights[index], weight_sem.at[index]
                ).wait()

        compute(block, gath, part, weights, ins, outs)
        partner_out[block] = part[1 - k].astype(jnp.bfloat16)
        sum_to_partner(block).start()
        sum_to_partner(block).wait_recv()
        total[block] = part[k] + partner_in[block].astype(jnp.float32)

        @pl.when((z == 0) & (block > 0))
        def _():
            line_out[block] = total[block].astype(jnp.bfloat16)
            for index in range(PARTS):
                sum_to_right(block, index).start()

        @pl.when((z == last) & (block < last))
        def _():
            line_out[block] = total[block].astype(jnp.bfloat16)
            for index in range(PARTS):
                sum_to_left(block, index).start()

        return carry

    lax.fori_loop(0, places, step, 0)

    n_left = jnp.where(has_left, places - z, 0)
    n_right = jnp.where(has_right, z + 1, 0)
    n_first = jnp.where(low_half, n_left, n_right)

    def finish(i, carry):
        in_first = i < n_first
        turn = jnp.where(in_first, i, i - n_first)
        is_left = in_first == low_half
        block = jnp.where(is_left, z + turn, z - turn)

        @pl.when(is_left)
        def _():
            for index in range(PARTS):
                sum_to_right(block, index).wait_recv()
                total[block, cut(index)] += from_left[block, cut(index)].astype(jnp.float32)

                @pl.when(block > z)
                def _():
                    line_out[block, cut(index)] = total[block, cut(index)].astype(jnp.bfloat16)
                    sum_to_right(block, index).start()

        @pl.when(jnp.logical_not(is_left))
        def _():
            for index in range(PARTS):
                sum_to_left(block, index).wait_recv()
                total[block, cut(index)] += from_right[block, cut(index)].astype(jnp.float32)

                @pl.when(block < z)
                def _():
                    line_out[block, cut(index)] = total[block, cut(index)].astype(jnp.bfloat16)
                    sum_to_left(block, index).start()

        return carry

    lax.fori_loop(0, n_left + n_right, finish, 0)
    y_ref[...] = total[z]

    def drain(block, carry):
        to_partner(block, gath.at[block, k]).wait_send()
        sum_to_partner(block).wait_send()
        for index in range(PARTS):

            @pl.when((block <= z) & has_right)
            def _():
                to_right(block, index, gath.at[block, k, cut(index)]).wait_send()

            @pl.when((block >= z) & has_left)
            def _():
                to_left(block, index, gath.at[block, k, cut(index)]).wait_send()

            @pl.when(block > z)
            def _():
                sum_to_right(block, index).wait_send()

            @pl.when(block < z)
            def _():
                sum_to_left(block, index).wait_send()

        return carry

    lax.fori_loop(0, places, drain, 0)


def tensor_pass(compute, name, ident, x, early_weights, late_weights, ins, out_widths):
    rows, width = x.shape
    places = lax.axis_size("dp") // 2
    vmem = pl.BlockSpec(memory_space=pltpu.VMEM)
    hbm = pl.BlockSpec(memory_space=pl.ANY)
    count = len(early_weights)
    dma = pltpu.SemaphoreType.DMA
    kernel = functools.partial(pass_kernel, compute, count, len(ins), len(out_widths), places)
    return pl.pallas_call(
        kernel,
        name=name,
        out_shape=[
            jax.ShapeDtypeStruct((rows, width), jnp.float32),
            jax.ShapeDtypeStruct((places, 2, rows, width), jnp.bfloat16),
        ]
        + [jax.ShapeDtypeStruct((places, 2 * rows, out), jnp.bfloat16) for out in out_widths],
        in_specs=[vmem] + [hbm] * (2 * count) + [vmem] * len(ins),
        out_specs=[vmem] * (2 + len(out_widths)),
        scratch_shapes=[pltpu.VMEM(weight.shape, weight.dtype) for weight in early_weights]
        + [
            pltpu.VMEM((2, rows, width), jnp.float32),
            pltpu.VMEM((places, rows, width), jnp.bfloat16),
            pltpu.VMEM((places, rows, width), jnp.bfloat16),
            pltpu.VMEM((places, rows, width), jnp.float32),
            pltpu.VMEM((places, rows, width), jnp.bfloat16),
            pltpu.VMEM((places, rows, width), jnp.bfloat16),
            pltpu.VMEM((places, rows, width), jnp.bfloat16),
            dma((count,)),
            dma((places, PARTS)),
            dma((places, PARTS)),
            dma((places,)),
            dma((places, PARTS)),
            dma((places,)),
            dma((places,)),
            dma((places,)),
            dma((places, PARTS)),
            dma((places, PARTS)),
            dma((places, PARTS)),
            dma((places, PARTS)),
        ],
        cost_estimate=pl.CostEstimate(
            flops=60_000_000_000, bytes_accessed=20_000_000, transcendentals=0
        ),
        compiler_params=pltpu.CompilerParams(
            collective_id=ident, has_side_effects=True, vmem_limit_bytes=60 * 1024 * 1024
        ),
    )(x, *early_weights, *late_weights, *ins)


def distribute_kernel(
    places, query, keyvalue, out, up, down,
    query_own, keyvalue_own, up_own, query_far, keyvalue_far, out_far, up_far, down_far,
    local_sem, query_send, query_recv, keyvalue_send, keyvalue_recv, up_send, up_recv,
    across_send, across_recv, over_send, over_recv,
):
    section = lax.axis_index("section")
    ctx = lax.axis_index("ctx")
    me = lax.axis_index("dp")
    z = me // 2
    k = me % 2
    last = places - 1
    rows = query.shape[0]
    half = rows // 2
    head_width = query_own.shape[1]
    unit_width = up_own.shape[1]
    across = {"section": 1 - section}
    over = {"ctx": 1 - ctx}

    def peers(act):
        act(2 * z + 1 - k)
        for away in range(1, places):

            @pl.when(z + away <= last)
            def _():
                act(2 * (z + away) + k)
                act(2 * (z + away) + 1 - k)

            @pl.when(z - away >= 0)
            def _():
                act(2 * (z - away) + k)
                act(2 * (z - away) + 1 - k)

    def remote(source, target, send, recv, device):
        return pltpu.make_async_remote_copy(
            source, target, send, recv, device_id=device, device_id_type=MESH
        )

    def piece(owner, part):
        which = jnp.where(part == 0, ctx, 1 - ctx)
        return pl.ds(pl.multiple_of(owner * rows + which * half, half), half)

    def query_copy(source, to):
        return remote(
            query.at[:, tile_at(to, head_width)], query_own.at[tile_at(source, rows)],
            query_send.at[to], query_recv.at[source], {"dp": to},
        )

    def keyvalue_copy(source, to):
        return remote(
            keyvalue, keyvalue_own.at[tile_at(source, rows)],
            keyvalue_send.at[to], keyvalue_recv.at[source], {"dp": to},
        )

    def up_copy(source, to, part):
        which = jnp.where(part == 0, ctx, 1 - ctx)
        return remote(
            up.at[tile_at(which, half), tile_at(to, unit_width)],
            up_own.at[piece(source, part)],
            up_send.at[to, part], up_recv.at[source, part], {"dp": to},
        )

    barrier = pltpu.get_barrier_semaphore()

    def greet(to):
        pl.semaphore_signal(barrier, inc=1, device_id={"dp": to}, device_id_type=MESH)

    peers(greet)
    pl.semaphore_signal(barrier, inc=1, device_id=across, device_id_type=MESH)
    pl.semaphore_signal(barrier, inc=1, device_id=over, device_id_type=MESH)
    pl.semaphore_wait(barrier, 2 * places + 1)

    local = [
        pltpu.make_async_copy(
            query.at[:, tile_at(me, head_width)], query_own.at[tile_at(me, rows)], local_sem.at[0]
        ),
        pltpu.make_async_copy(keyvalue, keyvalue_own.at[tile_at(me, rows)], local_sem.at[1]),
        pltpu.make_async_copy(
            up.at[:, tile_at(me, unit_width)], up_own.at[tile_at(me, rows)], local_sem.at[2]
        ),
    ]
    for copy in local:
        copy.start()
    peers(lambda to: query_copy(me, to).start())
    peers(lambda to: keyvalue_copy(me, to).start())
    peers(lambda to: up_copy(me, to, 0).start())

    out_half = tile_at(ctx, out.shape[0] // 2)
    quarter = down.shape[0] // 4
    flows = [(out, out_far, out_half)] + [
        (down, down_far, pl.ds(pl.multiple_of((2 * ctx + index) * quarter, quarter), quarter))
        for index in range(2)
    ]

    def flow_across(slot):
        source, target, at = flows[slot]
        return remote(
            source.at[at], target.at[at], across_send.at[slot], across_recv.at[slot], across
        )

    def flow_over(slot):
        source, target, at = flows[slot]
        return remote(target.at[at], target.at[at], over_send.at[slot], over_recv.at[slot], over)

    first_slot = len(flows)
    kinds = [(query_own, query_far), (keyvalue_own, keyvalue_far), (up_own, up_far)]

    def block_across(kind, owner):
        own, far = kinds[kind]
        slot = first_slot + kind * 2 * places + owner
        at = piece(owner, 0)
        return remote(own.at[at], far.at[at], across_send.at[slot], across_recv.at[slot], across)

    def block_over(kind, owner):
        own, far = kinds[kind]
        slot = first_slot + kind * 2 * places + owner
        at = piece(owner, 0)
        return remote(far.at[at], far.at[at], over_send.at[slot], over_recv.at[slot], over)

    flow_across(0).start()

    local[0].wait()
    local[1].wait()
    block_across(0, me).start()
    block_across(1, me).start()

    def pass_small(source):
        query_copy(source, me).wait_recv()
        block_across(0, source).start()
        keyvalue_copy(source, me).wait_recv()
        block_across(1, source).start()

    peers(pass_small)
    peers(lambda to: up_copy(me, to, 1).start())
    flow_across(1).start()
    flow_across(0).wait_recv()
    flow_over(0).start()
    local[2].wait()
    block_across(2, me).start()

    def pass_up(source):
        up_copy(source, me, 0).wait_recv()
        block_across(2, source).start()

    peers(pass_up)
    flow_across(2).start()

    def over_small(owner, carry):
        block_across(0, owner).wait_recv()
        block_over(0, owner).start()
        block_across(1, owner).wait_recv()
        block_over(1, owner).start()
        return carry

    lax.fori_loop(0, 2 * places, over_small, 0)
    flow_across(1).wait_recv()
    flow_over(1).start()

    def over_up(owner, carry):
        block_across(2, owner).wait_recv()
        block_over(2, owner).start()
        return carry

    lax.fori_loop(0, 2 * places, over_up, 0)
    flow_across(2).wait_recv()
    flow_over(2).start()

    peers(lambda source: up_copy(source, me, 1).wait_recv())

    def over_wait(slot_owner, carry):
        for kind in range(3):
            block_over_in(kind, slot_owner).wait_recv()
            block_across(kind, slot_owner).wait_send()
            block_over(kind, slot_owner).wait_send()
        return carry

    def block_over_in(kind, owner):
        own, far = kinds[kind]
        slot = first_slot + kind * 2 * places + owner
        at = piece(owner, 1)
        return remote(far.at[at], far.at[at], over_send.at[slot], over_recv.at[slot], over)

    lax.fori_loop(0, 2 * places, over_wait, 0)
    for slot in range(first_slot):
        flow_over(slot).wait_recv()
        flow_across(slot).wait_send()
        flow_over(slot).wait_send()

    def sent(to):
        query_copy(me, to).wait_send()
        keyvalue_copy(me, to).wait_send()
        up_copy(me, to, 0).wait_send()
        up_copy(me, to, 1).wait_send()

    peers(sent)


def distribute(query, keyvalue, out, up, down):
    size = lax.axis_size("dp")
    places = size // 2
    hbm = pl.BlockSpec(memory_space=pl.ANY)
    dma = pltpu.SemaphoreType.DMA
    rows = query.shape[0] * size
    turned = [(rows, query.shape[1] // size), (rows, keyvalue.shape[1]), (rows, up.shape[1] // size)]
    shapes = turned + turned[:2] + [out.shape, turned[2], down.shape]
    slots = 3 + 3 * size
    return pl.pallas_call(
        functools.partial(distribute_kernel, places),
        name="distribute",
        out_shape=[jax.ShapeDtypeStruct(shape, jnp.bfloat16) for shape in shapes],
        in_specs=[hbm] * 5,
        out_specs=[hbm] * 8,
        scratch_shapes=[dma((3,))]
        + [dma((size,))] * 4
        + [dma((size, 2))] * 2
        + [dma((slots,))] * 4,
        compiler_params=pltpu.CompilerParams(collective_id=4, has_side_effects=True),
    )(query, keyvalue, out, up, down)


def swapped(size):
    pairs = []
    for ctx in range(2):
        for at in range(size):
            z, k = at // 2, at % 2
            pairs.append((ctx * size + at, k * size + 2 * z + ctx))
    return pairs


def regroup(x):
    return lax.ppermute(x, ("ctx", "dp"), swapped(lax.axis_size("dp")))


def regroup_across(x):
    size = lax.axis_size("dp")
    half = 2 * size
    pairs = swapped(size)
    across = [(a, b + half) for a, b in pairs] + [(a + half, b) for a, b in pairs]
    return lax.ppermute(x, ("section", "ctx", "dp"), across)


def halves_summed(layer, grad):
    ctx = lax.axis_index("ctx")
    half = grad.shape[-2] // 2
    mine = lax.dynamic_slice_in_dim(grad, ctx * half, half, axis=-2)
    others = lax.dynamic_slice_in_dim(grad, (1 - ctx) * half, half, axis=-2)
    mine = mine + lax.ppermute(others, "ctx", [(0, 1), (1, 0)])
    return mine + lax.ppermute(mine, "section", [(1 - layer, layer)])


def both_halves(half):
    ctx = lax.axis_index("ctx")
    other = lax.ppermute(half, "ctx", [(0, 1), (1, 0)])
    first = jnp.where(ctx == 0, half, other)
    second = jnp.where(ctx == 0, other, half)
    return jnp.concatenate([first, second], axis=-2)


def spread_body(
    tokens, cotangent, segment_ids, w_query, w_keyvalue, w_out, w_up, w_down, ln_gains, ln_biases
):
    section = lax.axis_index("section")
    ctx = lax.axis_index("ctx")
    size = lax.axis_size("dp")
    places = size // 2
    early = section == 0
    width = tokens.shape[3]
    length = segment_ids.shape[2]
    tall = (places * tokens.shape[2] * 2, -1)

    def own_micro(x):
        return lax.dynamic_index_in_dim(x, section, 0, keepdims=False)[0]

    hidden = regroup(own_micro(tokens)).astype(jnp.float32)
    segments = lax.all_gather(own_micro(segment_ids), "dp").reshape(places, 2, length)
    segments = lax.dynamic_index_in_dim(segments, ctx, 1, keepdims=False)
    segs = [segments[:, :, None], segments[:, None, :]]
    scales = lax.all_gather(
        jnp.concatenate([ln_gains[0], ln_biases[0]], axis=0), ("section", "dp")
    ).reshape(2, size, 4, -1)
    scales = scales.transpose(0, 2, 1, 3).reshape(2, 4, width).astype(jnp.float32)
    out, down = w_out[0], w_down[0]
    query, keyvalue, up, query_far, keyvalue_far, out_far, up_far, down_far = distribute(
        w_query[0], w_keyvalue[0], out, w_up[0], down
    )
    attention_near, attention_far = [query, keyvalue, out], [query_far, keyvalue_far, out_far]
    attention_weights = [(attention_near, attention_far), (attention_far, attention_near)]
    ffn_weights = [([up, down], [up_far, down_far]), ([up_far, down_far], [up, down])]
    head_width = query.shape[1]
    unit_width = up.shape[1]

    def forward(layer, hidden):
        normed = layer_norm(hidden, scales[layer, 0], scales[layer, 2]).astype(jnp.bfloat16)
        y, normed_all, q, kv, mixed = tensor_pass(
            attention_forward_at, "attention_forward", 0, normed, *attention_weights[layer], segs,
            [head_width, keyvalue.shape[1], head_width],
        )
        after = hidden + y
        normed_two = layer_norm(after, scales[layer, 1], scales[layer, 3]).astype(jnp.bfloat16)
        y, normed_two_all, up_rows, activated = tensor_pass(
            ffn_forward_at, "ffn_forward", 1, normed_two, *ffn_weights[layer], [],
            [unit_width, unit_width],
        )
        result = (after + y).astype(jnp.bfloat16)
        return result, (hidden, normed_all, q, kv, mixed, after, normed_two_all, up_rows, activated)

    def product(left, right):
        return dense_left(left.reshape(tall), right.reshape(tall)).astype(jnp.bfloat16)

    def rows_of_all(grad):
        return grad.reshape(size, grad.shape[0] // size, grad.shape[1])

    def backward(layer, grad_low, kept):
        hidden, normed_all, q, kv, mixed, after, normed_two_all, up_rows, activated = kept
        y, grad_low_all, grad_upper = tensor_pass(
            ffn_backward_at, "ffn_backward", 2, grad_low, *ffn_weights[layer], [up_rows],
            [unit_width],
        )
        up_grad = halves_summed(layer, rows_of_all(product(normed_two_all, grad_upper)))
        down_grad = halves_summed(layer, product(activated, grad_low_all))
        _, norm_back = jax.vjp(layer_norm, after, scales[layer, 1], scales[layer, 3])
        grad_norm, gain_two, bias_two = norm_back(y)
        grad_after = grad_low.astype(jnp.float32) + grad_norm
        y, grad_branch_all, grad_query, grad_kv = tensor_pass(
            attention_backward_at, "attention_backward", 3, grad_after.astype(jnp.bfloat16),
            *attention_weights[layer], segs + [q, kv], [head_width, keyvalue.shape[1]],
        )
        query_grad = halves_summed(layer, rows_of_all(product(normed_all, grad_query)))
        out_grad = halves_summed(layer, product(mixed, grad_branch_all))
        keyvalue_grad = product(normed_all, grad_kv)
        _, norm_back = jax.vjp(layer_norm, hidden, scales[layer, 0], scales[layer, 2])
        grad_norm, gain_one, bias_one = norm_back(y)
        grad_input = (grad_after + grad_norm).astype(jnp.bfloat16)
        weight_grads = (query_grad, keyvalue_grad, out_grad, up_grad, down_grad)
        return grad_input, weight_grads, jnp.stack([gain_one, gain_two, bias_one, bias_two])

    first, kept_first = forward(0, hidden)
    second, kept_second = forward(1, first.astype(jnp.float32))
    grad_low = regroup(own_micro(cotangent))
    grad_second, weights_second, scales_second = backward(1, grad_low, kept_second)
    grad_first, weights_first, scales_first = backward(0, grad_second, kept_first)

    def both_rows(one, two):
        near = regroup(jnp.where(early, one, two))
        far = regroup_across(jnp.where(early, two, one))
        return jnp.stack([jnp.where(early, near, far), jnp.where(early, far, near)])[None, :, None]

    query_grad, _, out_grad, up_grad, down_grad = [
        jnp.where(early, one, two) for one, two in zip(weights_first, weights_second)
    ]

    def turned(grad):
        grad = lax.all_to_all(grad, "dp", 0, 0)
        return grad.transpose(1, 0, 2).reshape(grad.shape[1], size * grad.shape[2])

    keyvalue_grad = lax.psum_scatter(
        jnp.stack([weights_first[1], weights_second[1]]), "dp", scatter_dimension=1, tiled=True
    )
    keyvalue_grad = lax.psum(keyvalue_grad, ("section", "ctx"))
    keyvalue_grad = lax.dynamic_index_in_dim(keyvalue_grad, section, 0, keepdims=False)
    scale_grads = lax.psum_scatter(
        jnp.stack([scales_first, scales_second]), "dp", scatter_dimension=2, tiled=True
    )
    scale_grads = lax.psum(scale_grads, ("section", "ctx"))
    scale_grads = lax.dynamic_index_in_dim(scale_grads, section, 0, keepdims=True)

    def given(grad):
        return grad.astype(jnp.float32)[None]

    return (
        both_rows(first, second),
        both_rows(grad_first, grad_second),
        given(both_halves(turned(query_grad))),
        given(keyvalue_grad),
        given(both_halves(out_grad)),
        given(both_halves(turned(up_grad))),
        given(both_halves(down_grad)),
        scale_grads[:, 0:2],
        scale_grads[:, 2:4],
    )


def from_behind(x, axis, by):
    devices = lax.axis_size(axis)
    pairs = [(i, i + by) for i in range(devices) if 0 <= i + by < devices]
    return lax.ppermute(x, axis, pairs)


def allowed_keys(segments, cycle_place, cycle_size, tok_rows):
    offsets = jnp.arange(tok_rows, dtype=jnp.int32)
    query_pos = cycle_place * tok_rows + offsets
    query_seg = lax.dynamic_slice_in_dim(segments, cycle_place * tok_rows, tok_rows, axis=1)
    blocks = []
    for cycle_step in range(cycle_size):
        source = cycle_place - cycle_step
        key_pos = source * tok_rows + offsets
        key_seg = lax.dynamic_slice_in_dim(
            segments, jnp.maximum(source, 0) * tok_rows, tok_rows, axis=1
        )
        blocks.append(
            (source >= 0)
            & (key_pos[None, None, :] <= query_pos[None, :, None])
            & (key_seg[:, None, :] == query_seg[:, :, None])
        )
    return jnp.concatenate(blocks, axis=2)


def batched(left, right, left_dim, right_dim):
    return lax.dot_general(
        left, right, (((left_dim,), (right_dim,)), ((0,), (0,))), preferred_element_type=jnp.float32
    )


def head_scores(query, keyvalue_all, allowed):
    micro, rows, _ = allowed.shape
    head_rows = query.reshape(micro, rows * HEADS, HEAD)
    scores = batched(head_rows, keyvalue_all[:, :, :HEAD], 2, 2) * HEAD ** (-0.5)
    scores = scores.reshape(micro, rows, HEADS, -1)
    scores = jnp.where(allowed[:, :, None, :], scores, masked_score)
    return (scores.reshape(micro, rows * HEADS, -1), head_rows)


def layer_forward(hidden, segments, weights, micro, cycle_place, cycle_size):
    w_query, w_keyvalue, w_out, w_up, w_down, gains, biases = weights
    rows = hidden.shape[0] // micro
    normed = layer_norm(hidden, gains[0], biases[0]).astype(jnp.bfloat16)
    query = dense(normed, w_query).astype(jnp.bfloat16)
    keyvalue = dense(normed, w_keyvalue).astype(jnp.bfloat16)
    moving = from_behind(keyvalue, "ctx", 1)
    keyvalue_all = jnp.concatenate(
        [keyvalue.reshape(micro, rows, -1), moving.reshape(micro, rows, -1)], axis=1
    )
    allowed = allowed_keys(segments, cycle_place, cycle_size, rows)
    scores, _ = head_scores(query, keyvalue_all, allowed)
    top_score = jnp.max(scores, axis=2, keepdims=True)
    log_total = top_score + jnp.log(jnp.sum(jnp.exp(scores - top_score), axis=2, keepdims=True))
    attn_probs = jnp.exp(scores - log_total).astype(jnp.bfloat16)
    mixed = (
        batched(attn_probs, keyvalue_all[:, :, HEAD:], 2, 1)
        .reshape(micro * rows, HEADS * HEAD)
        .astype(jnp.bfloat16)
    )
    after = hidden + dense(mixed, w_out)
    normed_two = layer_norm(after, gains[1], biases[1]).astype(jnp.bfloat16)
    up_rows = dense(normed_two, w_up)
    activated = jax.nn.gelu(up_rows, approximate=True).astype(jnp.bfloat16)
    result = after + dense(activated, w_down)
    kept = (
        hidden,
        normed,
        query,
        keyvalue_all,
        log_total,
        mixed,
        after,
        normed_two,
        up_rows,
        activated,
    )
    return (result, kept)


def layer_backward(grad_result, kept, segments, weights, micro, cycle_place, cycle_size):
    w_query, w_keyvalue, w_out, w_up, w_down, gains, biases = weights
    hidden, normed, query, keyvalue_all, log_total, mixed, after, normed_two, up_rows, activated = (
        kept
    )
    rows = hidden.shape[0] // micro
    grad_low = grad_result.astype(jnp.bfloat16)
    grad_act = dense_right(grad_low, w_down)
    _, gelu_back = jax.vjp(lambda entries: jax.nn.gelu(entries, approximate=True), up_rows)
    grad_upper = gelu_back(grad_act)[0].astype(jnp.bfloat16)
    _, norm_back_two = jax.vjp(layer_norm, after, gains[1], biases[1])
    grad_after_norm, grad_gain_two, grad_bias_two = norm_back_two(dense_right(grad_upper, w_up))
    grad_after = grad_result + grad_after_norm
    grad_branch = grad_after.astype(jnp.bfloat16)
    grad_mixed = (
        dense_right(grad_branch, w_out).astype(jnp.bfloat16).reshape(micro, rows * HEADS, HEAD)
    )
    allowed = allowed_keys(segments, cycle_place, cycle_size, rows)
    scores, head_rows = head_scores(query, keyvalue_all, allowed)
    attn_probs = jnp.exp(scores - log_total)
    grad_probs = batched(grad_mixed, keyvalue_all[:, :, HEAD:], 2, 2)
    grad_values = batched(attn_probs.astype(jnp.bfloat16), grad_mixed, 1, 1)
    inner = jnp.sum(attn_probs * grad_probs, axis=2, keepdims=True)
    grad_scores = (attn_probs * (grad_probs - inner)).astype(jnp.bfloat16)
    scale_factor = HEAD ** (-0.5)
    grad_queries = (
        (batched(grad_scores, keyvalue_all[:, :, :HEAD], 2, 1) * scale_factor)
        .astype(jnp.bfloat16)
        .reshape(micro * rows, HEADS * HEAD)
    )
    grad_keys = batched(grad_scores, head_rows, 1, 1) * scale_factor
    grad_pieces = jnp.concatenate([grad_keys, grad_values], axis=2)
    carried = grad_pieces[:, (cycle_size - 1) * rows :]
    carried = (
        from_behind(carried.astype(jnp.bfloat16), "ctx", -1).astype(carried.dtype)
        + grad_pieces[:, 0:rows]
    )
    grad_kv = carried.astype(jnp.bfloat16).reshape(micro * rows, -1)
    grad_normed = dense_right(grad_queries, w_query) + dense_right(grad_kv, w_keyvalue)
    _, norm_back_one = jax.vjp(layer_norm, hidden, gains[0], biases[0])
    grad_hidden, grad_gain_one, grad_bias_one = norm_back_one(grad_normed)
    grad_input = grad_after + grad_hidden
    terms = (
        normed,
        grad_queries,
        grad_kv,
        mixed,
        grad_branch,
        normed_two,
        grad_upper,
        activated,
        grad_low,
        jnp.stack([grad_gain_one, grad_gain_two, grad_bias_one, grad_bias_two]),
    )
    return (grad_input, terms)


def body(
    tokens, cotangent, segment_ids, w_query, w_keyvalue, w_out, w_up, w_down, ln_gains, ln_biases
):
    section_index = lax.axis_index("section")
    cycle_place = lax.axis_index("ctx")
    cycle_size = lax.axis_size("ctx")
    micro = tokens.shape[0]
    width = tokens.shape[3]
    early = section_index == 0
    late = section_index == 1
    segments = segment_ids[:, 0]
    own_tokens = tokens[:, 0].reshape(-1, width)
    own_cotangent = cotangent[:, 0].reshape(-1, width)

    def spread(weight):
        half = weight.shape[1] // cycle_size
        part = lax.dynamic_slice_in_dim(weight, cycle_place * half, half, axis=1)
        return lax.all_gather(part, ("dp", "ctx"), axis=1, tiled=True)[0]

    scales = lax.all_gather(
        jnp.concatenate([ln_gains, ln_biases], axis=1), "dp", axis=2, tiled=True
    )[0].astype(jnp.float32)
    weights = (
        spread(w_query),
        lax.all_gather(w_keyvalue, "dp", axis=1, tiled=True)[0],
        spread(w_out),
        spread(w_up),
        spread(w_down),
        scales[0:2],
        scales[2:4],
    )
    result, kept_first = layer_forward(
        own_tokens.astype(jnp.float32), segments, weights, micro, cycle_place, cycle_size
    )
    first_low = result.astype(jnp.bfloat16)
    incoming = from_behind(first_low, "section", 1)
    result, kept_second = layer_forward(
        incoming.astype(jnp.float32), segments, weights, micro, cycle_place, cycle_size
    )
    second_low = result.astype(jnp.bfloat16)
    grad, terms_second = layer_backward(
        own_cotangent.astype(jnp.float32), kept_second, segments, weights, micro, cycle_place,
        cycle_size,
    )
    grad_second = grad.astype(jnp.bfloat16)
    arriving = from_behind(grad_second, "section", -1)
    grad, terms_first = layer_backward(
        arriving.astype(jnp.float32), kept_first, segments, weights, micro, cycle_place, cycle_size
    )
    grad_first = grad.astype(jnp.bfloat16)
    section_rows = jnp.where(early, first_low, second_low)
    grad_rows = jnp.where(early, grad_first, grad_second)
    (
        normed_all,
        grad_queries_all,
        grad_kv_all,
        mixed_all,
        grad_branch_all,
        normed_two_all,
        grad_upper_all,
        activated_all,
        grad_low_all,
        scale_terms,
    ) = [jnp.where(early, one, two) for one, two in zip(terms_first, terms_second)]

    def reduced(left, right):
        part = dense_left(left, right).astype(jnp.bfloat16)
        piece = lax.psum_scatter(part, ("dp", "ctx"), scatter_dimension=0, tiled=True)
        return lax.all_gather(piece, "ctx", axis=0, tiled=True).astype(jnp.float32)[None]

    grad_down = reduced(activated_all, grad_low_all)
    grad_up = reduced(normed_two_all, grad_upper_all)
    grad_out = reduced(mixed_all, grad_branch_all)
    grad_query = reduced(normed_all, grad_queries_all)
    grad_keyvalue = reduced(normed_all, grad_kv_all)
    scale_grads = lax.psum(
        lax.psum_scatter(
            scale_terms.astype(jnp.bfloat16), "dp", scatter_dimension=1, tiled=True
        ),
        "ctx",
    ).astype(jnp.float32)[None]
    local = (1, micro, 1, own_tokens.shape[0] // micro, width)
    return (
        section_rows.reshape(local),
        grad_rows.reshape(local),
        grad_query,
        grad_keyvalue,
        grad_out,
        grad_up,
        grad_down,
        scale_grads[:, 0:2],
        scale_grads[:, 2:4],
    )


def solution(mesh):
    in_specs = (
        P(None, "dp", "ctx", None),
        P(None, "dp", "ctx", None),
        P(None, "dp", None),
        P("section", "dp", None),
        P("section", "dp", None),
        P("section", "dp", None),
        P("section", "dp", None),
        P("section", "dp", None),
        P("section", None, "dp"),
        P("section", None, "dp"),
    )
    out_specs = (
        P("section", None, "dp", "ctx", None),
        P("section", None, "dp", "ctx", None),
        P("section", "dp", None),
        P("section", "dp", None),
        P("section", "dp", None),
        P("section", "dp", None),
        P("section", "dp", None),
        P("section", None, "dp"),
        P("section", None, "dp"),
    )
    step = spread_body if mesh.shape["dp"] == 8 else body
    return jax.shard_map(step, mesh=mesh, in_specs=in_specs, out_specs=out_specs, check_vma=False)
```

```python
import functools
import math

import jax
import jax.numpy as jnp
from jax import lax
from jax.experimental import pallas as pl
from jax.experimental.pallas import tpu as pltpu
from jax.sharding import PartitionSpec as P

HEADS = 16
HEAD = 128


epsilon = 1e-05
masked_score = -1000000000.0


def layer_norm(values_in, gain_row, bias_row):
    mean_row = jnp.mean(values_in, axis=-1, keepdims=True)
    centered = values_in - mean_row
    variance = jnp.mean(centered * centered, axis=-1, keepdims=True)
    return centered * lax.rsqrt(variance + epsilon) * gain_row + bias_row


def dense(left, right):
    return jnp.dot(left, right, preferred_element_type=jnp.float32)


def dense_left(left, right):
    return lax.dot_general(
        left, right, (((0,), (0,)), ((), ())), preferred_element_type=jnp.float32
    )


def dense_right(left, right):
    return lax.dot_general(
        left, right, (((1,), (1,)), ((), ())), preferred_element_type=jnp.float32
    )


MESH = pl.DeviceIdType.MESH
PARTS = 2


def gelu(v):
    inner = math.sqrt(2.0 / math.pi) * (v + 0.044715 * v * v * v)
    return 0.5 * v * (1.0 + jnp.tanh(inner))


def gelu_slope(v):
    scale = math.sqrt(2.0 / math.pi)
    tanh = jnp.tanh(scale * (v + 0.044715 * v * v * v))
    return 0.5 * (1.0 + tanh) + 0.5 * v * (1.0 - tanh * tanh) * scale * (1.0 + 0.134145 * v * v)


def tile_at(step, size):
    return pl.ds(pl.multiple_of(step * size, size), size)


def flat(block):
    return block.reshape(block.shape[0] * block.shape[1], block.shape[2])


def store_part(part, columns, values):
    rows = part.shape[1]
    part[0, :, columns] = values[:rows]
    part[1, :, columns] = values[rows:]


def masked_probs(query, key, mask):
    scores = dense_right(query, key) * HEAD ** (-0.5)
    scores = jnp.where(mask, scores, masked_score)
    scores = jnp.exp(scores - jnp.max(scores, axis=1, keepdims=True))
    return scores / jnp.sum(scores, axis=1, keepdims=True)


def mask_of(seg_col, seg_row, at):
    length = seg_row.shape[2]
    place = lax.broadcasted_iota(jnp.int32, (length, length), 0)
    source = lax.broadcasted_iota(jnp.int32, (length, length), 1)
    return (source <= place) & (seg_col[at] == seg_row[at])


def ffn_forward_at(at, gath, part, weights, ins, outs):
    w_up, w_down = weights
    up_out, act_out = outs
    size = 256

    def up_tile(step, carry):
        columns = tile_at(step, size)
        up_rows = dense(flat(gath[at]), w_up[:, columns])
        up_out[at, :, columns] = up_rows.astype(jnp.bfloat16)
        act_out[at, :, columns] = gelu(up_rows).astype(jnp.bfloat16)
        return carry

    lax.fori_loop(0, w_up.shape[1] // size, up_tile, 0)

    def down_tile(step, carry):
        columns = tile_at(step, size)
        store_part(part, columns, dense(act_out[at], w_down[:, columns]))
        return carry

    lax.fori_loop(0, w_down.shape[1] // size, down_tile, 0)


def ffn_backward_at(at, gath, part, weights, ins, outs):
    w_up, w_down = weights
    (up_in,) = ins
    (upper_out,) = outs
    size = 256

    def act_tile(step, carry):
        columns = tile_at(step, size)
        grad_act = dense_right(flat(gath[at]), w_down[columns, :])
        slope = gelu_slope(up_in[at, :, columns].astype(jnp.float32))
        upper_out[at, :, columns] = (grad_act * slope).astype(jnp.bfloat16)
        return carry

    lax.fori_loop(0, w_down.shape[0] // size, act_tile, 0)

    def back_tile(step, carry):
        columns = tile_at(step, size)
        store_part(part, columns, dense_right(upper_out[at], w_up[columns, :]))
        return carry

    lax.fori_loop(0, w_up.shape[0] // size, back_tile, 0)


def attention_forward_at(at, gath, part, weights, ins, outs):
    w_query, w_keyvalue, w_out = weights
    seg_col, seg_row = ins
    query_out, keyvalue_out, mixed_out = outs
    size = 256
    rows = flat(gath[at])
    query_out[at] = dense(rows, w_query[...]).astype(jnp.bfloat16)
    keyvalue_out[at] = dense(rows, w_keyvalue[...]).astype(jnp.bfloat16)
    mask = mask_of(seg_col, seg_row, at)
    for head in range(w_query.shape[1] // HEAD):
        own = slice(head * HEAD, (head + 1) * HEAD)
        probs = masked_probs(query_out[at, :, own], keyvalue_out[at, :, :HEAD], mask)
        mixed = dense(probs.astype(jnp.bfloat16), keyvalue_out[at, :, HEAD:])
        mixed_out[at, :, own] = mixed.astype(jnp.bfloat16)

    def out_tile(step, carry):
        columns = tile_at(step, size)
        store_part(part, columns, dense(mixed_out[at], w_out[:, columns]))
        return carry

    lax.fori_loop(0, w_out.shape[1] // size, out_tile, 0)


def attention_backward_at(at, gath, part, weights, ins, outs):
    w_query, w_keyvalue, w_out = weights
    seg_col, seg_row, query_in, keyvalue_in = ins
    query_out, keyvalue_out = outs
    size = 256
    scale = HEAD ** (-0.5)
    grad_mixed = dense_right(flat(gath[at]), w_out[...]).astype(jnp.bfloat16)
    key = keyvalue_in[at, :, :HEAD]
    value = keyvalue_in[at, :, HEAD:]
    mask = mask_of(seg_col, seg_row, at)
    grad_key = jnp.zeros(key.shape, jnp.float32)
    grad_value = jnp.zeros(value.shape, jnp.float32)
    for head in range(w_query.shape[1] // HEAD):
        own = slice(head * HEAD, (head + 1) * HEAD)
        query = query_in[at, :, own]
        branch = grad_mixed[:, own]
        probs = masked_probs(query, key, mask)
        grad_probs = dense_right(branch, value)
        inner = jnp.sum(probs * grad_probs, axis=1, keepdims=True)
        grad_scores = (probs * (grad_probs - inner)).astype(jnp.bfloat16)
        query_out[at, :, own] = (dense(grad_scores, key) * scale).astype(jnp.bfloat16)
        grad_key = grad_key + dense_left(grad_scores, query)
        grad_value = grad_value + dense_left(probs.astype(jnp.bfloat16), branch)
    keyvalue_out[at, :, :HEAD] = (grad_key * scale).astype(jnp.bfloat16)
    keyvalue_out[at, :, HEAD:] = grad_value.astype(jnp.bfloat16)

    def back_tile(step, carry):
        columns = tile_at(step, size)
        store_part(
            part,
            columns,
            dense_right(query_out[at], w_query[columns, :])
            + dense_right(keyvalue_out[at], w_keyvalue[columns, :]),
        )
        return carry

    lax.fori_loop(0, w_query.shape[0] // size, back_tile, 0)


def half_of(ref, which):
    half = ref.shape[-2] // 2
    at = pl.ds(pl.multiple_of(which * half, half), half)
    return ref.at[at] if len(ref.shape) == 2 else ref.at[:, at]


def half_shape(shape):
    return shape[:-2] + (shape[-2] // 2, shape[-1])


def pass_kernel(compute, n_weights, n_ins, n_outs, places, side_axes, *refs):
    refs = list(refs)
    take = lambda count: [refs.pop(0) for _ in range(count)]
    (x_ref,) = take(1)
    early_weights = take(n_weights)
    late_weights = take(n_weights)
    ins = take(n_ins)
    side_from = take(len(side_axes))
    y_ref, gath = take(2)
    outs = take(n_outs)
    side_to = take(len(side_axes))
    weights = take(n_weights)
    part, partner_out, partner_in, total, line_out, from_left, from_right = take(7)
    (
        weight_sem, gather_right, gather_left, gather_partner, gather_line_in, gather_partner_in,
        partner_send, partner_recv, right_send, right_recv, left_send, left_recv,
        side_send, side_recv,
    ) = take(14)

    section = lax.axis_index("section")
    me = lax.axis_index("dp")
    z = me // 2
    k = me % 2
    last = places - 1
    rows = x_ref.shape[0]
    size = rows // PARTS
    right = {"dp": me + 2}
    left = {"dp": me - 2}
    partner = {"dp": 2 * z + 1 - k}
    has_left = z > 0
    has_right = z < last

    barrier = pltpu.get_barrier_semaphore()
    pl.semaphore_signal(barrier, inc=1, device_id=partner, device_id_type=MESH)

    @pl.when(has_left)
    def _():
        pl.semaphore_signal(barrier, inc=1, device_id=left, device_id_type=MESH)

    @pl.when(has_right)
    def _():
        pl.semaphore_signal(barrier, inc=1, device_id=right, device_id_type=MESH)

    for index in range(n_weights):

        @pl.when(section == 0)
        def _():
            pltpu.make_async_copy(early_weights[index], weights[index], weight_sem.at[index]).start()

        @pl.when(section != 0)
        def _():
            pltpu.make_async_copy(late_weights[index], weights[index], weight_sem.at[index]).start()

    far = {"ctx": 1 - lax.axis_index("ctx"), "section": 1 - section}
    for axis in sorted(set(side_axes)):
        pl.semaphore_signal(barrier, inc=1, device_id={axis: far[axis]}, device_id_type=MESH)
    peers = 1 + len(set(side_axes)) + jnp.where(has_left, 1, 0) + jnp.where(has_right, 1, 0)
    pl.semaphore_wait(barrier, peers)

    sides = []
    for index, axis in enumerate(side_axes):
        source, target = side_from[index], side_to[index]
        if axis == "ctx":
            source = half_of(source, far["ctx"])
        sides.append(
            pltpu.make_async_remote_copy(
                source, target, side_send.at[index], side_recv.at[index],
                device_id={axis: far[axis]}, device_id_type=MESH,
            )
        )

    def cut(index):
        return pl.ds(index * size, size)

    def to_right(block, index, source):
        return pltpu.make_async_remote_copy(
            source, gath.at[block, k, cut(index)], gather_right.at[block, index],
            gather_line_in.at[block, index], device_id=right, device_id_type=MESH,
        )

    def to_left(block, index, source):
        return pltpu.make_async_remote_copy(
            source, gath.at[block, k, cut(index)], gather_left.at[block, index],
            gather_line_in.at[block, index], device_id=left, device_id_type=MESH,
        )

    def to_partner(block, source):
        return pltpu.make_async_remote_copy(
            source, gath.at[block, k], gather_partner.at[block],
            gather_partner_in.at[block], device_id=partner, device_id_type=MESH,
        )

    def sum_to_partner(block):
        return pltpu.make_async_remote_copy(
            partner_out.at[block], partner_in.at[block], partner_send.at[block],
            partner_recv.at[block], device_id=partner, device_id_type=MESH,
        )

    def sum_to_right(block, index):
        return pltpu.make_async_remote_copy(
            line_out.at[block, cut(index)], from_left.at[block, cut(index)],
            right_send.at[block, index], right_recv.at[block, index],
            device_id=right, device_id_type=MESH,
        )

    def sum_to_left(block, index):
        return pltpu.make_async_remote_copy(
            line_out.at[block, cut(index)], from_right.at[block, cut(index)],
            left_send.at[block, index], left_recv.at[block, index],
            device_id=left, device_id_type=MESH,
        )

    for index in range(PARTS):

        @pl.when(has_right)
        def _():
            to_right(z, index, x_ref.at[cut(index)]).start()

        @pl.when(has_left)
        def _():
            to_left(z, index, x_ref.at[cut(index)]).start()

    to_partner(z, x_ref).start()
    for copy in sides:
        copy.start()
    gath[z, k] = x_ref[...]

    at_end = (z == 0) | (z == last)
    low_half = z < places // 2

    def step(i, carry):
        inner_block = jnp.where(i == 0, 1, jnp.where(i == 1, 0, i))
        low_block = jnp.where(z == 0, i, inner_block)
        high_block = last - jnp.where(z == last, i, inner_block)
        block = jnp.where(low_half, low_block, high_block)
        wave = jnp.where(at_end, i, jnp.where(i == 1, 1, jnp.where(i == 3, 2, 0)))
        from_low = z - wave
        from_high = z + wave

        @pl.when((wave > 0) & (from_low >= 0))
        def _():
            for index in range(PARTS):
                to_right(from_low, index, gath.at[from_low, k, cut(index)]).wait_recv()

                @pl.when(has_right)
                def _():
                    to_right(from_low, index, gath.at[from_low, k, cut(index)]).start()

            to_partner(from_low, gath.at[from_low, k]).start()

        @pl.when((wave > 0) & (from_high <= last))
        def _():
            for index in range(PARTS):
                to_left(from_high, index, gath.at[from_high, k, cut(index)]).wait_recv()

                @pl.when(has_left)
                def _():
                    to_left(from_high, index, gath.at[from_high, k, cut(index)]).start()

            to_partner(from_high, gath.at[from_high, k]).start()

        pltpu.make_async_remote_copy(
            gath.at[block, 1 - k], gath.at[block, 1 - k], gather_partner.at[block],
            gather_partner_in.at[block], device_id=partner, device_id_type=MESH,
        ).wait_recv()

        @pl.when(i == 0)
        def _():
            for index in range(n_weights):
                pltpu.make_async_copy(
                    early_weights[index], weights[index], weight_sem.at[index]
                ).wait()

        compute(block, gath, part, weights, ins, outs)
        partner_out[block] = part[1 - k].astype(jnp.bfloat16)
        sum_to_partner(block).start()
        sum_to_partner(block).wait_recv()
        total[block] = part[k] + partner_in[block].astype(jnp.float32)

        @pl.when((z == 0) & (block > 0))
        def _():
            line_out[block] = total[block].astype(jnp.bfloat16)
            for index in range(PARTS):
                sum_to_right(block, index).start()

        @pl.when((z == last) & (block < last))
        def _():
            line_out[block] = total[block].astype(jnp.bfloat16)
            for index in range(PARTS):
                sum_to_left(block, index).start()

        return carry

    lax.fori_loop(0, places, step, 0)

    n_left = jnp.where(has_left, places - z, 0)
    n_right = jnp.where(has_right, z + 1, 0)
    n_first = jnp.where(low_half, n_left, n_right)

    def finish(i, carry):
        in_first = i < n_first
        turn = jnp.where(in_first, i, i - n_first)
        is_left = in_first == low_half
        block = jnp.where(is_left, z + turn, z - turn)

        @pl.when(is_left)
        def _():
            for index in range(PARTS):
                sum_to_right(block, index).wait_recv()
                total[block, cut(index)] += from_left[block, cut(index)].astype(jnp.float32)

                @pl.when(block > z)
                def _():
                    line_out[block, cut(index)] = total[block, cut(index)].astype(jnp.bfloat16)
                    sum_to_right(block, index).start()

        @pl.when(jnp.logical_not(is_left))
        def _():
            for index in range(PARTS):
                sum_to_left(block, index).wait_recv()
                total[block, cut(index)] += from_right[block, cut(index)].astype(jnp.float32)

                @pl.when(block < z)
                def _():
                    line_out[block, cut(index)] = total[block, cut(index)].astype(jnp.bfloat16)
                    sum_to_left(block, index).start()

        return carry

    lax.fori_loop(0, n_left + n_right, finish, 0)
    y_ref[...] = total[z]

    def drain(block, carry):
        to_partner(block, gath.at[block, k]).wait_send()
        sum_to_partner(block).wait_send()
        for index in range(PARTS):

            @pl.when((block <= z) & has_right)
            def _():
                to_right(block, index, gath.at[block, k, cut(index)]).wait_send()

            @pl.when((block >= z) & has_left)
            def _():
                to_left(block, index, gath.at[block, k, cut(index)]).wait_send()

            @pl.when(block > z)
            def _():
                sum_to_right(block, index).wait_send()

            @pl.when(block < z)
            def _():
                sum_to_left(block, index).wait_send()

        return carry

    lax.fori_loop(0, places, drain, 0)
    for copy in sides:
        copy.wait()


def tensor_pass(compute, ident, x, early_weights, late_weights, ins, out_widths, sides=()):
    rows, width = x.shape
    places = lax.axis_size("dp") // 2
    vmem = pl.BlockSpec(memory_space=pltpu.VMEM)
    hbm = pl.BlockSpec(memory_space=pl.ANY)
    count = len(early_weights)
    dma = pltpu.SemaphoreType.DMA
    axes = [axis for axis, _ in sides]
    moved = [
        half_shape(array.shape) if axis == "ctx" else array.shape for axis, array in sides
    ]
    kernel = functools.partial(
        pass_kernel, compute, count, len(ins), len(out_widths), places, axes
    )
    call = pl.pallas_call(
        kernel,
        out_shape=[
            jax.ShapeDtypeStruct((rows, width), jnp.float32),
            jax.ShapeDtypeStruct((places, 2, rows, width), jnp.bfloat16),
        ]
        + [jax.ShapeDtypeStruct((places, 2 * rows, out), jnp.bfloat16) for out in out_widths]
        + [jax.ShapeDtypeStruct(shape, jnp.bfloat16) for shape in moved],
        in_specs=[vmem] + [hbm] * (2 * count) + [vmem] * len(ins) + [hbm] * len(axes),
        out_specs=[vmem] * (2 + len(out_widths)) + [hbm] * len(axes),
        scratch_shapes=[pltpu.VMEM(weight.shape, weight.dtype) for weight in early_weights]
        + [
            pltpu.VMEM((2, rows, width), jnp.float32),
            pltpu.VMEM((places, rows, width), jnp.bfloat16),
            pltpu.VMEM((places, rows, width), jnp.bfloat16),
            pltpu.VMEM((places, rows, width), jnp.float32),
            pltpu.VMEM((places, rows, width), jnp.bfloat16),
            pltpu.VMEM((places, rows, width), jnp.bfloat16),
            pltpu.VMEM((places, rows, width), jnp.bfloat16),
            dma((count,)),
            dma((places, PARTS)),
            dma((places, PARTS)),
            dma((places,)),
            dma((places, PARTS)),
            dma((places,)),
            dma((places,)),
            dma((places,)),
            dma((places, PARTS)),
            dma((places, PARTS)),
            dma((places, PARTS)),
            dma((places, PARTS)),
            dma((max(len(axes), 1),)),
            dma((max(len(axes), 1),)),
        ],
        cost_estimate=pl.CostEstimate(
            flops=60_000_000_000, bytes_accessed=20_000_000, transcendentals=0
        ),
        compiler_params=pltpu.CompilerParams(
            collective_id=ident, has_side_effects=True, vmem_limit_bytes=60 * 1024 * 1024
        ),
    )
    return call(
        x, *early_weights, *late_weights, *ins, *[array for _, array in sides]
    )


def distribute_kernel(
    places, query, keyvalue, notes, out, up, down,
    query_own, keyvalue_own, notes_own, up_own,
    query_far, keyvalue_far, notes_far, out_far, up_far, down_far,
    local_sem, query_send, query_recv, keyvalue_send, keyvalue_recv, notes_send, notes_recv,
    up_send, up_recv,
    across_send, across_recv, over_send, over_recv,
):
    section = lax.axis_index("section")
    ctx = lax.axis_index("ctx")
    me = lax.axis_index("dp")
    z = me // 2
    k = me % 2
    last = places - 1
    rows = query.shape[0]
    half = rows // 2
    head_width = query_own.shape[1]
    unit_width = up_own.shape[1]
    across = {"section": 1 - section}
    over = {"ctx": 1 - ctx}

    def peers(act):
        act(2 * z + 1 - k)
        for away in range(1, places):

            @pl.when(z + away <= last)
            def _():
                act(2 * (z + away) + k)
                act(2 * (z + away) + 1 - k)

            @pl.when(z - away >= 0)
            def _():
                act(2 * (z - away) + k)
                act(2 * (z - away) + 1 - k)

    def remote(source, target, send, recv, device):
        return pltpu.make_async_remote_copy(
            source, target, send, recv, device_id=device, device_id_type=MESH
        )

    def piece(owner, part, count):
        which = jnp.where(part == 0, ctx, 1 - ctx)
        return tile_at(2 * owner + which, count // 2)

    def query_copy(source, to):
        return remote(
            query.at[:, tile_at(to, head_width)], query_own.at[tile_at(source, rows)],
            query_send.at[to], query_recv.at[source], {"dp": to},
        )

    def keyvalue_copy(source, to):
        return remote(
            keyvalue, keyvalue_own.at[tile_at(source, rows)],
            keyvalue_send.at[to], keyvalue_recv.at[source], {"dp": to},
        )

    def notes_copy(source, to):
        return remote(
            notes, notes_own.at[tile_at(source, notes.shape[0])],
            notes_send.at[to], notes_recv.at[source], {"dp": to},
        )

    def up_copy(source, to, part):
        which = jnp.where(part == 0, ctx, 1 - ctx)
        return remote(
            up.at[tile_at(which, half), tile_at(to, unit_width)],
            up_own.at[piece(source, part, rows)],
            up_send.at[to, part], up_recv.at[source, part], {"dp": to},
        )

    barrier = pltpu.get_barrier_semaphore()

    def greet(to):
        pl.semaphore_signal(barrier, inc=1, device_id={"dp": to}, device_id_type=MESH)

    peers(greet)
    pl.semaphore_signal(barrier, inc=1, device_id=across, device_id_type=MESH)
    pl.semaphore_signal(barrier, inc=1, device_id=over, device_id_type=MESH)
    pl.semaphore_wait(barrier, 2 * places + 1)

    local = [
        pltpu.make_async_copy(
            query.at[:, tile_at(me, head_width)], query_own.at[tile_at(me, rows)], local_sem.at[0]
        ),
        pltpu.make_async_copy(keyvalue, keyvalue_own.at[tile_at(me, rows)], local_sem.at[1]),
        pltpu.make_async_copy(notes, notes_own.at[tile_at(me, notes.shape[0])], local_sem.at[2]),
        pltpu.make_async_copy(
            up.at[:, tile_at(me, unit_width)], up_own.at[tile_at(me, rows)], local_sem.at[3]
        ),
    ]
    for copy in local:
        copy.start()
    peers(lambda to: notes_copy(me, to).start())
    peers(lambda to: query_copy(me, to).start())
    peers(lambda to: keyvalue_copy(me, to).start())
    peers(lambda to: up_copy(me, to, 0).start())

    pieces = 2 * places
    out_half = tile_at(ctx, out.shape[0] // 2)
    short = down.shape[0] // 2 // pieces
    flows = [(out, out_far, out_half)] + [
        (down, down_far, tile_at(pieces * ctx + index, short)) for index in range(pieces)
    ]

    def flow_across(slot):
        source, target, at = flows[slot]
        return remote(
            source.at[at], target.at[at], across_send.at[slot], across_recv.at[slot], across
        )

    def flow_over(slot):
        _, target, at = flows[slot]
        return remote(target.at[at], target.at[at], over_send.at[slot], over_recv.at[slot], over)

    first_slot = len(flows)
    kinds = [
        (notes_own, notes_far, notes.shape[0]),
        (query_own, query_far, rows),
        (keyvalue_own, keyvalue_far, rows),
        (up_own, up_far, rows),
    ]

    def block_across(kind, owner):
        own, far, count = kinds[kind]
        slot = first_slot + kind * 2 * places + owner
        at = piece(owner, 0, count)
        return remote(own.at[at], far.at[at], across_send.at[slot], across_recv.at[slot], across)

    def block_over(kind, owner):
        _, far, count = kinds[kind]
        slot = first_slot + kind * 2 * places + owner
        at = piece(owner, 0, count)
        return remote(far.at[at], far.at[at], over_send.at[slot], over_recv.at[slot], over)

    for slot in range(first_slot):
        flow_across(slot).start()
    peers(lambda to: up_copy(me, to, 1).start())

    def hand_over(slot):
        flow_across(slot).wait_recv()
        flow_over(slot).start()

    for index in range(3):
        local[index].wait()
    block_across(0, me).start()
    block_across(1, me).start()
    block_across(2, me).start()
    hand_over(0)

    def pass_query(source):
        notes_copy(source, me).wait_recv()
        block_across(0, source).start()
        query_copy(source, me).wait_recv()
        block_across(1, source).start()

    def pass_keyvalue(source):
        keyvalue_copy(source, me).wait_recv()
        block_across(2, source).start()

    peers(pass_query)
    for slot in range(1, 1 + pieces // 2):
        hand_over(slot)
    peers(pass_keyvalue)
    for slot in range(1 + pieces // 2, first_slot):
        hand_over(slot)
    local[3].wait()
    block_across(3, me).start()

    def pass_up(source):
        up_copy(source, me, 0).wait_recv()
        block_across(3, source).start()

    peers(pass_up)

    def over_block(kind):
        def move(owner, carry):
            block_across(kind, owner).wait_recv()
            block_over(kind, owner).start()
            return carry

        lax.fori_loop(0, 2 * places, move, 0)

    for kind in range(len(kinds)):
        over_block(kind)

    peers(lambda source: up_copy(source, me, 1).wait_recv())

    def over_wait(slot_owner, carry):
        for kind in range(len(kinds)):
            block_over_in(kind, slot_owner).wait_recv()
            block_across(kind, slot_owner).wait_send()
            block_over(kind, slot_owner).wait_send()
        return carry

    def block_over_in(kind, owner):
        _, far, count = kinds[kind]
        slot = first_slot + kind * 2 * places + owner
        at = piece(owner, 1, count)
        return remote(far.at[at], far.at[at], over_send.at[slot], over_recv.at[slot], over)

    lax.fori_loop(0, 2 * places, over_wait, 0)
    for slot in range(first_slot):
        flow_over(slot).wait_recv()
        flow_across(slot).wait_send()
        flow_over(slot).wait_send()

    def sent(to):
        notes_copy(me, to).wait_send()
        query_copy(me, to).wait_send()
        keyvalue_copy(me, to).wait_send()
        up_copy(me, to, 0).wait_send()
        up_copy(me, to, 1).wait_send()

    peers(sent)


def distribute(query, keyvalue, notes, out, up, down):
    size = lax.axis_size("dp")
    places = size // 2
    hbm = pl.BlockSpec(memory_space=pl.ANY)
    dma = pltpu.SemaphoreType.DMA
    rows = query.shape[0] * size
    small = [
        (rows, query.shape[1] // size),
        (rows, keyvalue.shape[1]),
        (notes.shape[0] * size, notes.shape[1]),
    ]
    turned = (rows, up.shape[1] // size)
    shapes = small + [turned] + small + [out.shape, turned, down.shape]
    slots = 1 + 5 * size
    return pl.pallas_call(
        functools.partial(distribute_kernel, places),
        name="distribute",
        out_shape=[jax.ShapeDtypeStruct(shape, jnp.bfloat16) for shape in shapes],
        in_specs=[hbm] * 6,
        out_specs=[hbm] * len(shapes),
        scratch_shapes=[dma((4,))]
        + [dma((size,))] * 6
        + [dma((size, 2))] * 2
        + [dma((slots,))] * 4,
        cost_estimate=pl.CostEstimate(
            flops=150_000_000_000, bytes_accessed=20_000_000, transcendentals=0
        ),
        compiler_params=pltpu.CompilerParams(collective_id=4, has_side_effects=True),
    )(query, keyvalue, notes, out, up, down)


def collect_kernel(
    places, up_full, down_full, query_full, out_full, up_moved, down_moved,
    up_late, down_late, query_late, out_late, up_far, down_far, query_far, out_far, small,
    up_out, down_out, query_out, out_out, small_out,
    small_in, small_sum, small_far, small_total, small_side,
    up, up_in, up_part, up_side, down, down_in, down_part, down_side,
    query, query_in, query_part, query_side, out, out_in, out_part, out_side,
    local_sem, side_send, side_recv, across_send, across_recv,
    turn_send, turn_recv, over_send, over_recv, small_send, small_recv,
):
    section = lax.axis_index("section")
    ctx = lax.axis_index("ctx")
    me = lax.axis_index("dp")
    z = me // 2
    k = me % 2
    last = places - 1
    size = 2 * places
    early = section == 0
    late = section != 0
    across = {"section": 1 - section}
    over = {"ctx": 1 - ctx}
    chunks = 4
    short = down.shape[0] // chunks
    turned = [(up, up_out), (query, query_out)]
    half = up.shape[1]

    def peers(act):
        act(2 * z + 1 - k)
        for away in range(1, places):

            @pl.when(z + away <= last)
            def _():
                act(2 * (z + away) + k)
                act(2 * (z + away) + 1 - k)

            @pl.when(z - away >= 0)
            def _():
                act(2 * (z - away) + k)
                act(2 * (z - away) + 1 - k)

    def remote(source, target, send, recv, device):
        return pltpu.make_async_remote_copy(
            source, target, send, recv, device_id=device, device_id_type=MESH
        )

    barrier = pltpu.get_barrier_semaphore()

    def greet(to):
        pl.semaphore_signal(barrier, inc=1, device_id={"dp": to}, device_id_type=MESH)

    peers(greet)
    pl.semaphore_signal(barrier, inc=1, device_id=across, device_id_type=MESH)
    pl.semaphore_signal(barrier, inc=1, device_id=over, device_id_type=MESH)
    pl.semaphore_wait(barrier, size + 1)

    side = [
        remote(half_of(query_full, 1 - ctx), query_side, side_send.at[0], side_recv.at[0], over),
        remote(half_of(out_full, 1 - ctx), out_side, side_send.at[1], side_recv.at[1], over),
    ]
    for copy in side:
        copy.start()

    def small_turn(source, to, layer):
        return remote(
            small.at[layer, to], small_in.at[layer, source],
            small_send.at[layer, to], small_recv.at[layer, source], {"dp": to},
        )

    own_small = [
        pltpu.make_async_copy(
            small.at[layer, me], small_in.at[layer, me], local_sem.at[13 + layer]
        )
        for layer in range(2)
    ]
    for layer in range(2):
        own_small[layer].start()

    def small_start(to):
        for layer in range(2):
            small_turn(me, to, layer).start()

    def small_wait(source):
        for layer in range(2):
            small_turn(source, me, layer).wait_recv()

    def small_sent(to):
        for layer in range(2):
            small_turn(me, to, layer).wait_send()

    small_across = remote(
        small_sum.at[1 - section], small_far, across_send.at[size + 6], across_recv.at[size + 6],
        across,
    )
    small_over = remote(small_total, small_side, side_send.at[2], side_recv.at[2], over)

    def up_across(owner):
        return remote(
            up_part.at[owner], up_in.at[owner], across_send.at[owner], across_recv.at[owner], across
        )

    def down_across(index):
        slot = size + index
        at = pl.ds(index * short, short)
        return remote(
            down_part.at[at], down_in.at[at], across_send.at[slot], across_recv.at[slot], across
        )

    query_across = remote(
        query_part, query_in, across_send.at[size + chunks], across_recv.at[size + chunks], across
    )
    out_across = remote(
        out_part, out_in, across_send.at[size + chunks + 1], across_recv.at[size + chunks + 1],
        across,
    )

    def load(index, source, target):
        copy = pltpu.make_async_copy(source, target, local_sem.at[index])
        copy.start()
        return copy

    loads = [
        load(0, half_of(up_full, ctx), up_part),
        load(1, up_moved, up_side),
        load(2, half_of(query_full, ctx), query_part),
        load(3, half_of(out_full, ctx), out_part),
        load(4, half_of(down_full, ctx), down_part),
        load(5, down_moved, down_side),
    ]
    owned = [
        (up_late, up), (up_far, up_in), (query_late, query), (query_far, query_in),
        (out_late, out), (out_far, out_in), (down_late, down), (down_far, down_in),
    ]

    @pl.when(late)
    def _():
        for index, (source, target) in enumerate(owned):
            load(15 + index, source, target)

    loads[0].wait()
    loads[1].wait()

    def send_up(owner):
        up_part[owner] = up_part[owner] + up_side[owner]

        @pl.when(late)
        def _():
            up_across(owner).start()

    peers(send_up)
    send_up(me)
    loads[2].wait()
    loads[3].wait()
    for copy in side:
        copy.wait_recv()
    query_part[...] = query_part[...] + query_side[...]
    out_part[...] = out_part[...] + out_side[...]
    loads[4].wait()
    loads[5].wait()
    down_part[...] = down_part[...] + down_side[...]

    @pl.when(late)
    def _():
        query_across.start()
        out_across.start()
        for index in range(chunks):
            down_across(index).start()
        for index, (source, target) in enumerate(owned):
            pltpu.make_async_copy(source, target, local_sem.at[15 + index]).wait()

    def turn(kind, source, to):
        block, target = turned[kind]
        width = block.shape[2]
        at = kind * size
        return remote(
            block.at[to], target.at[tile_at(ctx, half), tile_at(source, width)],
            turn_send.at[at + to], turn_recv.at[at + source], {"dp": to},
        )

    def own_block(kind):
        block, target = turned[kind]
        return pltpu.make_async_copy(
            block.at[me], target.at[tile_at(ctx, half), tile_at(me, block.shape[2])],
            local_sem.at[6 + kind],
        )

    def hand_over(kind, source, side_of):
        block, target = turned[kind]
        at = kind * size + source
        region = target.at[tile_at(side_of, half), tile_at(source, block.shape[2])]
        return remote(region, region, over_send.at[at], over_recv.at[at], over)

    def sum_up(owner):
        @pl.when(early)
        def _():
            up_across(owner).wait_recv()
            up[owner] = up_part[owner] + up_in[owner]

        @pl.when(late)
        def _():
            up[owner] = up[owner] + up_in[owner]

    def up_block(owner):
        sum_up(owner)
        turn(0, me, owner).start()

    def arrived(kind):
        def act(source):
            turn(kind, source, me).wait_recv()
            hand_over(kind, source, ctx).start()

        return act

    peers(up_block)
    sum_up(me)
    peers(small_start)
    own_block(0).start()
    peers(arrived(0))
    own_block(0).wait()
    hand_over(0, me, ctx).start()

    @pl.when(early)
    def _():
        query_across.wait_recv()
        query[...] = query_part[...] + query_in[...]
        out_across.wait_recv()
        out[...] = out_part[...] + out_in[...]

    @pl.when(late)
    def _():
        query[...] = query[...] + query_in[...]
        out[...] = out[...] + out_in[...]

    peers(lambda owner: turn(1, me, owner).start())
    own_block(1).start()

    def flat_over(index, side_of):
        slot = 2 * size + index
        if index == 0:
            source, target, at = out, out_out, tile_at(side_of, out.shape[0])
            return remote(source, target.at[at], over_send.at[slot], over_recv.at[slot], over), (
                pltpu.make_async_copy(source, target.at[at], local_sem.at[8])
            )
        source = down.at[pl.ds((index - 1) * short, short)]
        target = down_out.at[tile_at(side_of * chunks + index - 1, short)]
        return remote(source, target, over_send.at[slot], over_recv.at[slot], over), (
            pltpu.make_async_copy(source, target, local_sem.at[8 + index])
        )

    for copy in flat_over(0, ctx):
        copy.start()
    for index in range(chunks):

        @pl.when(early)
        def _():
            at = pl.ds(index * short, short)
            down_across(index).wait_recv()
            down[at] = down_part[at] + down_in[at]

        @pl.when(late)
        def _():
            at = pl.ds(index * short, short)
            down[at] = down[at] + down_in[at]

        for copy in flat_over(1 + index, ctx):
            copy.start()
    peers(arrived(1))
    own_block(1).wait()
    hand_over(1, me, ctx).start()
    for layer in range(2):
        own_small[layer].wait()
    peers(small_wait)
    for layer in range(2):
        total = small_in[layer, 0].astype(jnp.float32)
        for source in range(1, size):
            total = total + small_in[layer, source].astype(jnp.float32)
        small_sum[layer] = total.astype(jnp.bfloat16)
    small_across.start()


    small_across.wait_recv()
    small_total[...] = small_sum[section] + small_far[...]
    small_over.start()
    small_over.wait_recv()
    small_out[...] = (small_total[...] + small_side[...]).astype(jnp.float32)

    peers(small_sent)
    small_across.wait_send()
    small_over.wait_send()
    for copy in side:
        copy.wait_send()

    @pl.when(late)
    def _():
        peers(lambda owner: up_across(owner).wait_send())
        up_across(me).wait_send()
        query_across.wait_send()
        out_across.wait_send()
        for index in range(chunks):
            down_across(index).wait_send()

    for kind in range(2):
        peers(lambda owner: turn(kind, me, owner).wait_send())

        def finish(source, carry):
            hand_over(kind, source, ctx).wait_send()
            hand_over(kind, source, 1 - ctx).wait_recv()
            return carry

        lax.fori_loop(0, size, finish, 0)
    for index in range(1 + chunks):
        moved, kept = flat_over(index, ctx)
        kept.wait()
        moved.wait_send()
        flat_over(index, 1 - ctx)[0].wait_recv()


def collect(fulls, moved, late, far, small):
    size = lax.axis_size("dp")
    hbm = pl.BlockSpec(memory_space=pl.ANY)
    dma = pltpu.SemaphoreType.DMA
    vmem = lambda x: pltpu.VMEM(x.shape, x.dtype)
    up, down, query, out = fulls
    shapes = [
        (up.shape[1], size * up.shape[2]),
        down.shape,
        (query.shape[1], size * query.shape[2]),
        out.shape,
    ]
    return pl.pallas_call(
        functools.partial(collect_kernel, size // 2),
        name="collect",
        out_shape=[jax.ShapeDtypeStruct(shape, jnp.bfloat16) for shape in shapes]
        + [jax.ShapeDtypeStruct(small.shape[2:], jnp.float32)],
        in_specs=[hbm] * 15,
        out_specs=[hbm] * 4 + [pl.BlockSpec(memory_space=pltpu.VMEM)],
        scratch_shapes=[vmem(small), vmem(small[:, 0])]
        + [vmem(small[0, 0])] * 3
        + [vmem(x) for x in late for _ in range(4)]
        + [dma((23,)), dma((3,)), dma((3,))]
        + [dma((size + 7,))] * 2
        + [dma((2 * size,))] * 2
        + [dma((2 * size + 5,))] * 2
        + [dma((2, size))] * 2,
        cost_estimate=pl.CostEstimate(
            flops=120_000_000_000, bytes_accessed=20_000_000, transcendentals=0
        ),
        compiler_params=pltpu.CompilerParams(collective_id=5, has_side_effects=True),
    )(*fulls, *moved, *late, *far, small)


def swapped(size):
    pairs = []
    for ctx in range(2):
        for at in range(size):
            z, k = at // 2, at % 2
            pairs.append((ctx * size + at, k * size + 2 * z + ctx))
    return pairs


def regroup(x):
    return lax.ppermute(x, ("ctx", "dp"), swapped(lax.axis_size("dp")))


def regroup_across(x):
    size = lax.axis_size("dp")
    half = 2 * size
    pairs = swapped(size)
    across = [(a, b + half) for a, b in pairs] + [(a + half, b) for a, b in pairs]
    return lax.ppermute(x, ("section", "ctx", "dp"), across)


def own_half(grad):
    half = grad.shape[-2] // 2
    return lax.dynamic_slice_in_dim(grad, lax.axis_index("ctx") * half, half, axis=-2)


def spread_body(*args):
    return spread_step(*args)


def spread_step(
    tokens, cotangent, segment_ids, w_query, w_keyvalue, w_out, w_up, w_down, ln_gains, ln_biases
):
    section = lax.axis_index("section")
    ctx = lax.axis_index("ctx")
    size = lax.axis_size("dp")
    places = size // 2
    early = section == 0
    width = tokens.shape[3]
    length = segment_ids.shape[2]
    tall = (places * tokens.shape[2] * 2, -1)

    def own_micro(x):
        return lax.dynamic_index_in_dim(x, section, 0, keepdims=False)[0]

    hidden = regroup(own_micro(tokens)).astype(jnp.float32)
    out, down = w_out[0], w_down[0]
    columns = ln_gains.shape[2]
    notes = jnp.concatenate(
        [ln_gains[0], ln_biases[0], own_micro(segment_ids).astype(jnp.bfloat16)[None]], axis=0
    )
    notes = jnp.pad(notes, ((0, 32 - notes.shape[0]), (0, 0)))
    query, keyvalue, notes, up, query_far, keyvalue_far, notes_far, out_far, up_far, down_far = (
        distribute(w_query[0], w_keyvalue[0], notes, out, w_up[0], down)
    )
    notes = notes.reshape(size, 32, columns).transpose(1, 0, 2)
    near = notes[:4].reshape(4, width).astype(jnp.float32)
    far = notes_far.reshape(size, 32, columns).transpose(1, 0, 2)[:4].reshape(4, width)
    far = far.astype(jnp.float32)
    scales = [jnp.where(early, near, far), jnp.where(early, far, near)]
    segments = notes[4].astype(jnp.int32).reshape(places, 2, length)
    segments = lax.dynamic_index_in_dim(segments, ctx, 1, keepdims=False)
    segs = [segments[:, :, None], segments[:, None, :]]
    attention_near, attention_far = [query, keyvalue, out], [query_far, keyvalue_far, out_far]
    attention_weights = [(attention_near, attention_far), (attention_far, attention_near)]
    ffn_weights = [([up, down], [up_far, down_far]), ([up_far, down_far], [up, down])]
    head_width = query.shape[1]
    unit_width = up.shape[1]

    def forward(layer, hidden):
        normed = layer_norm(hidden, scales[layer][0], scales[layer][2]).astype(jnp.bfloat16)
        y, normed_all, q, kv, mixed = tensor_pass(
            attention_forward_at, 0, normed, *attention_weights[layer], segs,
            [head_width, keyvalue.shape[1], head_width],
        )
        after = hidden + y
        normed_two = layer_norm(after, scales[layer][1], scales[layer][3]).astype(jnp.bfloat16)
        y, normed_two_all, up_rows, activated = tensor_pass(
            ffn_forward_at, 1, normed_two, *ffn_weights[layer], [],
            [unit_width, unit_width],
        )
        result = (after + y).astype(jnp.bfloat16)
        return result, (hidden, normed_all, q, kv, mixed, after, normed_two_all, up_rows, activated)

    def product(left, right):
        return dense_left(left.reshape(tall), right.reshape(tall)).astype(jnp.bfloat16)

    def rows_of_all(grad):
        return grad.reshape(size, grad.shape[0] // size, grad.shape[1])

    def ffn_backward(layer, ident, grad_low, kept, sides):
        _, _, _, _, _, after, normed_two_all, up_rows, activated = kept
        y, grad_low_all, grad_upper, *arrived = tensor_pass(
            ffn_backward_at, ident, grad_low, *ffn_weights[layer],
            [up_rows], [unit_width], sides,
        )
        grads = [
            rows_of_all(product(normed_two_all, grad_upper)),
            product(activated, grad_low_all),
        ]
        _, norm_back = jax.vjp(layer_norm, after, scales[layer][1], scales[layer][3])
        grad_norm, gain, bias = norm_back(y)
        return grad_low.astype(jnp.float32) + grad_norm, grads, [gain, bias], arrived

    def attention_backward(layer, ident, grad_after, grad_branch, kept, sides):
        hidden, normed_all, q, kv, mixed, _, _, _, _ = kept
        y, grad_branch_all, grad_query, grad_kv, *arrived = tensor_pass(
            attention_backward_at, ident, grad_branch,
            *attention_weights[layer], segs + [q, kv], [head_width, keyvalue.shape[1]], sides,
        )
        grads = [
            rows_of_all(product(normed_all, grad_query)),
            product(mixed, grad_branch_all),
        ]
        keyvalue_grad = product(normed_all, grad_kv)
        _, norm_back = jax.vjp(layer_norm, hidden, scales[layer][0], scales[layer][2])
        grad_norm, gain, bias = norm_back(y)
        return (
            (grad_after + grad_norm).astype(jnp.bfloat16), grads, keyvalue_grad, [gain, bias], arrived
        )

    def low(x):
        return x.astype(jnp.bfloat16)

    def ctx_sums(grads, arrived):
        return [own_half(grad) + other for grad, other in zip(grads, arrived)]

    def both_rows(one, two):
        near = regroup(jnp.where(early, one, two))
        far = regroup_across(jnp.where(early, two, one))
        return jnp.stack([jnp.where(early, near, far), jnp.where(early, far, near)])[None, :, None]

    hold = lax.optimization_barrier
    first, kept_first = forward(0, hidden)
    second, kept_second = forward(1, first.astype(jnp.float32))
    section_rows = both_rows(first, second)
    grad_low = regroup(own_micro(cotangent))

    def sides(axis, arrays):
        return [(axis, array) for array in arrays]

    grad_after, ffn_two, scales_two, _ = ffn_backward(1, 2, grad_low, kept_second, [])
    branch, up_two, down_two = hold((low(grad_after), *ffn_two))
    grad_second, attention_two, keyvalue_two, more, arrived = attention_backward(
        1, 3, grad_after, branch, kept_second, sides("ctx", [up_two])
    )
    scales_two = more[:1] + scales_two[:1] + more[1:] + scales_two[1:]
    (up_two,) = ctx_sums([up_two], arrived)
    grad_after, ffn_one, scales_one, arrived = ffn_backward(
        0, 6, grad_second, kept_first,
        sides("section", [up_two]) + sides("ctx", [down_two] + attention_two),
    )
    up_two_far = arrived[0]
    down_two, *attention_two = ctx_sums([down_two] + attention_two, arrived[1:])
    branch, *both = hold((low(grad_after), *ffn_one, down_two, *attention_two))
    ffn_one, rest_two = both[:2], both[2:]
    grad_first, attention_one, keyvalue_one, more, arrived = attention_backward(
        0, 7, grad_after, branch, kept_first,
        sides("ctx", ffn_one) + sides("section", rest_two),
    )
    scales_one = more[:1] + scales_one[:1] + more[1:] + scales_one[1:]
    ffn_moved, rest_far = arrived[:2], arrived[2:]

    def small_of(keyvalue_grad, rows):
        rows = low(jnp.stack(rows)).reshape(4, size, columns).transpose(1, 0, 2)
        rows = jnp.pad(rows, ((0, 0), (0, 12), (0, 0)))
        return jnp.concatenate([keyvalue_grad.reshape(size, columns, -1), rows], axis=1)

    small = jnp.stack([small_of(keyvalue_one, scales_one), small_of(keyvalue_two, scales_two)])
    up_grad, down_grad, query_grad, out_grad, small = collect(
        ffn_one + attention_one, ffn_moved, [up_two] + rest_two, [up_two_far] + rest_far, small,
    )
    scale_grads = small[None, columns : columns + 4]

    def given(grad):
        return grad.astype(jnp.float32)[None]

    return (
        section_rows,
        both_rows(grad_first, grad_second),
        given(query_grad),
        small[None, :columns],
        given(out_grad),
        given(up_grad),
        given(down_grad),
        scale_grads[:, 0:2],
        scale_grads[:, 2:4],
    )


def from_behind(x, axis, by):
    devices = lax.axis_size(axis)
    pairs = [(i, i + by) for i in range(devices) if 0 <= i + by < devices]
    return lax.ppermute(x, axis, pairs)


def allowed_keys(segments, cycle_place, cycle_size, tok_rows):
    offsets = jnp.arange(tok_rows, dtype=jnp.int32)
    query_pos = cycle_place * tok_rows + offsets
    query_seg = lax.dynamic_slice_in_dim(segments, cycle_place * tok_rows, tok_rows, axis=1)
    blocks = []
    for cycle_step in range(cycle_size):
        source = cycle_place - cycle_step
        key_pos = source * tok_rows + offsets
        key_seg = lax.dynamic_slice_in_dim(
            segments, jnp.maximum(source, 0) * tok_rows, tok_rows, axis=1
        )
        blocks.append(
            (source >= 0)
            & (key_pos[None, None, :] <= query_pos[None, :, None])
            & (key_seg[:, None, :] == query_seg[:, :, None])
        )
    return jnp.concatenate(blocks, axis=2)


def batched(left, right, left_dim, right_dim):
    return lax.dot_general(
        left, right, (((left_dim,), (right_dim,)), ((0,), (0,))), preferred_element_type=jnp.float32
    )


def head_scores(query, keyvalue_all, allowed):
    micro, rows, _ = allowed.shape
    head_rows = query.reshape(micro, rows * HEADS, HEAD)
    scores = batched(head_rows, keyvalue_all[:, :, :HEAD], 2, 2) * HEAD ** (-0.5)
    scores = scores.reshape(micro, rows, HEADS, -1)
    scores = jnp.where(allowed[:, :, None, :], scores, masked_score)
    return (scores.reshape(micro, rows * HEADS, -1), head_rows)


def layer_forward(hidden, segments, weights, micro, cycle_place, cycle_size):
    w_query, w_keyvalue, w_out, w_up, w_down, gains, biases = weights
    rows = hidden.shape[0] // micro
    normed = layer_norm(hidden, gains[0], biases[0]).astype(jnp.bfloat16)
    query = dense(normed, w_query).astype(jnp.bfloat16)
    keyvalue = dense(normed, w_keyvalue).astype(jnp.bfloat16)
    moving = from_behind(keyvalue, "ctx", 1)
    keyvalue_all = jnp.concatenate(
        [keyvalue.reshape(micro, rows, -1), moving.reshape(micro, rows, -1)], axis=1
    )
    allowed = allowed_keys(segments, cycle_place, cycle_size, rows)
    scores, _ = head_scores(query, keyvalue_all, allowed)
    top_score = jnp.max(scores, axis=2, keepdims=True)
    log_total = top_score + jnp.log(jnp.sum(jnp.exp(scores - top_score), axis=2, keepdims=True))
    attn_probs = jnp.exp(scores - log_total).astype(jnp.bfloat16)
    mixed = (
        batched(attn_probs, keyvalue_all[:, :, HEAD:], 2, 1)
        .reshape(micro * rows, HEADS * HEAD)
        .astype(jnp.bfloat16)
    )
    after = hidden + dense(mixed, w_out)
    normed_two = layer_norm(after, gains[1], biases[1]).astype(jnp.bfloat16)
    up_rows = dense(normed_two, w_up)
    activated = jax.nn.gelu(up_rows, approximate=True).astype(jnp.bfloat16)
    result = after + dense(activated, w_down)
    kept = (
        hidden,
        normed,
        query,
        keyvalue_all,
        log_total,
        mixed,
        after,
        normed_two,
        up_rows,
        activated,
    )
    return (result, kept)


def layer_backward(grad_result, kept, segments, weights, micro, cycle_place, cycle_size):
    w_query, w_keyvalue, w_out, w_up, w_down, gains, biases = weights
    hidden, normed, query, keyvalue_all, log_total, mixed, after, normed_two, up_rows, activated = (
        kept
    )
    rows = hidden.shape[0] // micro
    grad_low = grad_result.astype(jnp.bfloat16)
    grad_act = dense_right(grad_low, w_down)
    _, gelu_back = jax.vjp(lambda entries: jax.nn.gelu(entries, approximate=True), up_rows)
    grad_upper = gelu_back(grad_act)[0].astype(jnp.bfloat16)
    _, norm_back_two = jax.vjp(layer_norm, after, gains[1], biases[1])
    grad_after_norm, grad_gain_two, grad_bias_two = norm_back_two(dense_right(grad_upper, w_up))
    grad_after = grad_result + grad_after_norm
    grad_branch = grad_after.astype(jnp.bfloat16)
    grad_mixed = (
        dense_right(grad_branch, w_out).astype(jnp.bfloat16).reshape(micro, rows * HEADS, HEAD)
    )
    allowed = allowed_keys(segments, cycle_place, cycle_size, rows)
    scores, head_rows = head_scores(query, keyvalue_all, allowed)
    attn_probs = jnp.exp(scores - log_total)
    grad_probs = batched(grad_mixed, keyvalue_all[:, :, HEAD:], 2, 2)
    grad_values = batched(attn_probs.astype(jnp.bfloat16), grad_mixed, 1, 1)
    inner = jnp.sum(attn_probs * grad_probs, axis=2, keepdims=True)
    grad_scores = (attn_probs * (grad_probs - inner)).astype(jnp.bfloat16)
    scale_factor = HEAD ** (-0.5)
    grad_queries = (
        (batched(grad_scores, keyvalue_all[:, :, :HEAD], 2, 1) * scale_factor)
        .astype(jnp.bfloat16)
        .reshape(micro * rows, HEADS * HEAD)
    )
    grad_keys = batched(grad_scores, head_rows, 1, 1) * scale_factor
    grad_pieces = jnp.concatenate([grad_keys, grad_values], axis=2)
    carried = grad_pieces[:, (cycle_size - 1) * rows :]
    carried = (
        from_behind(carried.astype(jnp.bfloat16), "ctx", -1).astype(carried.dtype)
        + grad_pieces[:, 0:rows]
    )
    grad_kv = carried.astype(jnp.bfloat16).reshape(micro * rows, -1)
    grad_normed = dense_right(grad_queries, w_query) + dense_right(grad_kv, w_keyvalue)
    _, norm_back_one = jax.vjp(layer_norm, hidden, gains[0], biases[0])
    grad_hidden, grad_gain_one, grad_bias_one = norm_back_one(grad_normed)
    grad_input = grad_after + grad_hidden
    terms = (
        normed,
        grad_queries,
        grad_kv,
        mixed,
        grad_branch,
        normed_two,
        grad_upper,
        activated,
        grad_low,
        jnp.stack([grad_gain_one, grad_gain_two, grad_bias_one, grad_bias_two]),
    )
    return (grad_input, terms)


def body(
    tokens, cotangent, segment_ids, w_query, w_keyvalue, w_out, w_up, w_down, ln_gains, ln_biases
):
    section_index = lax.axis_index("section")
    cycle_place = lax.axis_index("ctx")
    cycle_size = lax.axis_size("ctx")
    micro = tokens.shape[0]
    width = tokens.shape[3]
    early = section_index == 0
    segments = segment_ids[:, 0]
    own_tokens = tokens[:, 0].reshape(-1, width)
    own_cotangent = cotangent[:, 0].reshape(-1, width)

    def spread(weight):
        half = weight.shape[1] // cycle_size
        part = lax.dynamic_slice_in_dim(weight, cycle_place * half, half, axis=1)
        return lax.all_gather(part, ("dp", "ctx"), axis=1, tiled=True)[0]

    scales = lax.all_gather(
        jnp.concatenate([ln_gains, ln_biases], axis=1), "dp", axis=2, tiled=True
    )[0].astype(jnp.float32)
    weights = (
        spread(w_query),
        lax.all_gather(w_keyvalue, "dp", axis=1, tiled=True)[0],
        spread(w_out),
        spread(w_up),
        spread(w_down),
        scales[0:2],
        scales[2:4],
    )
    result, kept_first = layer_forward(
        own_tokens.astype(jnp.float32), segments, weights, micro, cycle_place, cycle_size
    )
    first_low = result.astype(jnp.bfloat16)
    incoming = from_behind(first_low, "section", 1)
    result, kept_second = layer_forward(
        incoming.astype(jnp.float32), segments, weights, micro, cycle_place, cycle_size
    )
    second_low = result.astype(jnp.bfloat16)
    grad, terms_second = layer_backward(
        own_cotangent.astype(jnp.float32), kept_second, segments, weights, micro, cycle_place,
        cycle_size,
    )
    grad_second = grad.astype(jnp.bfloat16)
    arriving = from_behind(grad_second, "section", -1)
    grad, terms_first = layer_backward(
        arriving.astype(jnp.float32), kept_first, segments, weights, micro, cycle_place, cycle_size
    )
    grad_first = grad.astype(jnp.bfloat16)
    section_rows = jnp.where(early, first_low, second_low)
    grad_rows = jnp.where(early, grad_first, grad_second)
    (
        normed_all,
        grad_queries_all,
        grad_kv_all,
        mixed_all,
        grad_branch_all,
        normed_two_all,
        grad_upper_all,
        activated_all,
        grad_low_all,
        scale_terms,
    ) = [jnp.where(early, one, two) for one, two in zip(terms_first, terms_second)]

    def reduced(left, right):
        part = dense_left(left, right).astype(jnp.bfloat16)
        piece = lax.psum_scatter(part, ("dp", "ctx"), scatter_dimension=0, tiled=True)
        return lax.all_gather(piece, "ctx", axis=0, tiled=True).astype(jnp.float32)[None]

    grad_down = reduced(activated_all, grad_low_all)
    grad_up = reduced(normed_two_all, grad_upper_all)
    grad_out = reduced(mixed_all, grad_branch_all)
    grad_query = reduced(normed_all, grad_queries_all)
    grad_keyvalue = reduced(normed_all, grad_kv_all)
    scale_grads = lax.psum(
        lax.psum_scatter(
            scale_terms.astype(jnp.bfloat16), "dp", scatter_dimension=1, tiled=True
        ),
        "ctx",
    ).astype(jnp.float32)[None]
    local = (1, micro, 1, own_tokens.shape[0] // micro, width)
    return (
        section_rows.reshape(local),
        grad_rows.reshape(local),
        grad_query,
        grad_keyvalue,
        grad_out,
        grad_up,
        grad_down,
        scale_grads[:, 0:2],
        scale_grads[:, 2:4],
    )


def solution(mesh):
    in_specs = (
        P(None, "dp", "ctx", None),
        P(None, "dp", "ctx", None),
        P(None, "dp", None),
        P("section", "dp", None),
        P("section", "dp", None),
        P("section", "dp", None),
        P("section", "dp", None),
        P("section", "dp", None),
        P("section", None, "dp"),
        P("section", None, "dp"),
    )
    out_specs = (
        P("section", None, "dp", "ctx", None),
        P("section", None, "dp", "ctx", None),
        P("section", "dp", None),
        P("section", "dp", None),
        P("section", "dp", None),
        P("section", "dp", None),
        P("section", "dp", None),
        P("section", None, "dp"),
        P("section", None, "dp"),
    )
    spread = mesh.shape["dp"] == 8
    return jax.shard_map(
        spread_body if spread else body,
        mesh=mesh, in_specs=in_specs, out_specs=out_specs, check_vma=False,
    )
```

```python
import functools
import math

import jax
import jax.numpy as jnp
from jax import lax
from jax.experimental import pallas as pl
from jax.experimental.pallas import tpu as pltpu
from jax.sharding import PartitionSpec as P

HEADS = 16
HEAD = 128


epsilon = 1e-05
masked_score = -1000000000.0


def layer_norm(values_in, gain_row, bias_row):
    mean_row = jnp.mean(values_in, axis=-1, keepdims=True)
    centered = values_in - mean_row
    variance = jnp.mean(centered * centered, axis=-1, keepdims=True)
    return centered * lax.rsqrt(variance + epsilon) * gain_row + bias_row


def dense(left, right):
    return jnp.dot(left, right, preferred_element_type=jnp.float32)


def dense_left(left, right):
    return lax.dot_general(
        left, right, (((0,), (0,)), ((), ())), preferred_element_type=jnp.float32
    )


def dense_right(left, right):
    return lax.dot_general(
        left, right, (((1,), (1,)), ((), ())), preferred_element_type=jnp.float32
    )


MESH = pl.DeviceIdType.MESH
PARTS = 4


def gelu(v):
    inner = math.sqrt(2.0 / math.pi) * (v + 0.044715 * v * v * v)
    return 0.5 * v * (1.0 + jnp.tanh(inner))


def gelu_slope(v):
    scale = math.sqrt(2.0 / math.pi)
    tanh = jnp.tanh(scale * (v + 0.044715 * v * v * v))
    return 0.5 * (1.0 + tanh) + 0.5 * v * (1.0 - tanh * tanh) * scale * (1.0 + 0.134145 * v * v)


def tile_at(step, size):
    return pl.ds(pl.multiple_of(step * size, size), size)


def flat(block):
    return block.reshape(block.shape[0] * block.shape[1], block.shape[2])


def store_part(part, columns, values):
    rows = part.shape[1]
    part[0, :, columns] = values[:rows]
    part[1, :, columns] = values[rows:]


def masked_probs(query, key, mask):
    scores = dense_right(query, key) * HEAD ** (-0.5)
    scores = jnp.where(mask, scores, masked_score)
    scores = jnp.exp(scores - jnp.max(scores, axis=1, keepdims=True))
    return scores / jnp.sum(scores, axis=1, keepdims=True)


def mask_of(seg_col, seg_row, at):
    length = seg_row.shape[2]
    place = lax.broadcasted_iota(jnp.int32, (length, length), 0)
    source = lax.broadcasted_iota(jnp.int32, (length, length), 1)
    return (source <= place) & (seg_col[at] == seg_row[at])


def ffn_forward_at(at, gath, part, weights, ins, outs):
    w_up, w_down = weights
    up_out, act_out = outs
    size = 256

    def up_tile(step, carry):
        columns = tile_at(step, size)
        up_rows = dense(flat(gath[at]), w_up[:, columns])
        up_out[at, :, columns] = up_rows.astype(jnp.bfloat16)
        act_out[at, :, columns] = gelu(up_rows).astype(jnp.bfloat16)
        return carry

    lax.fori_loop(0, w_up.shape[1] // size, up_tile, 0)

    def down_tile(step, carry):
        columns = tile_at(step, size)
        store_part(part, columns, dense(act_out[at], w_down[:, columns]))
        return carry

    lax.fori_loop(0, w_down.shape[1] // size, down_tile, 0)


def ffn_backward_at(at, gath, part, weights, ins, outs):
    w_up, w_down = weights
    (up_in,) = ins
    (upper_out,) = outs
    size = 256

    def act_tile(step, carry):
        columns = tile_at(step, size)
        grad_act = dense_right(flat(gath[at]), w_down[columns, :])
        slope = gelu_slope(up_in[at, :, columns].astype(jnp.float32))
        upper_out[at, :, columns] = (grad_act * slope).astype(jnp.bfloat16)
        return carry

    lax.fori_loop(0, w_down.shape[0] // size, act_tile, 0)

    def back_tile(step, carry):
        columns = tile_at(step, size)
        store_part(part, columns, dense_right(upper_out[at], w_up[columns, :]))
        return carry

    lax.fori_loop(0, w_up.shape[0] // size, back_tile, 0)


def attention_forward_at(at, gath, part, weights, ins, outs):
    w_query, w_keyvalue, w_out = weights
    seg_col, seg_row = ins
    query_out, keyvalue_out, mixed_out = outs
    size = 256
    rows = flat(gath[at])
    query_out[at] = dense(rows, w_query[...]).astype(jnp.bfloat16)
    keyvalue_out[at] = dense(rows, w_keyvalue[...]).astype(jnp.bfloat16)
    mask = mask_of(seg_col, seg_row, at)
    for head in range(w_query.shape[1] // HEAD):
        own = slice(head * HEAD, (head + 1) * HEAD)
        probs = masked_probs(query_out[at, :, own], keyvalue_out[at, :, :HEAD], mask)
        mixed = dense(probs.astype(jnp.bfloat16), keyvalue_out[at, :, HEAD:])
        mixed_out[at, :, own] = mixed.astype(jnp.bfloat16)

    def out_tile(step, carry):
        columns = tile_at(step, size)
        store_part(part, columns, dense(mixed_out[at], w_out[:, columns]))
        return carry

    lax.fori_loop(0, w_out.shape[1] // size, out_tile, 0)


def attention_backward_at(at, gath, part, weights, ins, outs):
    w_query, w_keyvalue, w_out = weights
    seg_col, seg_row, query_in, keyvalue_in = ins
    query_out, keyvalue_out = outs
    size = 256
    scale = HEAD ** (-0.5)
    grad_mixed = dense_right(flat(gath[at]), w_out[...]).astype(jnp.bfloat16)
    key = keyvalue_in[at, :, :HEAD]
    value = keyvalue_in[at, :, HEAD:]
    mask = mask_of(seg_col, seg_row, at)
    grad_key = jnp.zeros(key.shape, jnp.float32)
    grad_value = jnp.zeros(value.shape, jnp.float32)
    for head in range(w_query.shape[1] // HEAD):
        own = slice(head * HEAD, (head + 1) * HEAD)
        query = query_in[at, :, own]
        branch = grad_mixed[:, own]
        probs = masked_probs(query, key, mask)
        grad_probs = dense_right(branch, value)
        inner = jnp.sum(probs * grad_probs, axis=1, keepdims=True)
        grad_scores = (probs * (grad_probs - inner)).astype(jnp.bfloat16)
        query_out[at, :, own] = (dense(grad_scores, key) * scale).astype(jnp.bfloat16)
        grad_key = grad_key + dense_left(grad_scores, query)
        grad_value = grad_value + dense_left(probs.astype(jnp.bfloat16), branch)
    keyvalue_out[at, :, :HEAD] = (grad_key * scale).astype(jnp.bfloat16)
    keyvalue_out[at, :, HEAD:] = grad_value.astype(jnp.bfloat16)

    def back_tile(step, carry):
        columns = tile_at(step, size)
        store_part(
            part,
            columns,
            dense_right(query_out[at], w_query[columns, :])
            + dense_right(keyvalue_out[at], w_keyvalue[columns, :]),
        )
        return carry

    lax.fori_loop(0, w_query.shape[0] // size, back_tile, 0)


def half_of(ref, which):
    half = ref.shape[-2] // 2
    at = pl.ds(pl.multiple_of(which * half, half), half)
    return ref.at[at] if len(ref.shape) == 2 else ref.at[:, at]


def half_shape(shape):
    return shape[:-2] + (shape[-2] // 2, shape[-1])


def pass_kernel(compute, n_weights, n_ins, n_outs, places, side_axes, *refs):
    refs = list(refs)
    take = lambda count: [refs.pop(0) for _ in range(count)]
    (x_ref,) = take(1)
    early_weights = take(n_weights)
    late_weights = take(n_weights)
    ins = take(n_ins)
    side_from = take(len(side_axes))
    (y_ref,) = take(1)
    given = take(1 + n_outs)
    side_to = take(len(side_axes))
    kept = take(1 + n_outs)
    gath, outs = kept[0], kept[1:]
    weights = take(n_weights)
    part, partner_out, partner_in, total, line_out, from_left, from_right = take(7)
    (
        weight_sem, gather_right, gather_left, gather_partner, gather_line_in, gather_partner_in,
        partner_send, partner_recv, right_send, right_recv, left_send, left_recv,
        side_send, side_recv, given_sem,
    ) = take(15)

    section = lax.axis_index("section")
    me = lax.axis_index("dp")
    z = me // 2
    k = me % 2
    last = places - 1
    rows = x_ref.shape[0]
    size = rows // PARTS
    right = {"dp": me + 2}
    left = {"dp": me - 2}
    partner = {"dp": 2 * z + 1 - k}
    has_left = z > 0
    has_right = z < last

    barrier = pltpu.get_barrier_semaphore()
    pl.semaphore_signal(barrier, inc=1, device_id=partner, device_id_type=MESH)

    @pl.when(has_left)
    def _():
        pl.semaphore_signal(barrier, inc=1, device_id=left, device_id_type=MESH)

    @pl.when(has_right)
    def _():
        pl.semaphore_signal(barrier, inc=1, device_id=right, device_id_type=MESH)

    for index in range(n_weights):

        @pl.when(section == 0)
        def _():
            pltpu.make_async_copy(early_weights[index], weights[index], weight_sem.at[index]).start()

        @pl.when(section != 0)
        def _():
            pltpu.make_async_copy(late_weights[index], weights[index], weight_sem.at[index]).start()

    far = {"ctx": 1 - lax.axis_index("ctx"), "section": 1 - section}
    for axis in sorted(set(side_axes)):
        pl.semaphore_signal(barrier, inc=1, device_id={axis: far[axis]}, device_id_type=MESH)
    peers = 1 + len(set(side_axes)) + jnp.where(has_left, 1, 0) + jnp.where(has_right, 1, 0)
    pl.semaphore_wait(barrier, peers)

    sides = []
    for index, axis in enumerate(side_axes):
        source, target = side_from[index], side_to[index]
        if axis == "ctx":
            source = half_of(source, far["ctx"])
        sides.append(
            pltpu.make_async_remote_copy(
                source, target, side_send.at[index], side_recv.at[index],
                device_id={axis: far[axis]}, device_id_type=MESH,
            )
        )

    def cut(index):
        return pl.ds(index * size, size)

    def to_right(block, index, source):
        return pltpu.make_async_remote_copy(
            source, gath.at[block, k, cut(index)], gather_right.at[block, index],
            gather_line_in.at[block, index], device_id=right, device_id_type=MESH,
        )

    def to_left(block, index, source):
        return pltpu.make_async_remote_copy(
            source, gath.at[block, k, cut(index)], gather_left.at[block, index],
            gather_line_in.at[block, index], device_id=left, device_id_type=MESH,
        )

    def to_partner(block, source):
        return pltpu.make_async_remote_copy(
            source, gath.at[block, k], gather_partner.at[block],
            gather_partner_in.at[block], device_id=partner, device_id_type=MESH,
        )

    def sum_to_partner(block):
        return pltpu.make_async_remote_copy(
            partner_out.at[block], partner_in.at[block], partner_send.at[block],
            partner_recv.at[block], device_id=partner, device_id_type=MESH,
        )

    def sum_to_right(block, index):
        return pltpu.make_async_remote_copy(
            line_out.at[block, cut(index)], from_left.at[block, cut(index)],
            right_send.at[block, index], right_recv.at[block, index],
            device_id=right, device_id_type=MESH,
        )

    def sum_to_left(block, index):
        return pltpu.make_async_remote_copy(
            line_out.at[block, cut(index)], from_right.at[block, cut(index)],
            left_send.at[block, index], left_recv.at[block, index],
            device_id=left, device_id_type=MESH,
        )

    for index in range(PARTS):

        @pl.when(has_right)
        def _():
            to_right(z, index, x_ref.at[cut(index)]).start()

        @pl.when(has_left)
        def _():
            to_left(z, index, x_ref.at[cut(index)]).start()

    to_partner(z, x_ref).start()
    for copy in sides:
        copy.start()
    gath[z, k] = x_ref[...]

    at_end = (z == 0) | (z == last)
    low_half = z < places // 2

    def give(block):
        return [
            pltpu.make_async_copy(kept[index].at[block], given[index].at[block], given_sem.at[index, block])
            for index in range(1 + n_outs)
        ]

    def step(i, carry):
        inner_block = jnp.where(i == 0, 1, jnp.where(i == 1, 0, i))
        low_block = jnp.where(z == 0, i, inner_block)
        high_block = last - jnp.where(z == last, i, inner_block)
        block = jnp.where(low_half, low_block, high_block)
        wave = jnp.where(at_end, i, jnp.where(i == 1, 1, jnp.where(i == 3, 2, 0)))
        from_low = z - wave
        from_high = z + wave

        @pl.when((wave > 0) & (from_low >= 0))
        def _():
            for index in range(PARTS):
                to_right(from_low, index, gath.at[from_low, k, cut(index)]).wait_recv()

                @pl.when(has_right)
                def _():
                    to_right(from_low, index, gath.at[from_low, k, cut(index)]).start()

            to_partner(from_low, gath.at[from_low, k]).start()

        @pl.when((wave > 0) & (from_high <= last))
        def _():
            for index in range(PARTS):
                to_left(from_high, index, gath.at[from_high, k, cut(index)]).wait_recv()

                @pl.when(has_left)
                def _():
                    to_left(from_high, index, gath.at[from_high, k, cut(index)]).start()

            to_partner(from_high, gath.at[from_high, k]).start()

        pltpu.make_async_remote_copy(
            gath.at[block, 1 - k], gath.at[block, 1 - k], gather_partner.at[block],
            gather_partner_in.at[block], device_id=partner, device_id_type=MESH,
        ).wait_recv()

        @pl.when(i == 0)
        def _():
            for index in range(n_weights):
                pltpu.make_async_copy(
                    early_weights[index], weights[index], weight_sem.at[index]
                ).wait()

        compute(block, gath, part, weights, ins, outs)
        partner_out[block] = part[1 - k].astype(jnp.bfloat16)
        sum_to_partner(block).start()
        sum_to_partner(block).wait_recv()
        total[block] = part[k] + partner_in[block].astype(jnp.float32)

        for copy in give(block):
            copy.start()

        @pl.when((z == 0) & (block > 0))
        def _():
            line_out[block] = total[block].astype(jnp.bfloat16)
            for index in range(PARTS):
                sum_to_right(block, index).start()

        @pl.when((z == last) & (block < last))
        def _():
            line_out[block] = total[block].astype(jnp.bfloat16)
            for index in range(PARTS):
                sum_to_left(block, index).start()

        return carry

    lax.fori_loop(0, places, step, 0)

    n_left = jnp.where(has_left, places - z, 0)
    n_right = jnp.where(has_right, z + 1, 0)
    n_first = jnp.where(low_half, n_left, n_right)

    def finish(i, carry):
        in_first = i < n_first
        turn = jnp.where(in_first, i, i - n_first)
        is_left = in_first == low_half
        block = jnp.where(is_left, z + turn, z - turn)

        @pl.when(is_left)
        def _():
            for index in range(PARTS):
                sum_to_right(block, index).wait_recv()
                total[block, cut(index)] += from_left[block, cut(index)].astype(jnp.float32)

                @pl.when(block > z)
                def _():
                    line_out[block, cut(index)] = total[block, cut(index)].astype(jnp.bfloat16)
                    sum_to_right(block, index).start()

        @pl.when(jnp.logical_not(is_left))
        def _():
            for index in range(PARTS):
                sum_to_left(block, index).wait_recv()
                total[block, cut(index)] += from_right[block, cut(index)].astype(jnp.float32)

                @pl.when(block < z)
                def _():
                    line_out[block, cut(index)] = total[block, cut(index)].astype(jnp.bfloat16)
                    sum_to_left(block, index).start()

        return carry

    lax.fori_loop(0, n_left + n_right, finish, 0)
    y_ref[...] = total[z]

    def drain(block, carry):
        to_partner(block, gath.at[block, k]).wait_send()
        sum_to_partner(block).wait_send()
        for copy in give(block):
            copy.wait()
        for index in range(PARTS):

            @pl.when((block <= z) & has_right)
            def _():
                to_right(block, index, gath.at[block, k, cut(index)]).wait_send()

            @pl.when((block >= z) & has_left)
            def _():
                to_left(block, index, gath.at[block, k, cut(index)]).wait_send()

            @pl.when(block > z)
            def _():
                sum_to_right(block, index).wait_send()

            @pl.when(block < z)
            def _():
                sum_to_left(block, index).wait_send()

        return carry

    lax.fori_loop(0, places, drain, 0)
    for copy in sides:
        copy.wait()


def tensor_pass(compute, ident, x, early_weights, late_weights, ins, out_widths, sides=()):
    rows, width = x.shape
    places = lax.axis_size("dp") // 2
    vmem = pl.BlockSpec(memory_space=pltpu.VMEM)
    hbm = pl.BlockSpec(memory_space=pl.ANY)
    count = len(early_weights)
    dma = pltpu.SemaphoreType.DMA
    axes = [axis for axis, _ in sides]
    moved = [
        half_shape(array.shape) if axis == "ctx" else array.shape for axis, array in sides
    ]
    kernel = functools.partial(
        pass_kernel, compute, count, len(ins), len(out_widths), places, axes
    )
    call = pl.pallas_call(
        kernel,
        out_shape=[
            jax.ShapeDtypeStruct((rows, width), jnp.float32),
            jax.ShapeDtypeStruct((places, 2, rows, width), jnp.bfloat16),
        ]
        + [jax.ShapeDtypeStruct((places, 2 * rows, out), jnp.bfloat16) for out in out_widths]
        + [jax.ShapeDtypeStruct(shape, jnp.bfloat16) for shape in moved],
        in_specs=[vmem] + [hbm] * (2 * count) + [vmem] * len(ins) + [hbm] * len(axes),
        out_specs=[vmem] + [hbm] * (1 + len(out_widths) + len(axes)),
        scratch_shapes=[pltpu.VMEM((places, 2, rows, width), jnp.bfloat16)]
        + [pltpu.VMEM((places, 2 * rows, out), jnp.bfloat16) for out in out_widths]
        + [pltpu.VMEM(weight.shape, weight.dtype) for weight in early_weights]
        + [
            pltpu.VMEM((2, rows, width), jnp.float32),
            pltpu.VMEM((places, rows, width), jnp.bfloat16),
            pltpu.VMEM((places, rows, width), jnp.bfloat16),
            pltpu.VMEM((places, rows, width), jnp.float32),
            pltpu.VMEM((places, rows, width), jnp.bfloat16),
            pltpu.VMEM((places, rows, width), jnp.bfloat16),
            pltpu.VMEM((places, rows, width), jnp.bfloat16),
            dma((count,)),
            dma((places, PARTS)),
            dma((places, PARTS)),
            dma((places,)),
            dma((places, PARTS)),
            dma((places,)),
            dma((places,)),
            dma((places,)),
            dma((places, PARTS)),
            dma((places, PARTS)),
            dma((places, PARTS)),
            dma((places, PARTS)),
            dma((max(len(axes), 1),)),
            dma((max(len(axes), 1),)),
            dma((1 + len(out_widths), places)),
        ],
        cost_estimate=pl.CostEstimate(
            flops=60_000_000_000, bytes_accessed=20_000_000, transcendentals=0
        ),
        compiler_params=pltpu.CompilerParams(
            collective_id=ident, has_side_effects=True, vmem_limit_bytes=60 * 1024 * 1024
        ),
    )
    return call(
        x, *early_weights, *late_weights, *ins, *[array for _, array in sides]
    )


def distribute_kernel(
    places, query, keyvalue, notes, out, up, down,
    query_own, keyvalue_own, notes_own, up_own,
    query_far, keyvalue_far, notes_far, out_far, up_far, down_far,
    local_sem, query_send, query_recv, keyvalue_send, keyvalue_recv, notes_send, notes_recv,
    up_send, up_recv,
    across_send, across_recv, over_send, over_recv,
):
    section = lax.axis_index("section")
    ctx = lax.axis_index("ctx")
    me = lax.axis_index("dp")
    z = me // 2
    k = me % 2
    last = places - 1
    rows = query.shape[0]
    half = rows // 2
    head_width = query_own.shape[1]
    unit_width = up_own.shape[1]
    across = {"section": 1 - section}
    over = {"ctx": 1 - ctx}

    def group(away, act):
        if away == 0:
            act(2 * z + 1 - k)
            return

        @pl.when(z + away <= last)
        def _():
            act(2 * (z + away) + k)
            act(2 * (z + away) + 1 - k)

        @pl.when(z - away >= 0)
        def _():
            act(2 * (z - away) + k)
            act(2 * (z - away) + 1 - k)

    def peers(act):
        for away in range(places):
            group(away, act)

    def remote(source, target, send, recv, device):
        return pltpu.make_async_remote_copy(
            source, target, send, recv, device_id=device, device_id_type=MESH
        )

    def piece(owner, part, count):
        which = jnp.where(part == 0, ctx, 1 - ctx)
        return tile_at(2 * owner + which, count // 2)

    def query_copy(source, to):
        return remote(
            query.at[:, tile_at(to, head_width)], query_own.at[tile_at(source, rows)],
            query_send.at[to], query_recv.at[source], {"dp": to},
        )

    def keyvalue_copy(source, to):
        return remote(
            keyvalue, keyvalue_own.at[tile_at(source, rows)],
            keyvalue_send.at[to], keyvalue_recv.at[source], {"dp": to},
        )

    def notes_copy(source, to):
        return remote(
            notes, notes_own.at[tile_at(source, notes.shape[0])],
            notes_send.at[to], notes_recv.at[source], {"dp": to},
        )

    def up_copy(source, to, part):
        which = jnp.where(part == 0, ctx, 1 - ctx)
        return remote(
            up.at[tile_at(which, half), tile_at(to, unit_width)],
            up_own.at[piece(source, part, rows)],
            up_send.at[to, part], up_recv.at[source, part], {"dp": to},
        )

    barrier = pltpu.get_barrier_semaphore()

    def greet(to):
        pl.semaphore_signal(barrier, inc=1, device_id={"dp": to}, device_id_type=MESH)

    peers(greet)
    pl.semaphore_signal(barrier, inc=1, device_id=across, device_id_type=MESH)
    pl.semaphore_signal(barrier, inc=1, device_id=over, device_id_type=MESH)
    pl.semaphore_wait(barrier, 2 * places + 1)

    local = [
        pltpu.make_async_copy(
            query.at[:, tile_at(me, head_width)], query_own.at[tile_at(me, rows)], local_sem.at[0]
        ),
        pltpu.make_async_copy(keyvalue, keyvalue_own.at[tile_at(me, rows)], local_sem.at[1]),
        pltpu.make_async_copy(notes, notes_own.at[tile_at(me, notes.shape[0])], local_sem.at[2]),
        pltpu.make_async_copy(
            up.at[:, tile_at(me, unit_width)], up_own.at[tile_at(me, rows)], local_sem.at[3]
        ),
    ]
    for copy in local:
        copy.start()
    peers(lambda to: notes_copy(me, to).start())
    peers(lambda to: query_copy(me, to).start())
    peers(lambda to: keyvalue_copy(me, to).start())
    peers(lambda to: up_copy(me, to, 0).start())

    pieces = 2 * places
    out_half = tile_at(ctx, out.shape[0] // 2)
    short = down.shape[0] // 2 // pieces
    flows = [(out, out_far, out_half)] + [
        (down, down_far, tile_at(pieces * ctx + index, short)) for index in range(pieces)
    ]

    def flow_across(slot):
        source, target, at = flows[slot]
        return remote(
            source.at[at], target.at[at], across_send.at[slot], across_recv.at[slot], across
        )

    def flow_over(slot):
        _, target, at = flows[slot]
        return remote(target.at[at], target.at[at], over_send.at[slot], over_recv.at[slot], over)

    first_slot = len(flows)
    kinds = [
        (notes_own, notes_far, notes.shape[0]),
        (query_own, query_far, rows),
        (keyvalue_own, keyvalue_far, rows),
        (up_own, up_far, rows),
    ]

    def block_across(kind, owner):
        own, far, count = kinds[kind]
        slot = first_slot + kind * 2 * places + owner
        at = piece(owner, 0, count)
        return remote(own.at[at], far.at[at], across_send.at[slot], across_recv.at[slot], across)

    def block_over(kind, owner):
        _, far, count = kinds[kind]
        slot = first_slot + kind * 2 * places + owner
        at = piece(owner, 0, count)
        return remote(far.at[at], far.at[at], over_send.at[slot], over_recv.at[slot], over)

    for slot in range(first_slot):
        flow_across(slot).start()
    peers(lambda to: up_copy(me, to, 1).start())

    def hand_over(slot):
        flow_across(slot).wait_recv()
        flow_over(slot).start()

    for index in range(3):
        local[index].wait()
    block_across(0, me).start()
    block_across(1, me).start()
    block_across(2, me).start()
    hand_over(0)

    def pass_query(source):
        notes_copy(source, me).wait_recv()
        block_across(0, source).start()
        query_copy(source, me).wait_recv()
        block_across(1, source).start()

    def pass_keyvalue(source):
        keyvalue_copy(source, me).wait_recv()
        block_across(2, source).start()

    peers(pass_query)
    for slot in range(1, 1 + pieces // 2):
        hand_over(slot)
    peers(pass_keyvalue)
    for slot in range(1 + pieces // 2, first_slot):
        hand_over(slot)
    local[3].wait()
    block_across(3, me).start()

    def pass_up(source):
        up_copy(source, me, 0).wait_recv()
        block_across(3, source).start()

    def over_block(kind):
        def move(owner):
            block_across(kind, owner).wait_recv()
            block_over(kind, owner).start()

        return move

    group(0, pass_up)
    group(1, pass_up)
    for kind in range(3):
        over_block(kind)(me)
        peers(over_block(kind))
    over_block(3)(me)
    for away in range(2, places):
        group(away, pass_up)
        group(away - 2, over_block(3))
    group(places - 2, over_block(3))
    group(places - 1, over_block(3))

    peers(lambda source: up_copy(source, me, 1).wait_recv())

    def over_wait(slot_owner, carry):
        for kind in range(len(kinds)):
            block_over_in(kind, slot_owner).wait_recv()
            block_across(kind, slot_owner).wait_send()
            block_over(kind, slot_owner).wait_send()
        return carry

    def block_over_in(kind, owner):
        _, far, count = kinds[kind]
        slot = first_slot + kind * 2 * places + owner
        at = piece(owner, 1, count)
        return remote(far.at[at], far.at[at], over_send.at[slot], over_recv.at[slot], over)

    lax.fori_loop(0, 2 * places, over_wait, 0)
    for slot in range(first_slot):
        flow_over(slot).wait_recv()
        flow_across(slot).wait_send()
        flow_over(slot).wait_send()

    def sent(to):
        notes_copy(me, to).wait_send()
        query_copy(me, to).wait_send()
        keyvalue_copy(me, to).wait_send()
        up_copy(me, to, 0).wait_send()
        up_copy(me, to, 1).wait_send()

    peers(sent)


def distribute(query, keyvalue, notes, out, up, down):
    size = lax.axis_size("dp")
    places = size // 2
    hbm = pl.BlockSpec(memory_space=pl.ANY)
    dma = pltpu.SemaphoreType.DMA
    rows = query.shape[0] * size
    small = [
        (rows, query.shape[1] // size),
        (rows, keyvalue.shape[1]),
        (notes.shape[0] * size, notes.shape[1]),
    ]
    turned = (rows, up.shape[1] // size)
    shapes = small + [turned] + small + [out.shape, turned, down.shape]
    slots = 1 + 5 * size
    return pl.pallas_call(
        functools.partial(distribute_kernel, places),
        name="distribute",
        out_shape=[jax.ShapeDtypeStruct(shape, jnp.bfloat16) for shape in shapes],
        in_specs=[hbm] * 6,
        out_specs=[hbm] * len(shapes),
        scratch_shapes=[dma((4,))]
        + [dma((size,))] * 6
        + [dma((size, 2))] * 2
        + [dma((slots,))] * 4,
        cost_estimate=pl.CostEstimate(
            flops=150_000_000_000, bytes_accessed=20_000_000, transcendentals=0
        ),
        compiler_params=pltpu.CompilerParams(collective_id=4, has_side_effects=True),
    )(query, keyvalue, notes, out, up, down)


def collect_kernel(
    places, up_full, down_full, query_full, out_full, up_moved, down_moved,
    up_late, down_late, query_late, out_late, up_far, down_far, query_far, out_far, small,
    up_out, down_out, query_out, out_out, small_out,
    small_in, small_sum, small_far, small_total, small_side,
    up, up_in, up_part, up_side, down, down_in, down_part, down_side,
    query, query_in, query_part, query_side, out, out_in, out_part, out_side,
    local_sem, side_send, side_recv, across_send, across_recv,
    turn_send, turn_recv, over_send, over_recv, small_send, small_recv,
):
    section = lax.axis_index("section")
    ctx = lax.axis_index("ctx")
    me = lax.axis_index("dp")
    z = me // 2
    k = me % 2
    last = places - 1
    size = 2 * places
    early = section == 0
    late = section != 0
    across = {"section": 1 - section}
    over = {"ctx": 1 - ctx}
    chunks = 4
    short = down.shape[0] // chunks
    turned = [(up, up_out), (query, query_out)]
    half = up.shape[1]

    def group(away, act):
        if away == 0:
            act(2 * z + 1 - k)
            return

        @pl.when(z + away <= last)
        def _():
            act(2 * (z + away) + k)
            act(2 * (z + away) + 1 - k)

        @pl.when(z - away >= 0)
        def _():
            act(2 * (z - away) + k)
            act(2 * (z - away) + 1 - k)

    def peers(act):
        for away in range(places):
            group(away, act)

    def remote(source, target, send, recv, device):
        return pltpu.make_async_remote_copy(
            source, target, send, recv, device_id=device, device_id_type=MESH
        )

    barrier = pltpu.get_barrier_semaphore()

    def greet(to):
        pl.semaphore_signal(barrier, inc=1, device_id={"dp": to}, device_id_type=MESH)

    peers(greet)
    pl.semaphore_signal(barrier, inc=1, device_id=across, device_id_type=MESH)
    pl.semaphore_signal(barrier, inc=1, device_id=over, device_id_type=MESH)
    pl.semaphore_wait(barrier, size + 1)

    side = [
        remote(half_of(query_full, 1 - ctx), query_side, side_send.at[0], side_recv.at[0], over),
        remote(half_of(out_full, 1 - ctx), out_side, side_send.at[1], side_recv.at[1], over),
    ]
    for copy in side:
        copy.start()

    def small_turn(source, to, layer):
        return remote(
            small.at[layer, to], small_in.at[layer, source],
            small_send.at[layer, to], small_recv.at[layer, source], {"dp": to},
        )

    own_small = [
        pltpu.make_async_copy(
            small.at[layer, me], small_in.at[layer, me], local_sem.at[13 + layer]
        )
        for layer in range(2)
    ]
    for layer in range(2):
        own_small[layer].start()

    def small_start(to):
        for layer in range(2):
            small_turn(me, to, layer).start()

    def small_wait(source):
        for layer in range(2):
            small_turn(source, me, layer).wait_recv()

    def small_sent(to):
        for layer in range(2):
            small_turn(me, to, layer).wait_send()

    small_across = remote(
        small_sum.at[1 - section], small_far, across_send.at[size + 6], across_recv.at[size + 6],
        across,
    )
    small_over = remote(small_total, small_side, side_send.at[2], side_recv.at[2], over)

    def up_across(owner):
        return remote(
            up_part.at[owner], up_in.at[owner], across_send.at[owner], across_recv.at[owner], across
        )

    def down_across(index):
        slot = size + index
        at = pl.ds(index * short, short)
        return remote(
            down_part.at[at], down_in.at[at], across_send.at[slot], across_recv.at[slot], across
        )

    query_across = remote(
        query_part, query_in, across_send.at[size + chunks], across_recv.at[size + chunks], across
    )
    out_across = remote(
        out_part, out_in, across_send.at[size + chunks + 1], across_recv.at[size + chunks + 1],
        across,
    )

    def load(index, source, target):
        copy = pltpu.make_async_copy(source, target, local_sem.at[index])
        copy.start()
        return copy

    loads = [
        load(0, half_of(up_full, ctx), up_part),
        load(1, up_moved, up_side),
        load(2, half_of(query_full, ctx), query_part),
        load(3, half_of(out_full, ctx), out_part),
        load(4, half_of(down_full, ctx), down_part),
        load(5, down_moved, down_side),
    ]
    owned = [
        (up_late, up), (up_far, up_in), (query_late, query), (query_far, query_in),
        (out_late, out), (out_far, out_in), (down_late, down), (down_far, down_in),
    ]

    @pl.when(late)
    def _():
        for index, (source, target) in enumerate(owned):
            load(15 + index, source, target)

    loads[0].wait()
    loads[1].wait()

    def send_up(owner):
        up_part[owner] = up_part[owner] + up_side[owner]

        @pl.when(late)
        def _():
            up_across(owner).start()

    peers(send_up)
    send_up(me)
    loads[2].wait()
    loads[3].wait()
    for copy in side:
        copy.wait_recv()
    query_part[...] = query_part[...] + query_side[...]
    out_part[...] = out_part[...] + out_side[...]
    loads[4].wait()
    loads[5].wait()
    down_part[...] = down_part[...] + down_side[...]

    @pl.when(late)
    def _():
        query_across.start()
        out_across.start()
        for index in range(chunks):
            down_across(index).start()
        for index, (source, target) in enumerate(owned):
            pltpu.make_async_copy(source, target, local_sem.at[15 + index]).wait()

    def turn(kind, source, to):
        block, target = turned[kind]
        width = block.shape[2]
        at = kind * size
        return remote(
            block.at[to], target.at[tile_at(ctx, half), tile_at(source, width)],
            turn_send.at[at + to], turn_recv.at[at + source], {"dp": to},
        )

    def own_block(kind):
        block, target = turned[kind]
        return pltpu.make_async_copy(
            block.at[me], target.at[tile_at(ctx, half), tile_at(me, block.shape[2])],
            local_sem.at[6 + kind],
        )

    def hand_over(kind, source, side_of):
        block, target = turned[kind]
        at = kind * size + source
        region = target.at[tile_at(side_of, half), tile_at(source, block.shape[2])]
        return remote(region, region, over_send.at[at], over_recv.at[at], over)

    def sum_up(owner):
        @pl.when(early)
        def _():
            up_across(owner).wait_recv()
            up[owner] = up_part[owner] + up_in[owner]

        @pl.when(late)
        def _():
            up[owner] = up[owner] + up_in[owner]

    def up_block(owner):
        sum_up(owner)
        turn(0, me, owner).start()

    def arrived(kind):
        def act(source):
            turn(kind, source, me).wait_recv()
            hand_over(kind, source, ctx).start()

        return act

    for away in range(places):
        group(away, up_block)
        if away > 0:
            group(away - 1, arrived(0))
    sum_up(me)
    peers(small_start)
    own_block(0).start()
    group(last, arrived(0))
    own_block(0).wait()
    hand_over(0, me, ctx).start()

    @pl.when(early)
    def _():
        query_across.wait_recv()
        query[...] = query_part[...] + query_in[...]
        out_across.wait_recv()
        out[...] = out_part[...] + out_in[...]

    @pl.when(late)
    def _():
        query[...] = query[...] + query_in[...]
        out[...] = out[...] + out_in[...]

    peers(lambda owner: turn(1, me, owner).start())
    own_block(1).start()

    def flat_over(index, side_of):
        slot = 2 * size + index
        if index == 0:
            source, target, at = out, out_out, tile_at(side_of, out.shape[0])
            return remote(source, target.at[at], over_send.at[slot], over_recv.at[slot], over), (
                pltpu.make_async_copy(source, target.at[at], local_sem.at[8])
            )
        source = down.at[pl.ds((index - 1) * short, short)]
        target = down_out.at[tile_at(side_of * chunks + index - 1, short)]
        return remote(source, target, over_send.at[slot], over_recv.at[slot], over), (
            pltpu.make_async_copy(source, target, local_sem.at[8 + index])
        )

    for copy in flat_over(0, ctx):
        copy.start()
    for index in range(chunks):

        @pl.when(early)
        def _():
            at = pl.ds(index * short, short)
            down_across(index).wait_recv()
            down[at] = down_part[at] + down_in[at]

        @pl.when(late)
        def _():
            at = pl.ds(index * short, short)
            down[at] = down[at] + down_in[at]

        for copy in flat_over(1 + index, ctx):
            copy.start()
    peers(arrived(1))
    own_block(1).wait()
    hand_over(1, me, ctx).start()
    for layer in range(2):
        own_small[layer].wait()
    peers(small_wait)
    for layer in range(2):
        total = small_in[layer, 0].astype(jnp.float32)
        for source in range(1, size):
            total = total + small_in[layer, source].astype(jnp.float32)
        small_sum[layer] = total.astype(jnp.bfloat16)
    small_across.start()


    small_across.wait_recv()
    small_total[...] = small_sum[section] + small_far[...]
    small_over.start()
    small_over.wait_recv()
    small_out[...] = (small_total[...] + small_side[...]).astype(jnp.float32)

    peers(small_sent)
    small_across.wait_send()
    small_over.wait_send()
    for copy in side:
        copy.wait_send()

    @pl.when(late)
    def _():
        peers(lambda owner: up_across(owner).wait_send())
        up_across(me).wait_send()
        query_across.wait_send()
        out_across.wait_send()
        for index in range(chunks):
            down_across(index).wait_send()

    for kind in range(2):
        peers(lambda owner: turn(kind, me, owner).wait_send())

        def finish(source, carry):
            hand_over(kind, source, ctx).wait_send()
            hand_over(kind, source, 1 - ctx).wait_recv()
            return carry

        lax.fori_loop(0, size, finish, 0)
    for index in range(1 + chunks):
        moved, kept = flat_over(index, ctx)
        kept.wait()
        moved.wait_send()
        flat_over(index, 1 - ctx)[0].wait_recv()


def collect(fulls, moved, late, far, small):
    size = lax.axis_size("dp")
    hbm = pl.BlockSpec(memory_space=pl.ANY)
    dma = pltpu.SemaphoreType.DMA
    vmem = lambda x: pltpu.VMEM(x.shape, x.dtype)
    up, down, query, out = fulls
    shapes = [
        (up.shape[1], size * up.shape[2]),
        down.shape,
        (query.shape[1], size * query.shape[2]),
        out.shape,
    ]
    return pl.pallas_call(
        functools.partial(collect_kernel, size // 2),
        name="collect",
        out_shape=[jax.ShapeDtypeStruct(shape, jnp.bfloat16) for shape in shapes]
        + [jax.ShapeDtypeStruct(small.shape[2:], jnp.float32)],
        in_specs=[hbm] * 15,
        out_specs=[hbm] * 4 + [pl.BlockSpec(memory_space=pltpu.VMEM)],
        scratch_shapes=[vmem(small), vmem(small[:, 0])]
        + [vmem(small[0, 0])] * 3
        + [vmem(x) for x in late for _ in range(4)]
        + [dma((23,)), dma((3,)), dma((3,))]
        + [dma((size + 7,))] * 2
        + [dma((2 * size,))] * 2
        + [dma((2 * size + 5,))] * 2
        + [dma((2, size))] * 2,
        cost_estimate=pl.CostEstimate(
            flops=120_000_000_000, bytes_accessed=20_000_000, transcendentals=0
        ),
        compiler_params=pltpu.CompilerParams(collective_id=5, has_side_effects=True),
    )(*fulls, *moved, *late, *far, small)


def swapped(size):
    pairs = []
    for ctx in range(2):
        for at in range(size):
            z, k = at // 2, at % 2
            pairs.append((ctx * size + at, k * size + 2 * z + ctx))
    return pairs


def regroup(x):
    return lax.ppermute(x, ("ctx", "dp"), swapped(lax.axis_size("dp")))


def regroup_across(x):
    size = lax.axis_size("dp")
    half = 2 * size
    pairs = swapped(size)
    across = [(a, b + half) for a, b in pairs] + [(a + half, b) for a, b in pairs]
    return lax.ppermute(x, ("section", "ctx", "dp"), across)


def own_half(grad):
    half = grad.shape[-2] // 2
    return lax.dynamic_slice_in_dim(grad, lax.axis_index("ctx") * half, half, axis=-2)


def spread_body(*args):
    return spread_step(*args)


def spread_step(
    tokens, cotangent, segment_ids, w_query, w_keyvalue, w_out, w_up, w_down, ln_gains, ln_biases
):
    section = lax.axis_index("section")
    ctx = lax.axis_index("ctx")
    size = lax.axis_size("dp")
    places = size // 2
    early = section == 0
    width = tokens.shape[3]
    length = segment_ids.shape[2]
    tall = (places * tokens.shape[2] * 2, -1)

    def own_micro(x):
        return lax.dynamic_index_in_dim(x, section, 0, keepdims=False)[0]

    hidden = regroup(own_micro(tokens)).astype(jnp.float32)
    out, down = w_out[0], w_down[0]
    columns = ln_gains.shape[2]
    notes = jnp.concatenate(
        [ln_gains[0], ln_biases[0], own_micro(segment_ids).astype(jnp.bfloat16)[None]], axis=0
    )
    notes = jnp.pad(notes, ((0, 32 - notes.shape[0]), (0, 0)))
    query, keyvalue, notes, up, query_far, keyvalue_far, notes_far, out_far, up_far, down_far = (
        distribute(w_query[0], w_keyvalue[0], notes, out, w_up[0], down)
    )
    notes = notes.reshape(size, 32, columns).transpose(1, 0, 2)
    near = notes[:4].reshape(4, width).astype(jnp.float32)
    far = notes_far.reshape(size, 32, columns).transpose(1, 0, 2)[:4].reshape(4, width)
    far = far.astype(jnp.float32)
    scales = [jnp.where(early, near, far), jnp.where(early, far, near)]
    segments = notes[4].astype(jnp.int32).reshape(places, 2, length)
    segments = lax.dynamic_index_in_dim(segments, ctx, 1, keepdims=False)
    segs = [segments[:, :, None], segments[:, None, :]]
    attention_near, attention_far = [query, keyvalue, out], [query_far, keyvalue_far, out_far]
    attention_weights = [(attention_near, attention_far), (attention_far, attention_near)]
    ffn_weights = [([up, down], [up_far, down_far]), ([up_far, down_far], [up, down])]
    head_width = query.shape[1]
    unit_width = up.shape[1]

    def forward(layer, hidden):
        normed = layer_norm(hidden, scales[layer][0], scales[layer][2]).astype(jnp.bfloat16)
        y, normed_all, q, kv, mixed = tensor_pass(
            attention_forward_at, 0, normed, *attention_weights[layer], segs,
            [head_width, keyvalue.shape[1], head_width],
        )
        after = hidden + y
        normed_two = layer_norm(after, scales[layer][1], scales[layer][3]).astype(jnp.bfloat16)
        y, normed_two_all, up_rows, activated = tensor_pass(
            ffn_forward_at, 1, normed_two, *ffn_weights[layer], [],
            [unit_width, unit_width],
        )
        result = (after + y).astype(jnp.bfloat16)
        return result, (hidden, normed_all, q, kv, mixed, after, normed_two_all, up_rows, activated)

    def product(left, right):
        return dense_left(left.reshape(tall), right.reshape(tall)).astype(jnp.bfloat16)

    def rows_of_all(grad):
        return grad.reshape(size, grad.shape[0] // size, grad.shape[1])

    def ffn_backward(layer, ident, grad_low, kept, sides):
        _, _, _, _, _, after, normed_two_all, up_rows, activated = kept
        y, grad_low_all, grad_upper, *arrived = tensor_pass(
            ffn_backward_at, ident, grad_low, *ffn_weights[layer],
            [up_rows], [unit_width], sides,
        )
        grads = [
            rows_of_all(product(normed_two_all, grad_upper)),
            product(activated, grad_low_all),
        ]
        _, norm_back = jax.vjp(layer_norm, after, scales[layer][1], scales[layer][3])
        grad_norm, gain, bias = norm_back(y)
        return grad_low.astype(jnp.float32) + grad_norm, grads, [gain, bias], arrived

    def attention_backward(layer, ident, grad_after, grad_branch, kept, sides):
        hidden, normed_all, q, kv, mixed, _, _, _, _ = kept
        y, grad_branch_all, grad_query, grad_kv, *arrived = tensor_pass(
            attention_backward_at, ident, grad_branch,
            *attention_weights[layer], segs + [q, kv], [head_width, keyvalue.shape[1]], sides,
        )
        grads = [
            rows_of_all(product(normed_all, grad_query)),
            product(mixed, grad_branch_all),
        ]
        keyvalue_grad = product(normed_all, grad_kv)
        _, norm_back = jax.vjp(layer_norm, hidden, scales[layer][0], scales[layer][2])
        grad_norm, gain, bias = norm_back(y)
        return (
            (grad_after + grad_norm).astype(jnp.bfloat16), grads, keyvalue_grad, [gain, bias], arrived
        )

    def low(x):
        return x.astype(jnp.bfloat16)

    def ctx_sums(grads, arrived):
        return [own_half(grad) + other for grad, other in zip(grads, arrived)]

    def both_rows(one, two):
        near = regroup(jnp.where(early, one, two))
        far = regroup_across(jnp.where(early, two, one))
        return jnp.stack([jnp.where(early, near, far), jnp.where(early, far, near)])[None, :, None]

    hold = lax.optimization_barrier
    first, kept_first = forward(0, hidden)
    second, kept_second = forward(1, first.astype(jnp.float32))
    section_rows = both_rows(first, second)
    grad_low = regroup(own_micro(cotangent))

    def sides(axis, arrays):
        return [(axis, array) for array in arrays]

    grad_after, ffn_two, scales_two, _ = ffn_backward(1, 2, grad_low, kept_second, [])
    branch, up_two, down_two = hold((low(grad_after), *ffn_two))
    grad_second, attention_two, keyvalue_two, more, arrived = attention_backward(
        1, 3, grad_after, branch, kept_second, sides("ctx", [up_two])
    )
    scales_two = more[:1] + scales_two[:1] + more[1:] + scales_two[1:]
    (up_two,) = ctx_sums([up_two], arrived)
    grad_after, ffn_one, scales_one, arrived = ffn_backward(
        0, 6, grad_second, kept_first,
        sides("section", [up_two]) + sides("ctx", [down_two] + attention_two),
    )
    up_two_far = arrived[0]
    down_two, *attention_two = ctx_sums([down_two] + attention_two, arrived[1:])
    branch, *both = hold((low(grad_after), *ffn_one, down_two, *attention_two))
    ffn_one, rest_two = both[:2], both[2:]
    grad_first, attention_one, keyvalue_one, more, arrived = attention_backward(
        0, 7, grad_after, branch, kept_first,
        sides("ctx", ffn_one) + sides("section", rest_two),
    )
    scales_one = more[:1] + scales_one[:1] + more[1:] + scales_one[1:]
    ffn_moved, rest_far = arrived[:2], arrived[2:]

    def small_of(keyvalue_grad, rows):
        rows = low(jnp.stack(rows)).reshape(4, size, columns).transpose(1, 0, 2)
        rows = jnp.pad(rows, ((0, 0), (0, 12), (0, 0)))
        return jnp.concatenate([keyvalue_grad.reshape(size, columns, -1), rows], axis=1)

    small = jnp.stack([small_of(keyvalue_one, scales_one), small_of(keyvalue_two, scales_two)])
    up_grad, down_grad, query_grad, out_grad, small = collect(
        ffn_one + attention_one, ffn_moved, [up_two] + rest_two, [up_two_far] + rest_far, small,
    )
    scale_grads = small[None, columns : columns + 4]

    def given(grad):
        return grad.astype(jnp.float32)[None]

    return (
        section_rows,
        both_rows(grad_first, grad_second),
        given(query_grad),
        small[None, :columns],
        given(out_grad),
        given(up_grad),
        given(down_grad),
        scale_grads[:, 0:2],
        scale_grads[:, 2:4],
    )


def from_behind(x, axis, by):
    devices = lax.axis_size(axis)
    pairs = [(i, i + by) for i in range(devices) if 0 <= i + by < devices]
    return lax.ppermute(x, axis, pairs)


def allowed_keys(segments, cycle_place, cycle_size, tok_rows):
    offsets = jnp.arange(tok_rows, dtype=jnp.int32)
    query_pos = cycle_place * tok_rows + offsets
    query_seg = lax.dynamic_slice_in_dim(segments, cycle_place * tok_rows, tok_rows, axis=1)
    blocks = []
    for cycle_step in range(cycle_size):
        source = cycle_place - cycle_step
        key_pos = source * tok_rows + offsets
        key_seg = lax.dynamic_slice_in_dim(
            segments, jnp.maximum(source, 0) * tok_rows, tok_rows, axis=1
        )
        blocks.append(
            (source >= 0)
            & (key_pos[None, None, :] <= query_pos[None, :, None])
            & (key_seg[:, None, :] == query_seg[:, :, None])
        )
    return jnp.concatenate(blocks, axis=2)


def batched(left, right, left_dim, right_dim):
    return lax.dot_general(
        left, right, (((left_dim,), (right_dim,)), ((0,), (0,))), preferred_element_type=jnp.float32
    )


def head_scores(query, keyvalue_all, allowed):
    micro, rows, _ = allowed.shape
    head_rows = query.reshape(micro, rows * HEADS, HEAD)
    scores = batched(head_rows, keyvalue_all[:, :, :HEAD], 2, 2) * HEAD ** (-0.5)
    scores = scores.reshape(micro, rows, HEADS, -1)
    scores = jnp.where(allowed[:, :, None, :], scores, masked_score)
    return (scores.reshape(micro, rows * HEADS, -1), head_rows)


def layer_forward(hidden, segments, weights, micro, cycle_place, cycle_size):
    w_query, w_keyvalue, w_out, w_up, w_down, gains, biases = weights
    rows = hidden.shape[0] // micro
    normed = layer_norm(hidden, gains[0], biases[0]).astype(jnp.bfloat16)
    query = dense(normed, w_query).astype(jnp.bfloat16)
    keyvalue = dense(normed, w_keyvalue).astype(jnp.bfloat16)
    moving = from_behind(keyvalue, "ctx", 1)
    keyvalue_all = jnp.concatenate(
        [keyvalue.reshape(micro, rows, -1), moving.reshape(micro, rows, -1)], axis=1
    )
    allowed = allowed_keys(segments, cycle_place, cycle_size, rows)
    scores, _ = head_scores(query, keyvalue_all, allowed)
    top_score = jnp.max(scores, axis=2, keepdims=True)
    log_total = top_score + jnp.log(jnp.sum(jnp.exp(scores - top_score), axis=2, keepdims=True))
    attn_probs = jnp.exp(scores - log_total).astype(jnp.bfloat16)
    mixed = (
        batched(attn_probs, keyvalue_all[:, :, HEAD:], 2, 1)
        .reshape(micro * rows, HEADS * HEAD)
        .astype(jnp.bfloat16)
    )
    after = hidden + dense(mixed, w_out)
    normed_two = layer_norm(after, gains[1], biases[1]).astype(jnp.bfloat16)
    up_rows = dense(normed_two, w_up)
    activated = jax.nn.gelu(up_rows, approximate=True).astype(jnp.bfloat16)
    result = after + dense(activated, w_down)
    kept = (
        hidden,
        normed,
        query,
        keyvalue_all,
        log_total,
        mixed,
        after,
        normed_two,
        up_rows,
        activated,
    )
    return (result, kept)


def layer_backward(grad_result, kept, segments, weights, micro, cycle_place, cycle_size):
    w_query, w_keyvalue, w_out, w_up, w_down, gains, biases = weights
    hidden, normed, query, keyvalue_all, log_total, mixed, after, normed_two, up_rows, activated = (
        kept
    )
    rows = hidden.shape[0] // micro
    grad_low = grad_result.astype(jnp.bfloat16)
    grad_act = dense_right(grad_low, w_down)
    _, gelu_back = jax.vjp(lambda entries: jax.nn.gelu(entries, approximate=True), up_rows)
    grad_upper = gelu_back(grad_act)[0].astype(jnp.bfloat16)
    _, norm_back_two = jax.vjp(layer_norm, after, gains[1], biases[1])
    grad_after_norm, grad_gain_two, grad_bias_two = norm_back_two(dense_right(grad_upper, w_up))
    grad_after = grad_result + grad_after_norm
    grad_branch = grad_after.astype(jnp.bfloat16)
    grad_mixed = (
        dense_right(grad_branch, w_out).astype(jnp.bfloat16).reshape(micro, rows * HEADS, HEAD)
    )
    allowed = allowed_keys(segments, cycle_place, cycle_size, rows)
    scores, head_rows = head_scores(query, keyvalue_all, allowed)
    attn_probs = jnp.exp(scores - log_total)
    grad_probs = batched(grad_mixed, keyvalue_all[:, :, HEAD:], 2, 2)
    grad_values = batched(attn_probs.astype(jnp.bfloat16), grad_mixed, 1, 1)
    inner = jnp.sum(attn_probs * grad_probs, axis=2, keepdims=True)
    grad_scores = (attn_probs * (grad_probs - inner)).astype(jnp.bfloat16)
    scale_factor = HEAD ** (-0.5)
    grad_queries = (
        (batched(grad_scores, keyvalue_all[:, :, :HEAD], 2, 1) * scale_factor)
        .astype(jnp.bfloat16)
        .reshape(micro * rows, HEADS * HEAD)
    )
    grad_keys = batched(grad_scores, head_rows, 1, 1) * scale_factor
    grad_pieces = jnp.concatenate([grad_keys, grad_values], axis=2)
    carried = grad_pieces[:, (cycle_size - 1) * rows :]
    carried = (
        from_behind(carried.astype(jnp.bfloat16), "ctx", -1).astype(carried.dtype)
        + grad_pieces[:, 0:rows]
    )
    grad_kv = carried.astype(jnp.bfloat16).reshape(micro * rows, -1)
    grad_normed = dense_right(grad_queries, w_query) + dense_right(grad_kv, w_keyvalue)
    _, norm_back_one = jax.vjp(layer_norm, hidden, gains[0], biases[0])
    grad_hidden, grad_gain_one, grad_bias_one = norm_back_one(grad_normed)
    grad_input = grad_after + grad_hidden
    terms = (
        normed,
        grad_queries,
        grad_kv,
        mixed,
        grad_branch,
        normed_two,
        grad_upper,
        activated,
        grad_low,
        jnp.stack([grad_gain_one, grad_gain_two, grad_bias_one, grad_bias_two]),
    )
    return (grad_input, terms)


def body(
    tokens, cotangent, segment_ids, w_query, w_keyvalue, w_out, w_up, w_down, ln_gains, ln_biases
):
    section_index = lax.axis_index("section")
    cycle_place = lax.axis_index("ctx")
    cycle_size = lax.axis_size("ctx")
    micro = tokens.shape[0]
    width = tokens.shape[3]
    early = section_index == 0
    segments = segment_ids[:, 0]
    own_tokens = tokens[:, 0].reshape(-1, width)
    own_cotangent = cotangent[:, 0].reshape(-1, width)

    def spread(weight):
        half = weight.shape[1] // cycle_size
        part = lax.dynamic_slice_in_dim(weight, cycle_place * half, half, axis=1)
        return lax.all_gather(part, ("dp", "ctx"), axis=1, tiled=True)[0]

    scales = lax.all_gather(
        jnp.concatenate([ln_gains, ln_biases], axis=1), "dp", axis=2, tiled=True
    )[0].astype(jnp.float32)
    weights = (
        spread(w_query),
        lax.all_gather(w_keyvalue, "dp", axis=1, tiled=True)[0],
        spread(w_out),
        spread(w_up),
        spread(w_down),
        scales[0:2],
        scales[2:4],
    )
    result, kept_first = layer_forward(
        own_tokens.astype(jnp.float32), segments, weights, micro, cycle_place, cycle_size
    )
    first_low = result.astype(jnp.bfloat16)
    incoming = from_behind(first_low, "section", 1)
    result, kept_second = layer_forward(
        incoming.astype(jnp.float32), segments, weights, micro, cycle_place, cycle_size
    )
    second_low = result.astype(jnp.bfloat16)
    grad, terms_second = layer_backward(
        own_cotangent.astype(jnp.float32), kept_second, segments, weights, micro, cycle_place,
        cycle_size,
    )
    grad_second = grad.astype(jnp.bfloat16)
    arriving = from_behind(grad_second, "section", -1)
    grad, terms_first = layer_backward(
        arriving.astype(jnp.float32), kept_first, segments, weights, micro, cycle_place, cycle_size
    )
    grad_first = grad.astype(jnp.bfloat16)
    section_rows = jnp.where(early, first_low, second_low)
    grad_rows = jnp.where(early, grad_first, grad_second)
    (
        normed_all,
        grad_queries_all,
        grad_kv_all,
        mixed_all,
        grad_branch_all,
        normed_two_all,
        grad_upper_all,
        activated_all,
        grad_low_all,
        scale_terms,
    ) = [jnp.where(early, one, two) for one, two in zip(terms_first, terms_second)]

    def reduced(left, right):
        part = dense_left(left, right).astype(jnp.bfloat16)
        piece = lax.psum_scatter(part, ("dp", "ctx"), scatter_dimension=0, tiled=True)
        return lax.all_gather(piece, "ctx", axis=0, tiled=True).astype(jnp.float32)[None]

    grad_down = reduced(activated_all, grad_low_all)
    grad_up = reduced(normed_two_all, grad_upper_all)
    grad_out = reduced(mixed_all, grad_branch_all)
    grad_query = reduced(normed_all, grad_queries_all)
    grad_keyvalue = reduced(normed_all, grad_kv_all)
    scale_grads = lax.psum(
        lax.psum_scatter(
            scale_terms.astype(jnp.bfloat16), "dp", scatter_dimension=1, tiled=True
        ),
        "ctx",
    ).astype(jnp.float32)[None]
    local = (1, micro, 1, own_tokens.shape[0] // micro, width)
    return (
        section_rows.reshape(local),
        grad_rows.reshape(local),
        grad_query,
        grad_keyvalue,
        grad_out,
        grad_up,
        grad_down,
        scale_grads[:, 0:2],
        scale_grads[:, 2:4],
    )


def solution(mesh):
    in_specs = (
        P(None, "dp", "ctx", None),
        P(None, "dp", "ctx", None),
        P(None, "dp", None),
        P("section", "dp", None),
        P("section", "dp", None),
        P("section", "dp", None),
        P("section", "dp", None),
        P("section", "dp", None),
        P("section", None, "dp"),
        P("section", None, "dp"),
    )
    out_specs = (
        P("section", None, "dp", "ctx", None),
        P("section", None, "dp", "ctx", None),
        P("section", "dp", None),
        P("section", "dp", None),
        P("section", "dp", None),
        P("section", "dp", None),
        P("section", "dp", None),
        P("section", None, "dp"),
        P("section", None, "dp"),
    )
    spread = mesh.shape["dp"] == 8
    return jax.shard_map(
        spread_body if spread else body,
        mesh=mesh, in_specs=in_specs, out_specs=out_specs, check_vma=False,
    )
```

```python
import functools
import math

import jax
import jax.numpy as jnp
from jax import lax
from jax.experimental import pallas as pl
from jax.experimental.pallas import tpu as pltpu
from jax.sharding import PartitionSpec as P

HEADS = 16
HEAD = 128


epsilon = 1e-05
masked_score = -1000000000.0


def layer_norm(values_in, gain_row, bias_row):
    mean_row = jnp.mean(values_in, axis=-1, keepdims=True)
    centered = values_in - mean_row
    variance = jnp.mean(centered * centered, axis=-1, keepdims=True)
    return centered * lax.rsqrt(variance + epsilon) * gain_row + bias_row


def dense(left, right):
    return jnp.dot(left, right, preferred_element_type=jnp.float32)


def dense_left(left, right):
    return lax.dot_general(
        left, right, (((0,), (0,)), ((), ())), preferred_element_type=jnp.float32
    )


def dense_right(left, right):
    return lax.dot_general(
        left, right, (((1,), (1,)), ((), ())), preferred_element_type=jnp.float32
    )


MESH = pl.DeviceIdType.MESH
PARTS = 4


def gelu(v):
    inner = math.sqrt(2.0 / math.pi) * (v + 0.044715 * v * v * v)
    return 0.5 * v * (1.0 + jnp.tanh(inner))


def gelu_slope(v):
    scale = math.sqrt(2.0 / math.pi)
    tanh = jnp.tanh(scale * (v + 0.044715 * v * v * v))
    return 0.5 * (1.0 + tanh) + 0.5 * v * (1.0 - tanh * tanh) * scale * (1.0 + 0.134145 * v * v)


def tile_at(step, size):
    return pl.ds(pl.multiple_of(step * size, size), size)


def flat(block):
    return block.reshape(block.shape[0] * block.shape[1], block.shape[2])


def store_part(part, columns, values):
    rows = part.shape[1]
    part[0, :, columns] = values[:rows]
    part[1, :, columns] = values[rows:]


def masked_probs(query, key, mask):
    scores = dense_right(query, key) * HEAD ** (-0.5)
    scores = jnp.where(mask, scores, masked_score)
    scores = jnp.exp(scores - jnp.max(scores, axis=1, keepdims=True))
    return scores / jnp.sum(scores, axis=1, keepdims=True)


def mask_of(seg_col, seg_row, at):
    length = seg_row.shape[2]
    place = lax.broadcasted_iota(jnp.int32, (length, length), 0)
    source = lax.broadcasted_iota(jnp.int32, (length, length), 1)
    return (source <= place) & (seg_col[at] == seg_row[at])


def ffn_forward_at(at, gath, part, weights, ins, outs):
    w_up, w_down = weights
    up_out, act_out = outs
    size = 256

    def up_tile(step, carry):
        columns = tile_at(step, size)
        up_rows = dense(flat(gath[at]), w_up[:, columns])
        up_out[at, :, columns] = up_rows.astype(jnp.bfloat16)
        act_out[at, :, columns] = gelu(up_rows).astype(jnp.bfloat16)
        return carry

    lax.fori_loop(0, w_up.shape[1] // size, up_tile, 0)

    def down_tile(step, carry):
        columns = tile_at(step, size)
        store_part(part, columns, dense(act_out[at], w_down[:, columns]))
        return carry

    lax.fori_loop(0, w_down.shape[1] // size, down_tile, 0)


def ffn_backward_at(at, gath, part, weights, ins, outs):
    w_up, w_down = weights
    (up_in,) = ins
    (upper_out,) = outs
    size = 256

    def act_tile(step, carry):
        columns = tile_at(step, size)
        grad_act = dense_right(flat(gath[at]), w_down[columns, :])
        slope = gelu_slope(up_in[at, :, columns].astype(jnp.float32))
        upper_out[at, :, columns] = (grad_act * slope).astype(jnp.bfloat16)
        return carry

    lax.fori_loop(0, w_down.shape[0] // size, act_tile, 0)

    def back_tile(step, carry):
        columns = tile_at(step, size)
        store_part(part, columns, dense_right(upper_out[at], w_up[columns, :]))
        return carry

    lax.fori_loop(0, w_up.shape[0] // size, back_tile, 0)


def attention_forward_at(at, gath, part, weights, ins, outs):
    w_query, w_keyvalue, w_out = weights
    seg_col, seg_row = ins
    query_out, keyvalue_out, mixed_out = outs
    size = 256
    rows = flat(gath[at])
    query_out[at] = dense(rows, w_query[...]).astype(jnp.bfloat16)
    keyvalue_out[at] = dense(rows, w_keyvalue[...]).astype(jnp.bfloat16)
    mask = mask_of(seg_col, seg_row, at)
    for head in range(w_query.shape[1] // HEAD):
        own = slice(head * HEAD, (head + 1) * HEAD)
        probs = masked_probs(query_out[at, :, own], keyvalue_out[at, :, :HEAD], mask)
        mixed = dense(probs.astype(jnp.bfloat16), keyvalue_out[at, :, HEAD:])
        mixed_out[at, :, own] = mixed.astype(jnp.bfloat16)

    def out_tile(step, carry):
        columns = tile_at(step, size)
        store_part(part, columns, dense(mixed_out[at], w_out[:, columns]))
        return carry

    lax.fori_loop(0, w_out.shape[1] // size, out_tile, 0)


def attention_backward_at(at, gath, part, weights, ins, outs):
    w_query, w_keyvalue, w_out = weights
    seg_col, seg_row, query_in, keyvalue_in = ins
    query_out, keyvalue_out = outs
    size = 256
    scale = HEAD ** (-0.5)
    grad_mixed = dense_right(flat(gath[at]), w_out[...]).astype(jnp.bfloat16)
    key = keyvalue_in[at, :, :HEAD]
    value = keyvalue_in[at, :, HEAD:]
    mask = mask_of(seg_col, seg_row, at)
    grad_key = jnp.zeros(key.shape, jnp.float32)
    grad_value = jnp.zeros(value.shape, jnp.float32)
    for head in range(w_query.shape[1] // HEAD):
        own = slice(head * HEAD, (head + 1) * HEAD)
        query = query_in[at, :, own]
        branch = grad_mixed[:, own]
        probs = masked_probs(query, key, mask)
        grad_probs = dense_right(branch, value)
        inner = jnp.sum(probs * grad_probs, axis=1, keepdims=True)
        grad_scores = (probs * (grad_probs - inner)).astype(jnp.bfloat16)
        query_out[at, :, own] = (dense(grad_scores, key) * scale).astype(jnp.bfloat16)
        grad_key = grad_key + dense_left(grad_scores, query)
        grad_value = grad_value + dense_left(probs.astype(jnp.bfloat16), branch)
    keyvalue_out[at, :, :HEAD] = (grad_key * scale).astype(jnp.bfloat16)
    keyvalue_out[at, :, HEAD:] = grad_value.astype(jnp.bfloat16)

    def back_tile(step, carry):
        columns = tile_at(step, size)
        store_part(
            part,
            columns,
            dense_right(query_out[at], w_query[columns, :])
            + dense_right(keyvalue_out[at], w_keyvalue[columns, :]),
        )
        return carry

    lax.fori_loop(0, w_query.shape[0] // size, back_tile, 0)


class Rows:
    def __init__(self, one, two, rows, near_send, near_recv, far_send, far_recv, local):
        section, ctx, me = lax.axis_index("section"), lax.axis_index("ctx"), lax.axis_index("dp")
        k = me % 2
        self.early, self.stays = section == 0, k == ctx
        self.one, self.two = one, two
        place = {"ctx": k, "dp": me - k + ctx}
        self.peers = (place, {**place, "section": 1 - section})

        def near(source, at):
            return pltpu.make_async_remote_copy(
                source, rows.at[at], near_send, near_recv, device_id=place, device_id_type=MESH
            )

        def far(source, at):
            return pltpu.make_async_remote_copy(
                source, rows.at[at], far_send, far_recv,
                device_id=self.peers[1], device_id_type=MESH,
            )

        self.near = lambda source: near(source, section)
        self.far = lambda source: far(source, section)
        self.far_in = far(two, 1 - section)
        self.kept = lambda source: pltpu.make_async_copy(source, rows.at[section], local)
        self.count = 1 + jnp.where(self.stays, 0, 1)

    def greet(self, barrier):
        pl.semaphore_signal(barrier, inc=1, device_id=self.peers[1], device_id_type=MESH)

        @pl.when(jnp.logical_not(self.stays))
        def _():
            pl.semaphore_signal(barrier, inc=1, device_id=self.peers[0], device_id_type=MESH)

    def start(self):
        for cond, mine, other in (
            (self.early, self.one, self.two),
            (jnp.logical_not(self.early), self.two, self.one),
        ):

            @pl.when(cond)
            def _():
                self.far(other).start()

            @pl.when(cond & self.stays)
            def _():
                self.kept(mine).start()

            @pl.when(cond & jnp.logical_not(self.stays))
            def _():
                self.near(mine).start()

    def wait(self):
        self.far(self.two).wait_send()
        self.far_in.wait_recv()

        @pl.when(self.stays)
        def _():
            self.kept(self.one).wait()

        @pl.when(jnp.logical_not(self.stays))
        def _():
            self.near(self.one).wait()


def half_of(ref, which):
    half = ref.shape[-2] // 2
    at = pl.ds(pl.multiple_of(which * half, half), half)
    return ref.at[at] if len(ref.shape) == 2 else ref.at[:, at]


def half_shape(shape):
    return shape[:-2] + (shape[-2] // 2, shape[-1])


def pass_kernel(compute, n_weights, n_ins, n_outs, places, side_axes, has_rows, *refs):
    refs = list(refs)
    take = lambda count: [refs.pop(0) for _ in range(count)]
    (x_ref,) = take(1)
    early_weights = take(n_weights)
    late_weights = take(n_weights)
    ins = take(n_ins)
    side_from = take(len(side_axes))
    rows_from = take(2 * has_rows)
    (y_ref,) = take(1)
    given = take(1 + n_outs)
    side_to = take(len(side_axes))
    rows_to = take(has_rows)
    kept = take(1 + n_outs)
    gath, outs = kept[0], kept[1:]
    weights = take(n_weights)
    part, partner_out, partner_in, total, line_out, from_left, from_right = take(7)
    (
        weight_sem, gather_right, gather_left, gather_partner, gather_line_in, gather_partner_in,
        partner_send, partner_recv, right_send, right_recv, left_send, left_recv,
        side_send, side_recv, given_sem, rows_sem,
    ) = take(16)

    section = lax.axis_index("section")
    me = lax.axis_index("dp")
    z = me // 2
    k = me % 2
    last = places - 1
    rows = x_ref.shape[0]
    size = rows // PARTS
    right = {"dp": me + 2}
    left = {"dp": me - 2}
    partner = {"dp": 2 * z + 1 - k}
    has_left = z > 0
    has_right = z < last

    barrier = pltpu.get_barrier_semaphore()
    pl.semaphore_signal(barrier, inc=1, device_id=partner, device_id_type=MESH)

    @pl.when(has_left)
    def _():
        pl.semaphore_signal(barrier, inc=1, device_id=left, device_id_type=MESH)

    @pl.when(has_right)
    def _():
        pl.semaphore_signal(barrier, inc=1, device_id=right, device_id_type=MESH)

    for index in range(n_weights):

        @pl.when(section == 0)
        def _():
            pltpu.make_async_copy(early_weights[index], weights[index], weight_sem.at[index]).start()

        @pl.when(section != 0)
        def _():
            pltpu.make_async_copy(late_weights[index], weights[index], weight_sem.at[index]).start()

    far = {"ctx": 1 - lax.axis_index("ctx"), "section": 1 - section}
    for axis in sorted(set(side_axes)):
        pl.semaphore_signal(barrier, inc=1, device_id={axis: far[axis]}, device_id_type=MESH)
    moved = [Rows(*rows_from, *rows_to, *[rows_sem.at[i] for i in range(5)])] if has_rows else []
    for rows_back in moved:
        rows_back.greet(barrier)
    extra = sum([rows_back.count for rows_back in moved], len(set(side_axes)))
    peers = 1 + extra + jnp.where(has_left, 1, 0) + jnp.where(has_right, 1, 0)
    pl.semaphore_wait(barrier, peers)

    sides = []
    for index, axis in enumerate(side_axes):
        source, target = side_from[index], side_to[index]
        if axis == "ctx":
            source = half_of(source, far["ctx"])
        sides.append(
            pltpu.make_async_remote_copy(
                source, target, side_send.at[index], side_recv.at[index],
                device_id={axis: far[axis]}, device_id_type=MESH,
            )
        )

    def cut(index):
        return pl.ds(index * size, size)

    def to_right(block, index, source):
        return pltpu.make_async_remote_copy(
            source, gath.at[block, k, cut(index)], gather_right.at[block, index],
            gather_line_in.at[block, index], device_id=right, device_id_type=MESH,
        )

    def to_left(block, index, source):
        return pltpu.make_async_remote_copy(
            source, gath.at[block, k, cut(index)], gather_left.at[block, index],
            gather_line_in.at[block, index], device_id=left, device_id_type=MESH,
        )

    def to_partner(block, source):
        return pltpu.make_async_remote_copy(
            source, gath.at[block, k], gather_partner.at[block],
            gather_partner_in.at[block], device_id=partner, device_id_type=MESH,
        )

    def sum_to_partner(block):
        return pltpu.make_async_remote_copy(
            partner_out.at[block], partner_in.at[block], partner_send.at[block],
            partner_recv.at[block], device_id=partner, device_id_type=MESH,
        )

    def sum_to_right(block, index):
        return pltpu.make_async_remote_copy(
            line_out.at[block, cut(index)], from_left.at[block, cut(index)],
            right_send.at[block, index], right_recv.at[block, index],
            device_id=right, device_id_type=MESH,
        )

    def sum_to_left(block, index):
        return pltpu.make_async_remote_copy(
            line_out.at[block, cut(index)], from_right.at[block, cut(index)],
            left_send.at[block, index], left_recv.at[block, index],
            device_id=left, device_id_type=MESH,
        )

    for index in range(PARTS):

        @pl.when(has_right)
        def _():
            to_right(z, index, x_ref.at[cut(index)]).start()

        @pl.when(has_left)
        def _():
            to_left(z, index, x_ref.at[cut(index)]).start()

    to_partner(z, x_ref).start()
    for copy in sides + moved:
        copy.start()
    gath[z, k] = x_ref[...]

    at_end = (z == 0) | (z == last)
    low_half = z < places // 2

    def give(block):
        return [
            pltpu.make_async_copy(kept[index].at[block], given[index].at[block], given_sem.at[index, block])
            for index in range(1 + n_outs)
        ]

    def step(i, carry):
        inner_block = jnp.where(i == 0, 1, jnp.where(i == 1, 0, i))
        low_block = jnp.where(z == 0, i, inner_block)
        high_block = last - jnp.where(z == last, i, inner_block)
        block = jnp.where(low_half, low_block, high_block)
        wave = jnp.where(at_end, i, jnp.where(i == 1, 1, jnp.where(i == 3, 2, 0)))
        from_low = z - wave
        from_high = z + wave

        @pl.when((wave > 0) & (from_low >= 0))
        def _():
            for index in range(PARTS):
                to_right(from_low, index, gath.at[from_low, k, cut(index)]).wait_recv()

                @pl.when(has_right)
                def _():
                    to_right(from_low, index, gath.at[from_low, k, cut(index)]).start()

            to_partner(from_low, gath.at[from_low, k]).start()

        @pl.when((wave > 0) & (from_high <= last))
        def _():
            for index in range(PARTS):
                to_left(from_high, index, gath.at[from_high, k, cut(index)]).wait_recv()

                @pl.when(has_left)
                def _():
                    to_left(from_high, index, gath.at[from_high, k, cut(index)]).start()

            to_partner(from_high, gath.at[from_high, k]).start()

        pltpu.make_async_remote_copy(
            gath.at[block, 1 - k], gath.at[block, 1 - k], gather_partner.at[block],
            gather_partner_in.at[block], device_id=partner, device_id_type=MESH,
        ).wait_recv()

        @pl.when(i == 0)
        def _():
            for index in range(n_weights):
                pltpu.make_async_copy(
                    early_weights[index], weights[index], weight_sem.at[index]
                ).wait()

        compute(block, gath, part, weights, ins, outs)
        partner_out[block] = part[1 - k].astype(jnp.bfloat16)
        sum_to_partner(block).start()
        sum_to_partner(block).wait_recv()
        total[block] = part[k] + partner_in[block].astype(jnp.float32)

        for copy in give(block):
            copy.start()

        @pl.when((z == 0) & (block > 0))
        def _():
            line_out[block] = total[block].astype(jnp.bfloat16)
            for index in range(PARTS):
                sum_to_right(block, index).start()

        @pl.when((z == last) & (block < last))
        def _():
            line_out[block] = total[block].astype(jnp.bfloat16)
            for index in range(PARTS):
                sum_to_left(block, index).start()

        return carry

    lax.fori_loop(0, places, step, 0)

    n_left = jnp.where(has_left, places - z, 0)
    n_right = jnp.where(has_right, z + 1, 0)
    n_first = jnp.where(low_half, n_left, n_right)

    def finish(i, carry):
        in_first = i < n_first
        turn = jnp.where(in_first, i, i - n_first)
        is_left = in_first == low_half
        block = jnp.where(is_left, z + turn, z - turn)

        @pl.when(is_left)
        def _():
            for index in range(PARTS):
                sum_to_right(block, index).wait_recv()
                total[block, cut(index)] += from_left[block, cut(index)].astype(jnp.float32)

                @pl.when(block > z)
                def _():
                    line_out[block, cut(index)] = total[block, cut(index)].astype(jnp.bfloat16)
                    sum_to_right(block, index).start()

        @pl.when(jnp.logical_not(is_left))
        def _():
            for index in range(PARTS):
                sum_to_left(block, index).wait_recv()
                total[block, cut(index)] += from_right[block, cut(index)].astype(jnp.float32)

                @pl.when(block < z)
                def _():
                    line_out[block, cut(index)] = total[block, cut(index)].astype(jnp.bfloat16)
                    sum_to_left(block, index).start()

        return carry

    lax.fori_loop(0, n_left + n_right, finish, 0)
    y_ref[...] = total[z]

    def drain(block, carry):
        to_partner(block, gath.at[block, k]).wait_send()
        sum_to_partner(block).wait_send()
        for copy in give(block):
            copy.wait()
        for index in range(PARTS):

            @pl.when((block <= z) & has_right)
            def _():
                to_right(block, index, gath.at[block, k, cut(index)]).wait_send()

            @pl.when((block >= z) & has_left)
            def _():
                to_left(block, index, gath.at[block, k, cut(index)]).wait_send()

            @pl.when(block > z)
            def _():
                sum_to_right(block, index).wait_send()

            @pl.when(block < z)
            def _():
                sum_to_left(block, index).wait_send()

        return carry

    lax.fori_loop(0, places, drain, 0)
    for copy in sides + moved:
        copy.wait()


def tensor_pass(compute, ident, x, early_weights, late_weights, ins, out_widths, sides=(), back=()):
    rows, width = x.shape
    places = lax.axis_size("dp") // 2
    vmem = pl.BlockSpec(memory_space=pltpu.VMEM)
    hbm = pl.BlockSpec(memory_space=pl.ANY)
    count = len(early_weights)
    dma = pltpu.SemaphoreType.DMA
    axes = [axis for axis, _ in sides]
    moved = [
        half_shape(array.shape) if axis == "ctx" else array.shape for axis, array in sides
    ]
    kernel = functools.partial(
        pass_kernel, compute, count, len(ins), len(out_widths), places, axes, len(back) // 2
    )
    call = pl.pallas_call(
        kernel,
        out_shape=[
            jax.ShapeDtypeStruct((rows, width), jnp.float32),
            jax.ShapeDtypeStruct((places, 2, rows, width), jnp.bfloat16),
        ]
        + [jax.ShapeDtypeStruct((places, 2 * rows, out), jnp.bfloat16) for out in out_widths]
        + [jax.ShapeDtypeStruct(shape, jnp.bfloat16) for shape in moved]
        + [jax.ShapeDtypeStruct((2, rows, width), jnp.bfloat16)] * (len(back) // 2),
        in_specs=[vmem] + [hbm] * (2 * count) + [vmem] * len(ins) + [hbm] * len(axes) + [vmem] * len(back),
        out_specs=[vmem] + [hbm] * (1 + len(out_widths) + len(axes) + len(back) // 2),
        scratch_shapes=[pltpu.VMEM((places, 2, rows, width), jnp.bfloat16)]
        + [pltpu.VMEM((places, 2 * rows, out), jnp.bfloat16) for out in out_widths]
        + [pltpu.VMEM(weight.shape, weight.dtype) for weight in early_weights]
        + [
            pltpu.VMEM((2, rows, width), jnp.float32),
            pltpu.VMEM((places, rows, width), jnp.bfloat16),
            pltpu.VMEM((places, rows, width), jnp.bfloat16),
            pltpu.VMEM((places, rows, width), jnp.float32),
            pltpu.VMEM((places, rows, width), jnp.bfloat16),
            pltpu.VMEM((places, rows, width), jnp.bfloat16),
            pltpu.VMEM((places, rows, width), jnp.bfloat16),
            dma((count,)),
            dma((places, PARTS)),
            dma((places, PARTS)),
            dma((places,)),
            dma((places, PARTS)),
            dma((places,)),
            dma((places,)),
            dma((places,)),
            dma((places, PARTS)),
            dma((places, PARTS)),
            dma((places, PARTS)),
            dma((places, PARTS)),
            dma((max(len(axes), 1),)),
            dma((max(len(axes), 1),)),
            dma((1 + len(out_widths), places)),
            dma((5,)),
        ],
        cost_estimate=pl.CostEstimate(
            flops=60_000_000_000, bytes_accessed=20_000_000, transcendentals=0
        ),
        compiler_params=pltpu.CompilerParams(
            collective_id=ident, has_side_effects=True, vmem_limit_bytes=60 * 1024 * 1024
        ),
    )
    return call(
        x, *early_weights, *late_weights, *ins, *[array for _, array in sides], *back
    )


def distribute_kernel(
    places, query, keyvalue, notes, out, up, down, tokens, cotangent,
    query_own, keyvalue_own, notes_own, up_own,
    query_far, keyvalue_far, notes_far, out_far, up_far, down_far, tokens_out, cotangent_out,
    local_sem, query_send, query_recv, keyvalue_send, keyvalue_recv, notes_send, notes_recv,
    up_send, up_recv,
    across_send, across_recv, over_send, over_recv, rows_send, rows_recv,
):
    section = lax.axis_index("section")
    ctx = lax.axis_index("ctx")
    me = lax.axis_index("dp")
    z = me // 2
    k = me % 2
    last = places - 1
    rows = query.shape[0]
    half = rows // 2
    head_width = query_own.shape[1]
    unit_width = up_own.shape[1]
    across = {"section": 1 - section}
    over = {"ctx": 1 - ctx}

    def group(away, act):
        if away == 0:
            act(2 * z + 1 - k)
            return

        @pl.when(z + away <= last)
        def _():
            act(2 * (z + away) + k)
            act(2 * (z + away) + 1 - k)

        @pl.when(z - away >= 0)
        def _():
            act(2 * (z - away) + k)
            act(2 * (z - away) + 1 - k)

    def peers(act):
        for away in range(places):
            group(away, act)

    def remote(source, target, send, recv, device):
        return pltpu.make_async_remote_copy(
            source, target, send, recv, device_id=device, device_id_type=MESH
        )

    def piece(owner, part, count):
        which = jnp.where(part == 0, ctx, 1 - ctx)
        return tile_at(2 * owner + which, count // 2)

    def query_copy(source, to):
        return remote(
            query.at[:, tile_at(to, head_width)], query_own.at[tile_at(source, rows)],
            query_send.at[to], query_recv.at[source], {"dp": to},
        )

    def keyvalue_copy(source, to):
        return remote(
            keyvalue, keyvalue_own.at[tile_at(source, rows)],
            keyvalue_send.at[to], keyvalue_recv.at[source], {"dp": to},
        )

    def notes_copy(source, to):
        return remote(
            notes, notes_own.at[tile_at(source, notes.shape[0])],
            notes_send.at[to], notes_recv.at[source], {"dp": to},
        )

    def up_copy(source, to, part):
        which = jnp.where(part == 0, ctx, 1 - ctx)
        return remote(
            up.at[tile_at(which, half), tile_at(to, unit_width)],
            up_own.at[piece(source, part, rows)],
            up_send.at[to, part], up_recv.at[source, part], {"dp": to},
        )

    barrier = pltpu.get_barrier_semaphore()

    def greet(to):
        pl.semaphore_signal(barrier, inc=1, device_id={"dp": to}, device_id_type=MESH)

    peers(greet)
    pl.semaphore_signal(barrier, inc=1, device_id=across, device_id_type=MESH)
    pl.semaphore_signal(barrier, inc=1, device_id=over, device_id_type=MESH)
    stays = k == ctx
    place = {"ctx": k, "dp": 2 * z + ctx}
    pairs = [(tokens.at[section, 0], tokens_out), (cotangent.at[section, 0], cotangent_out)]
    rows_moves = [
        remote(source, target, rows_send.at[i], rows_recv.at[i], place)
        for i, (source, target) in enumerate(pairs)
    ]
    rows_kept = [
        pltpu.make_async_copy(source, target, rows_send.at[2 + i])
        for i, (source, target) in enumerate(pairs)
    ]

    @pl.when(jnp.logical_not(stays))
    def _():
        pl.semaphore_signal(barrier, inc=1, device_id=place, device_id_type=MESH)

    pl.semaphore_wait(barrier, 2 * places + 1 + jnp.where(stays, 0, 1))

    local = [
        pltpu.make_async_copy(
            query.at[:, tile_at(me, head_width)], query_own.at[tile_at(me, rows)], local_sem.at[0]
        ),
        pltpu.make_async_copy(keyvalue, keyvalue_own.at[tile_at(me, rows)], local_sem.at[1]),
        pltpu.make_async_copy(notes, notes_own.at[tile_at(me, notes.shape[0])], local_sem.at[2]),
        pltpu.make_async_copy(
            up.at[:, tile_at(me, unit_width)], up_own.at[tile_at(me, rows)], local_sem.at[3]
        ),
    ]
    for copy in local:
        copy.start()
    peers(lambda to: notes_copy(me, to).start())
    peers(lambda to: query_copy(me, to).start())
    peers(lambda to: keyvalue_copy(me, to).start())
    peers(lambda to: up_copy(me, to, 0).start())

    pieces = 2 * places
    out_half = tile_at(ctx, out.shape[0] // 2)
    short = down.shape[0] // 2 // pieces
    flows = [(out, out_far, out_half)] + [
        (down, down_far, tile_at(pieces * ctx + index, short)) for index in range(pieces)
    ]

    def flow_across(slot):
        source, target, at = flows[slot]
        return remote(
            source.at[at], target.at[at], across_send.at[slot], across_recv.at[slot], across
        )

    def flow_over(slot):
        _, target, at = flows[slot]
        return remote(target.at[at], target.at[at], over_send.at[slot], over_recv.at[slot], over)

    first_slot = len(flows)
    kinds = [
        (notes_own, notes_far, notes.shape[0]),
        (query_own, query_far, rows),
        (keyvalue_own, keyvalue_far, rows),
        (up_own, up_far, rows),
    ]

    def block_across(kind, owner):
        own, far, count = kinds[kind]
        slot = first_slot + kind * 2 * places + owner
        at = piece(owner, 0, count)
        return remote(own.at[at], far.at[at], across_send.at[slot], across_recv.at[slot], across)

    def block_over(kind, owner):
        _, far, count = kinds[kind]
        slot = first_slot + kind * 2 * places + owner
        at = piece(owner, 0, count)
        return remote(far.at[at], far.at[at], over_send.at[slot], over_recv.at[slot], over)

    for slot in range(first_slot):
        flow_across(slot).start()
    peers(lambda to: up_copy(me, to, 1).start())

    def hand_over(slot):
        flow_across(slot).wait_recv()
        flow_over(slot).start()

    for index in range(3):
        local[index].wait()
    block_across(0, me).start()
    block_across(1, me).start()
    block_across(2, me).start()
    hand_over(0)

    def pass_query(source):
        notes_copy(source, me).wait_recv()
        block_across(0, source).start()
        query_copy(source, me).wait_recv()
        block_across(1, source).start()

    def pass_keyvalue(source):
        keyvalue_copy(source, me).wait_recv()
        block_across(2, source).start()

    peers(pass_query)
    for slot in range(1, 1 + pieces // 2):
        hand_over(slot)
    peers(pass_keyvalue)
    for slot in range(1 + pieces // 2, first_slot):
        hand_over(slot)
    local[3].wait()
    block_across(3, me).start()

    def pass_up(source):
        up_copy(source, me, 0).wait_recv()
        block_across(3, source).start()

    def over_block(kind):
        def move(owner):
            block_across(kind, owner).wait_recv()
            block_over(kind, owner).start()

        return move

    group(0, pass_up)
    group(1, pass_up)
    for kind in range(3):
        over_block(kind)(me)
        peers(over_block(kind))
    over_block(3)(me)
    for away in range(2, places):
        group(away, pass_up)
        group(away - 2, over_block(3))
    group(places - 2, over_block(3))
    group(places - 1, over_block(3))

    @pl.when(stays)
    def _():
        for copy in rows_kept:
            copy.start()
        for copy in rows_kept:
            copy.wait()

    @pl.when(jnp.logical_not(stays))
    def _():
        for copy in rows_moves:
            copy.start()
        for copy in rows_moves:
            copy.wait()

    peers(lambda source: up_copy(source, me, 1).wait_recv())

    def over_wait(slot_owner, carry):
        for kind in range(len(kinds)):
            block_over_in(kind, slot_owner).wait_recv()
            block_across(kind, slot_owner).wait_send()
            block_over(kind, slot_owner).wait_send()
        return carry

    def block_over_in(kind, owner):
        _, far, count = kinds[kind]
        slot = first_slot + kind * 2 * places + owner
        at = piece(owner, 1, count)
        return remote(far.at[at], far.at[at], over_send.at[slot], over_recv.at[slot], over)

    lax.fori_loop(0, 2 * places, over_wait, 0)
    for slot in range(first_slot):
        flow_over(slot).wait_recv()
        flow_across(slot).wait_send()
        flow_over(slot).wait_send()

    def sent(to):
        notes_copy(me, to).wait_send()
        query_copy(me, to).wait_send()
        keyvalue_copy(me, to).wait_send()
        up_copy(me, to, 0).wait_send()
        up_copy(me, to, 1).wait_send()

    peers(sent)


def distribute(query, keyvalue, notes, out, up, down, tokens, cotangent):
    size = lax.axis_size("dp")
    places = size // 2
    vmem = pl.BlockSpec(memory_space=pltpu.VMEM)
    hbm = pl.BlockSpec(memory_space=pl.ANY)
    dma = pltpu.SemaphoreType.DMA
    rows = query.shape[0] * size
    small = [
        (rows, query.shape[1] // size),
        (rows, keyvalue.shape[1]),
        (notes.shape[0] * size, notes.shape[1]),
    ]
    turned = (rows, up.shape[1] // size)
    shapes = small + [turned] + small + [out.shape, turned, down.shape]
    shapes += [tokens.shape[2:]] * 2
    slots = 1 + 5 * size
    return pl.pallas_call(
        functools.partial(distribute_kernel, places),
        name="distribute",
        out_shape=[jax.ShapeDtypeStruct(shape, jnp.bfloat16) for shape in shapes],
        in_specs=[vmem] * 3 + [hbm, vmem, hbm] + [vmem] * 2,
        out_specs=[hbm] * len(shapes),
        scratch_shapes=[dma((4,))]
        + [dma((size,))] * 6
        + [dma((size, 2))] * 2
        + [dma((slots,))] * 4
        + [dma((4,)), dma((2,))],
        cost_estimate=pl.CostEstimate(
            flops=150_000_000_000, bytes_accessed=20_000_000, transcendentals=0
        ),
        compiler_params=pltpu.CompilerParams(collective_id=4, has_side_effects=True),
    )(query, keyvalue, notes, out, up, down, tokens, cotangent)


def collect_kernel(
    places, up_full, down_full, query_full, out_full, up_moved, down_moved,
    up_late, down_late, query_late, out_late, up_far, down_far, query_far, out_far, small, grad_one, grad_two,
    up_out, down_out, query_out, out_out, small_out, rows_out,
    small_in, small_sum, small_far, small_total, small_side,
    up, up_in, up_part, up_side, down, down_in, down_part, down_side,
    query, query_in, query_part, query_side, out, out_in, out_part, out_side,
    local_sem, side_send, side_recv, across_send, across_recv,
    turn_send, turn_recv, over_send, over_recv, small_send, small_recv, rows_sem,
):
    section = lax.axis_index("section")
    ctx = lax.axis_index("ctx")
    me = lax.axis_index("dp")
    z = me // 2
    k = me % 2
    last = places - 1
    size = 2 * places
    early = section == 0
    late = section != 0
    across = {"section": 1 - section}
    over = {"ctx": 1 - ctx}
    chunks = 4
    short = down.shape[0] // chunks
    turned = [(up, up_out), (query, query_out)]
    half = up.shape[1]

    def group(away, act):
        if away == 0:
            act(2 * z + 1 - k)
            return

        @pl.when(z + away <= last)
        def _():
            act(2 * (z + away) + k)
            act(2 * (z + away) + 1 - k)

        @pl.when(z - away >= 0)
        def _():
            act(2 * (z - away) + k)
            act(2 * (z - away) + 1 - k)

    def peers(act):
        for away in range(places):
            group(away, act)

    def remote(source, target, send, recv, device):
        return pltpu.make_async_remote_copy(
            source, target, send, recv, device_id=device, device_id_type=MESH
        )

    barrier = pltpu.get_barrier_semaphore()

    def greet(to):
        pl.semaphore_signal(barrier, inc=1, device_id={"dp": to}, device_id_type=MESH)

    peers(greet)
    pl.semaphore_signal(barrier, inc=1, device_id=across, device_id_type=MESH)
    pl.semaphore_signal(barrier, inc=1, device_id=over, device_id_type=MESH)
    rows_back = Rows(grad_one, grad_two, rows_out, *[rows_sem.at[i] for i in range(5)])
    rows_back.greet(barrier)
    pl.semaphore_wait(barrier, size + 1 + rows_back.count)

    side = [
        remote(half_of(query_full, 1 - ctx), query_side, side_send.at[0], side_recv.at[0], over),
        remote(half_of(out_full, 1 - ctx), out_side, side_send.at[1], side_recv.at[1], over),
    ]
    for copy in side + [rows_back]:
        copy.start()

    def small_turn(source, to, layer):
        return remote(
            small.at[layer, to], small_in.at[layer, source],
            small_send.at[layer, to], small_recv.at[layer, source], {"dp": to},
        )

    own_small = [
        pltpu.make_async_copy(
            small.at[layer, me], small_in.at[layer, me], local_sem.at[13 + layer]
        )
        for layer in range(2)
    ]
    for layer in range(2):
        own_small[layer].start()

    def small_start(to):
        for layer in range(2):
            small_turn(me, to, layer).start()

    def small_wait(source):
        for layer in range(2):
            small_turn(source, me, layer).wait_recv()

    def small_sent(to):
        for layer in range(2):
            small_turn(me, to, layer).wait_send()

    small_across = remote(
        small_sum.at[1 - section], small_far, across_send.at[size + 6], across_recv.at[size + 6],
        across,
    )
    small_over = remote(small_total, small_side, side_send.at[2], side_recv.at[2], over)

    def up_across(owner):
        return remote(
            up_part.at[owner], up_in.at[owner], across_send.at[owner], across_recv.at[owner], across
        )

    def down_across(index):
        slot = size + index
        at = pl.ds(index * short, short)
        return remote(
            down_part.at[at], down_in.at[at], across_send.at[slot], across_recv.at[slot], across
        )

    query_across = remote(
        query_part, query_in, across_send.at[size + chunks], across_recv.at[size + chunks], across
    )
    out_across = remote(
        out_part, out_in, across_send.at[size + chunks + 1], across_recv.at[size + chunks + 1],
        across,
    )

    def load(index, source, target):
        copy = pltpu.make_async_copy(source, target, local_sem.at[index])
        copy.start()
        return copy

    loads = [
        load(0, half_of(up_full, ctx), up_part),
        load(1, up_moved, up_side),
        load(2, half_of(query_full, ctx), query_part),
        load(3, half_of(out_full, ctx), out_part),
        load(4, half_of(down_full, ctx), down_part),
        load(5, down_moved, down_side),
    ]
    owned = [
        (up_late, up), (up_far, up_in), (query_late, query), (query_far, query_in),
        (out_late, out), (out_far, out_in), (down_late, down), (down_far, down_in),
    ]

    @pl.when(late)
    def _():
        for index, (source, target) in enumerate(owned):
            load(15 + index, source, target)

    loads[0].wait()
    loads[1].wait()

    def send_up(owner):
        up_part[owner] = up_part[owner] + up_side[owner]

        @pl.when(late)
        def _():
            up_across(owner).start()

    peers(send_up)
    send_up(me)
    loads[2].wait()
    loads[3].wait()
    for copy in side:
        copy.wait_recv()
    query_part[...] = query_part[...] + query_side[...]
    out_part[...] = out_part[...] + out_side[...]
    loads[4].wait()
    loads[5].wait()
    down_part[...] = down_part[...] + down_side[...]

    @pl.when(late)
    def _():
        query_across.start()
        out_across.start()
        for index in range(chunks):
            down_across(index).start()
        for index, (source, target) in enumerate(owned):
            pltpu.make_async_copy(source, target, local_sem.at[15 + index]).wait()

    def turn(kind, source, to):
        block, target = turned[kind]
        width = block.shape[2]
        at = kind * size
        return remote(
            block.at[to], target.at[tile_at(ctx, half), tile_at(source, width)],
            turn_send.at[at + to], turn_recv.at[at + source], {"dp": to},
        )

    def own_block(kind):
        block, target = turned[kind]
        return pltpu.make_async_copy(
            block.at[me], target.at[tile_at(ctx, half), tile_at(me, block.shape[2])],
            local_sem.at[6 + kind],
        )

    def hand_over(kind, source, side_of):
        block, target = turned[kind]
        at = kind * size + source
        region = target.at[tile_at(side_of, half), tile_at(source, block.shape[2])]
        return remote(region, region, over_send.at[at], over_recv.at[at], over)

    def sum_up(owner):
        @pl.when(early)
        def _():
            up_across(owner).wait_recv()
            up[owner] = up_part[owner] + up_in[owner]

        @pl.when(late)
        def _():
            up[owner] = up[owner] + up_in[owner]

    def up_block(owner):
        sum_up(owner)
        turn(0, me, owner).start()

    def arrived(kind):
        def act(source):
            turn(kind, source, me).wait_recv()
            hand_over(kind, source, ctx).start()

        return act

    for away in range(places):
        group(away, up_block)
        if away > 0:
            group(away - 1, arrived(0))
    sum_up(me)
    peers(small_start)
    own_block(0).start()
    group(last, arrived(0))
    own_block(0).wait()
    hand_over(0, me, ctx).start()

    @pl.when(early)
    def _():
        query_across.wait_recv()
        query[...] = query_part[...] + query_in[...]
        out_across.wait_recv()
        out[...] = out_part[...] + out_in[...]

    @pl.when(late)
    def _():
        query[...] = query[...] + query_in[...]
        out[...] = out[...] + out_in[...]

    peers(lambda owner: turn(1, me, owner).start())
    own_block(1).start()

    def flat_over(index, side_of):
        slot = 2 * size + index
        if index == 0:
            source, target, at = out, out_out, tile_at(side_of, out.shape[0])
            return remote(source, target.at[at], over_send.at[slot], over_recv.at[slot], over), (
                pltpu.make_async_copy(source, target.at[at], local_sem.at[8])
            )
        source = down.at[pl.ds((index - 1) * short, short)]
        target = down_out.at[tile_at(side_of * chunks + index - 1, short)]
        return remote(source, target, over_send.at[slot], over_recv.at[slot], over), (
            pltpu.make_async_copy(source, target, local_sem.at[8 + index])
        )

    for copy in flat_over(0, ctx):
        copy.start()
    for index in range(chunks):

        @pl.when(early)
        def _():
            at = pl.ds(index * short, short)
            down_across(index).wait_recv()
            down[at] = down_part[at] + down_in[at]

        @pl.when(late)
        def _():
            at = pl.ds(index * short, short)
            down[at] = down[at] + down_in[at]

        for copy in flat_over(1 + index, ctx):
            copy.start()
    peers(arrived(1))
    own_block(1).wait()
    hand_over(1, me, ctx).start()
    for layer in range(2):
        own_small[layer].wait()
    peers(small_wait)
    for layer in range(2):
        total = small_in[layer, 0].astype(jnp.float32)
        for source in range(1, size):
            total = total + small_in[layer, source].astype(jnp.float32)
        small_sum[layer] = total.astype(jnp.bfloat16)
    small_across.start()


    small_across.wait_recv()
    small_total[...] = small_sum[section] + small_far[...]
    small_over.start()
    small_over.wait_recv()
    small_out[...] = (small_total[...] + small_side[...]).astype(jnp.float32)

    rows_back.wait()
    peers(small_sent)
    small_across.wait_send()
    small_over.wait_send()
    for copy in side:
        copy.wait_send()

    @pl.when(late)
    def _():
        peers(lambda owner: up_across(owner).wait_send())
        up_across(me).wait_send()
        query_across.wait_send()
        out_across.wait_send()
        for index in range(chunks):
            down_across(index).wait_send()

    for kind in range(2):
        peers(lambda owner: turn(kind, me, owner).wait_send())

        def finish(source, carry):
            hand_over(kind, source, ctx).wait_send()
            hand_over(kind, source, 1 - ctx).wait_recv()
            return carry

        lax.fori_loop(0, size, finish, 0)
    for index in range(1 + chunks):
        moved, kept = flat_over(index, ctx)
        kept.wait()
        moved.wait_send()
        flat_over(index, 1 - ctx)[0].wait_recv()


def collect(fulls, moved, late, far, small, rows):
    size = lax.axis_size("dp")
    hbm = pl.BlockSpec(memory_space=pl.ANY)
    dma = pltpu.SemaphoreType.DMA
    vmem = lambda x: pltpu.VMEM(x.shape, x.dtype)
    up, down, query, out = fulls
    shapes = [
        (up.shape[1], size * up.shape[2]),
        down.shape,
        (query.shape[1], size * query.shape[2]),
        out.shape,
    ]
    return pl.pallas_call(
        functools.partial(collect_kernel, size // 2),
        name="collect",
        out_shape=[jax.ShapeDtypeStruct(shape, jnp.bfloat16) for shape in shapes]
        + [jax.ShapeDtypeStruct(small.shape[2:], jnp.float32)]
        + [jax.ShapeDtypeStruct((2,) + rows[0].shape, jnp.bfloat16)],
        in_specs=[hbm] * 15 + [pl.BlockSpec(memory_space=pltpu.VMEM)] * 2,
        out_specs=[hbm] * 4 + [pl.BlockSpec(memory_space=pltpu.VMEM), hbm],
        scratch_shapes=[vmem(small), vmem(small[:, 0])]
        + [vmem(small[0, 0])] * 3
        + [vmem(x) for x in late for _ in range(4)]
        + [dma((23,)), dma((3,)), dma((3,))]
        + [dma((size + 7,))] * 2
        + [dma((2 * size,))] * 2
        + [dma((2 * size + 5,))] * 2
        + [dma((2, size))] * 2
        + [dma((5,))],
        cost_estimate=pl.CostEstimate(
            flops=120_000_000_000, bytes_accessed=20_000_000, transcendentals=0
        ),
        compiler_params=pltpu.CompilerParams(collective_id=5, has_side_effects=True),
    )(*fulls, *moved, *late, *far, small, *rows)


def own_half(grad):
    half = grad.shape[-2] // 2
    return lax.dynamic_slice_in_dim(grad, lax.axis_index("ctx") * half, half, axis=-2)


def spread_body(*args):
    return spread_step(*args)


def spread_step(
    tokens, cotangent, segment_ids, w_query, w_keyvalue, w_out, w_up, w_down, ln_gains, ln_biases
):
    section = lax.axis_index("section")
    ctx = lax.axis_index("ctx")
    size = lax.axis_size("dp")
    places = size // 2
    early = section == 0
    width = tokens.shape[3]
    length = segment_ids.shape[2]
    tall = (places * tokens.shape[2] * 2, -1)

    def own_micro(x):
        return lax.dynamic_index_in_dim(x, section, 0, keepdims=False)[0]

    out, down = w_out[0], w_down[0]
    columns = ln_gains.shape[2]
    notes = jnp.concatenate(
        [ln_gains[0], ln_biases[0], own_micro(segment_ids).astype(jnp.bfloat16)[None]], axis=0
    )
    notes = jnp.pad(notes, ((0, 32 - notes.shape[0]), (0, 0)))
    query, keyvalue, notes, up, query_far, keyvalue_far, notes_far, out_far, *rest = (
        distribute(w_query[0], w_keyvalue[0], notes, out, w_up[0], down, tokens, cotangent)
    )
    up_far, down_far, hidden, grad_low = rest
    hidden = hidden.astype(jnp.float32)
    notes = notes.reshape(size, 32, columns).transpose(1, 0, 2)
    near = notes[:4].reshape(4, width).astype(jnp.float32)
    far = notes_far.reshape(size, 32, columns).transpose(1, 0, 2)[:4].reshape(4, width)
    far = far.astype(jnp.float32)
    scales = [jnp.where(early, near, far), jnp.where(early, far, near)]
    segments = notes[4].astype(jnp.int32).reshape(places, 2, length)
    segments = lax.dynamic_index_in_dim(segments, ctx, 1, keepdims=False)
    segs = [segments[:, :, None], segments[:, None, :]]
    attention_near, attention_far = [query, keyvalue, out], [query_far, keyvalue_far, out_far]
    attention_weights = [(attention_near, attention_far), (attention_far, attention_near)]
    ffn_weights = [([up, down], [up_far, down_far]), ([up_far, down_far], [up, down])]
    head_width = query.shape[1]
    unit_width = up.shape[1]

    def forward(layer, hidden):
        normed = layer_norm(hidden, scales[layer][0], scales[layer][2]).astype(jnp.bfloat16)
        y, normed_all, q, kv, mixed = tensor_pass(
            attention_forward_at, 0, normed, *attention_weights[layer], segs,
            [head_width, keyvalue.shape[1], head_width],
        )
        after = hidden + y
        normed_two = layer_norm(after, scales[layer][1], scales[layer][3]).astype(jnp.bfloat16)
        y, normed_two_all, up_rows, activated = tensor_pass(
            ffn_forward_at, 1, normed_two, *ffn_weights[layer], [],
            [unit_width, unit_width],
        )
        result = (after + y).astype(jnp.bfloat16)
        return result, (hidden, normed_all, q, kv, mixed, after, normed_two_all, up_rows, activated)

    def product(left, right):
        return dense_left(left.reshape(tall), right.reshape(tall)).astype(jnp.bfloat16)

    def rows_of_all(grad):
        return grad.reshape(size, grad.shape[0] // size, grad.shape[1])

    def ffn_backward(layer, ident, grad_low, kept, sides, back=()):
        _, _, _, _, _, after, normed_two_all, up_rows, activated = kept
        y, grad_low_all, grad_upper, *arrived = tensor_pass(
            ffn_backward_at, ident, grad_low, *ffn_weights[layer],
            [up_rows], [unit_width], sides, back,
        )
        grads = [
            rows_of_all(product(normed_two_all, grad_upper)),
            product(activated, grad_low_all),
        ]
        _, norm_back = jax.vjp(layer_norm, after, scales[layer][1], scales[layer][3])
        grad_norm, gain, bias = norm_back(y)
        return grad_low.astype(jnp.float32) + grad_norm, grads, [gain, bias], arrived

    def attention_backward(layer, ident, grad_after, grad_branch, kept, sides):
        hidden, normed_all, q, kv, mixed, _, _, _, _ = kept
        y, grad_branch_all, grad_query, grad_kv, *arrived = tensor_pass(
            attention_backward_at, ident, grad_branch,
            *attention_weights[layer], segs + [q, kv], [head_width, keyvalue.shape[1]], sides,
        )
        grads = [
            rows_of_all(product(normed_all, grad_query)),
            product(mixed, grad_branch_all),
        ]
        keyvalue_grad = product(normed_all, grad_kv)
        _, norm_back = jax.vjp(layer_norm, hidden, scales[layer][0], scales[layer][2])
        grad_norm, gain, bias = norm_back(y)
        return (
            (grad_after + grad_norm).astype(jnp.bfloat16), grads, keyvalue_grad, [gain, bias], arrived
        )

    def low(x):
        return x.astype(jnp.bfloat16)

    def ctx_sums(grads, arrived):
        return [own_half(grad) + other for grad, other in zip(grads, arrived)]

    hold = lax.optimization_barrier
    first, kept_first = forward(0, hidden)
    second, kept_second = forward(1, first.astype(jnp.float32))

    def sides(axis, arrays):
        return [(axis, array) for array in arrays]

    grad_after, ffn_two, scales_two, (section_rows,) = ffn_backward(
        1, 2, grad_low, kept_second, [], [first, second]
    )
    branch, up_two, down_two = hold((low(grad_after), *ffn_two))
    grad_second, attention_two, keyvalue_two, more, arrived = attention_backward(
        1, 3, grad_after, branch, kept_second, sides("ctx", [up_two])
    )
    scales_two = more[:1] + scales_two[:1] + more[1:] + scales_two[1:]
    (up_two,) = ctx_sums([up_two], arrived)
    grad_after, ffn_one, scales_one, arrived = ffn_backward(
        0, 6, grad_second, kept_first,
        sides("section", [up_two]) + sides("ctx", [down_two] + attention_two),
    )
    up_two_far = arrived[0]
    down_two, *attention_two = ctx_sums([down_two] + attention_two, arrived[1:])
    branch, *both = hold((low(grad_after), *ffn_one, down_two, *attention_two))
    ffn_one, rest_two = both[:2], both[2:]
    grad_first, attention_one, keyvalue_one, more, arrived = attention_backward(
        0, 7, grad_after, branch, kept_first,
        sides("ctx", ffn_one) + sides("section", rest_two),
    )
    scales_one = more[:1] + scales_one[:1] + more[1:] + scales_one[1:]
    ffn_moved, rest_far = arrived[:2], arrived[2:]

    def small_of(keyvalue_grad, rows):
        rows = low(jnp.stack(rows)).reshape(4, size, columns).transpose(1, 0, 2)
        rows = jnp.pad(rows, ((0, 0), (0, 12), (0, 0)))
        return jnp.concatenate([keyvalue_grad.reshape(size, columns, -1), rows], axis=1)

    small = jnp.stack([small_of(keyvalue_one, scales_one), small_of(keyvalue_two, scales_two)])
    up_grad, down_grad, query_grad, out_grad, small, grad_rows = collect(
        ffn_one + attention_one, ffn_moved, [up_two] + rest_two, [up_two_far] + rest_far, small,
        [grad_first, grad_second],
    )
    scale_grads = small[None, columns : columns + 4]

    def given(grad):
        return grad.astype(jnp.float32)[None]

    return (
        section_rows[None, :, None],
        grad_rows[None, :, None],
        given(query_grad),
        small[None, :columns],
        given(out_grad),
        given(up_grad),
        given(down_grad),
        scale_grads[:, 0:2],
        scale_grads[:, 2:4],
    )


def from_behind(x, axis, by):
    devices = lax.axis_size(axis)
    pairs = [(i, i + by) for i in range(devices) if 0 <= i + by < devices]
    return lax.ppermute(x, axis, pairs)


def allowed_keys(segments, cycle_place, cycle_size, tok_rows):
    offsets = jnp.arange(tok_rows, dtype=jnp.int32)
    query_pos = cycle_place * tok_rows + offsets
    query_seg = lax.dynamic_slice_in_dim(segments, cycle_place * tok_rows, tok_rows, axis=1)
    blocks = []
    for cycle_step in range(cycle_size):
        source = cycle_place - cycle_step
        key_pos = source * tok_rows + offsets
        key_seg = lax.dynamic_slice_in_dim(
            segments, jnp.maximum(source, 0) * tok_rows, tok_rows, axis=1
        )
        blocks.append(
            (source >= 0)
            & (key_pos[None, None, :] <= query_pos[None, :, None])
            & (key_seg[:, None, :] == query_seg[:, :, None])
        )
    return jnp.concatenate(blocks, axis=2)


def batched(left, right, left_dim, right_dim):
    return lax.dot_general(
        left, right, (((left_dim,), (right_dim,)), ((0,), (0,))), preferred_element_type=jnp.float32
    )


def head_scores(query, keyvalue_all, allowed):
    micro, rows, _ = allowed.shape
    head_rows = query.reshape(micro, rows * HEADS, HEAD)
    scores = batched(head_rows, keyvalue_all[:, :, :HEAD], 2, 2) * HEAD ** (-0.5)
    scores = scores.reshape(micro, rows, HEADS, -1)
    scores = jnp.where(allowed[:, :, None, :], scores, masked_score)
    return (scores.reshape(micro, rows * HEADS, -1), head_rows)


def layer_forward(hidden, segments, weights, micro, cycle_place, cycle_size):
    w_query, w_keyvalue, w_out, w_up, w_down, gains, biases = weights
    rows = hidden.shape[0] // micro
    normed = layer_norm(hidden, gains[0], biases[0]).astype(jnp.bfloat16)
    query = dense(normed, w_query).astype(jnp.bfloat16)
    keyvalue = dense(normed, w_keyvalue).astype(jnp.bfloat16)
    moving = from_behind(keyvalue, "ctx", 1)
    keyvalue_all = jnp.concatenate(
        [keyvalue.reshape(micro, rows, -1), moving.reshape(micro, rows, -1)], axis=1
    )
    allowed = allowed_keys(segments, cycle_place, cycle_size, rows)
    scores, _ = head_scores(query, keyvalue_all, allowed)
    top_score = jnp.max(scores, axis=2, keepdims=True)
    log_total = top_score + jnp.log(jnp.sum(jnp.exp(scores - top_score), axis=2, keepdims=True))
    attn_probs = jnp.exp(scores - log_total).astype(jnp.bfloat16)
    mixed = (
        batched(attn_probs, keyvalue_all[:, :, HEAD:], 2, 1)
        .reshape(micro * rows, HEADS * HEAD)
        .astype(jnp.bfloat16)
    )
    after = hidden + dense(mixed, w_out)
    normed_two = layer_norm(after, gains[1], biases[1]).astype(jnp.bfloat16)
    up_rows = dense(normed_two, w_up)
    activated = jax.nn.gelu(up_rows, approximate=True).astype(jnp.bfloat16)
    result = after + dense(activated, w_down)
    kept = (
        hidden,
        normed,
        query,
        keyvalue_all,
        log_total,
        mixed,
        after,
        normed_two,
        up_rows,
        activated,
    )
    return (result, kept)


def layer_backward(grad_result, kept, segments, weights, micro, cycle_place, cycle_size):
    w_query, w_keyvalue, w_out, w_up, w_down, gains, biases = weights
    hidden, normed, query, keyvalue_all, log_total, mixed, after, normed_two, up_rows, activated = (
        kept
    )
    rows = hidden.shape[0] // micro
    grad_low = grad_result.astype(jnp.bfloat16)
    grad_act = dense_right(grad_low, w_down)
    _, gelu_back = jax.vjp(lambda entries: jax.nn.gelu(entries, approximate=True), up_rows)
    grad_upper = gelu_back(grad_act)[0].astype(jnp.bfloat16)
    _, norm_back_two = jax.vjp(layer_norm, after, gains[1], biases[1])
    grad_after_norm, grad_gain_two, grad_bias_two = norm_back_two(dense_right(grad_upper, w_up))
    grad_after = grad_result + grad_after_norm
    grad_branch = grad_after.astype(jnp.bfloat16)
    grad_mixed = (
        dense_right(grad_branch, w_out).astype(jnp.bfloat16).reshape(micro, rows * HEADS, HEAD)
    )
    allowed = allowed_keys(segments, cycle_place, cycle_size, rows)
    scores, head_rows = head_scores(query, keyvalue_all, allowed)
    attn_probs = jnp.exp(scores - log_total)
    grad_probs = batched(grad_mixed, keyvalue_all[:, :, HEAD:], 2, 2)
    grad_values = batched(attn_probs.astype(jnp.bfloat16), grad_mixed, 1, 1)
    inner = jnp.sum(attn_probs * grad_probs, axis=2, keepdims=True)
    grad_scores = (attn_probs * (grad_probs - inner)).astype(jnp.bfloat16)
    scale_factor = HEAD ** (-0.5)
    grad_queries = (
        (batched(grad_scores, keyvalue_all[:, :, :HEAD], 2, 1) * scale_factor)
        .astype(jnp.bfloat16)
        .reshape(micro * rows, HEADS * HEAD)
    )
    grad_keys = batched(grad_scores, head_rows, 1, 1) * scale_factor
    grad_pieces = jnp.concatenate([grad_keys, grad_values], axis=2)
    carried = grad_pieces[:, (cycle_size - 1) * rows :]
    carried = (
        from_behind(carried.astype(jnp.bfloat16), "ctx", -1).astype(carried.dtype)
        + grad_pieces[:, 0:rows]
    )
    grad_kv = carried.astype(jnp.bfloat16).reshape(micro * rows, -1)
    grad_normed = dense_right(grad_queries, w_query) + dense_right(grad_kv, w_keyvalue)
    _, norm_back_one = jax.vjp(layer_norm, hidden, gains[0], biases[0])
    grad_hidden, grad_gain_one, grad_bias_one = norm_back_one(grad_normed)
    grad_input = grad_after + grad_hidden
    terms = (
        normed,
        grad_queries,
        grad_kv,
        mixed,
        grad_branch,
        normed_two,
        grad_upper,
        activated,
        grad_low,
        jnp.stack([grad_gain_one, grad_gain_two, grad_bias_one, grad_bias_two]),
    )
    return (grad_input, terms)


def body(
    tokens, cotangent, segment_ids, w_query, w_keyvalue, w_out, w_up, w_down, ln_gains, ln_biases
):
    section_index = lax.axis_index("section")
    cycle_place = lax.axis_index("ctx")
    cycle_size = lax.axis_size("ctx")
    micro = tokens.shape[0]
    width = tokens.shape[3]
    early = section_index == 0
    segments = segment_ids[:, 0]
    own_tokens = tokens[:, 0].reshape(-1, width)
    own_cotangent = cotangent[:, 0].reshape(-1, width)

    def spread(weight):
        half = weight.shape[1] // cycle_size
        part = lax.dynamic_slice_in_dim(weight, cycle_place * half, half, axis=1)
        return lax.all_gather(part, ("dp", "ctx"), axis=1, tiled=True)[0]

    scales = lax.all_gather(
        jnp.concatenate([ln_gains, ln_biases], axis=1), "dp", axis=2, tiled=True
    )[0].astype(jnp.float32)
    weights = (
        spread(w_query),
        lax.all_gather(w_keyvalue, "dp", axis=1, tiled=True)[0],
        spread(w_out),
        spread(w_up),
        spread(w_down),
        scales[0:2],
        scales[2:4],
    )
    result, kept_first = layer_forward(
        own_tokens.astype(jnp.float32), segments, weights, micro, cycle_place, cycle_size
    )
    first_low = result.astype(jnp.bfloat16)
    incoming = from_behind(first_low, "section", 1)
    result, kept_second = layer_forward(
        incoming.astype(jnp.float32), segments, weights, micro, cycle_place, cycle_size
    )
    second_low = result.astype(jnp.bfloat16)
    grad, terms_second = layer_backward(
        own_cotangent.astype(jnp.float32), kept_second, segments, weights, micro, cycle_place,
        cycle_size,
    )
    grad_second = grad.astype(jnp.bfloat16)
    arriving = from_behind(grad_second, "section", -1)
    grad, terms_first = layer_backward(
        arriving.astype(jnp.float32), kept_first, segments, weights, micro, cycle_place, cycle_size
    )
    grad_first = grad.astype(jnp.bfloat16)
    section_rows = jnp.where(early, first_low, second_low)
    grad_rows = jnp.where(early, grad_first, grad_second)
    (
        normed_all,
        grad_queries_all,
        grad_kv_all,
        mixed_all,
        grad_branch_all,
        normed_two_all,
        grad_upper_all,
        activated_all,
        grad_low_all,
        scale_terms,
    ) = [jnp.where(early, one, two) for one, two in zip(terms_first, terms_second)]

    def reduced(left, right):
        part = dense_left(left, right).astype(jnp.bfloat16)
        piece = lax.psum_scatter(part, ("dp", "ctx"), scatter_dimension=0, tiled=True)
        return lax.all_gather(piece, "ctx", axis=0, tiled=True).astype(jnp.float32)[None]

    grad_down = reduced(activated_all, grad_low_all)
    grad_up = reduced(normed_two_all, grad_upper_all)
    grad_out = reduced(mixed_all, grad_branch_all)
    grad_query = reduced(normed_all, grad_queries_all)
    grad_keyvalue = reduced(normed_all, grad_kv_all)
    scale_grads = lax.psum(
        lax.psum_scatter(
            scale_terms.astype(jnp.bfloat16), "dp", scatter_dimension=1, tiled=True
        ),
        "ctx",
    ).astype(jnp.float32)[None]
    local = (1, micro, 1, own_tokens.shape[0] // micro, width)
    return (
        section_rows.reshape(local),
        grad_rows.reshape(local),
        grad_query,
        grad_keyvalue,
        grad_out,
        grad_up,
        grad_down,
        scale_grads[:, 0:2],
        scale_grads[:, 2:4],
    )


def solution(mesh):
    in_specs = (
        P(None, "dp", "ctx", None),
        P(None, "dp", "ctx", None),
        P(None, "dp", None),
        P("section", "dp", None),
        P("section", "dp", None),
        P("section", "dp", None),
        P("section", "dp", None),
        P("section", "dp", None),
        P("section", None, "dp"),
        P("section", None, "dp"),
    )
    out_specs = (
        P("section", None, "dp", "ctx", None),
        P("section", None, "dp", "ctx", None),
        P("section", "dp", None),
        P("section", "dp", None),
        P("section", "dp", None),
        P("section", "dp", None),
        P("section", "dp", None),
        P("section", None, "dp"),
        P("section", None, "dp"),
    )
    spread = mesh.shape["dp"] == 8
    return jax.shard_map(
        spread_body if spread else body,
        mesh=mesh, in_specs=in_specs, out_specs=out_specs, check_vma=False,
    )
```
